512 devices in a mesh: gx: 16 (over y, core), gy: 4 (over x), gz: 8 (over z).
Axes of the slice: x: 4, y: 8, z: 8, core: 2. Of those that a mesh axis runs over, the one named last changes fastest.
Arguments:
- fractions: float32 [3, 16, 8, 16, 128], P(None, 'gx', 'gy', 'gz'), may hold values from 0 to 1
- polarizability: float32 [16, 8, 16, 128], P('gx', 'gy', 'gz'), may hold values from 0.5 to 2
- occupancy: int32 [16, 8, 16, 128], P('gx', 'gy', 'gz'), may hold values 0 or 1
- pair_mask: int32 [16, 8, 16, 27], P('gx', 'gy', 'gz'), may hold values from 0 to 1, as said below
- perm_field: float32 [6, 16, 8, 16, 128], P(None, 'gx', 'gy', 'gz'), may hold values from -6 to 6
- history: float32 [6, 6, 16, 8, 16, 128], P(None, None, 'gx', 'gy', 'gz'), may hold values from -12 to 12
Outputs:
- induced: float32 [6, 16, 8, 16, 128], P(None, 'gx', 'gy', 'gz')
- change: float32 [], replicated
The draws below stay inside these ranges and needn't reach their ends.
Inputs may be any that keep to these rules, and one draw needn't show every extreme that they name: pair_mask[t, k] equals pair_mask at tile t + offset(k) for the opposite offset 26 - k (periodic); pair_mask[t, 13] (the tile itself) is 1.
All inputs are finite; a program needn't handle non-finite values. No bound on the sum of `occupancy` on one device may be relied on, other than what follows from the above.
Results may differ from the reference program's by a relative error of at most 0.0003.
Values sent between devices are 32-bit elements; how exact they have to be, the bound alone decides.
No kernel may reach another device: no remote copies, remote signals or barrier semaphores. Data moves between devices by JAX's collectives and lax.ppermute only.
A program may use at most 64 MiB of HBM per device.

```python
import math
import jax
import jax.numpy as jnp
from jax import lax

TILE = 128
HIST = 6
TILES_X = 1
TILES_Y = 2
TILES_Z = 2
BOX_X = 16
BOX_Y = 8
BOX_Z = 16


def draw_history(key, part):
    subkeys = jax.random.split(key, 6)
    full_shape = (6, BOX_X, BOX_Y, BOX_Z, TILE)
    block_counts = (BOX_X // TILES_X, BOX_Y // TILES_Y, BOX_Z // TILES_Z)
    frequency_table = jax.random.uniform(subkeys[4], block_counts, jnp.float32, 0.25, 2.2)
    index_x = jnp.arange(BOX_X) // TILES_X
    index_y = jnp.arange(BOX_Y) // TILES_Y
    index_z = jnp.arange(BOX_Z) // TILES_Z
    frequency = frequency_table[index_x[:, None, None], index_y[None, :, None], index_z[None, None, :]]
    step_index = jnp.arange(HIST, dtype=jnp.float32).reshape(HIST, 1, 1, 1, 1, 1)
    phase_angle = step_index * frequency[None, None, :, :, :, None]
    baseline = jax.random.normal(subkeys[0], full_shape, jnp.float32)
    cosine_part = jax.random.normal(subkeys[1], full_shape, jnp.float32)
    sine_part = jax.random.normal(subkeys[2], full_shape, jnp.float32)
    jitter = 0.2 * jax.random.normal(subkeys[3], (HIST,) + full_shape, jnp.float32)
    amplitude = jnp.exp(jax.random.uniform(subkeys[5], (1, 1, BOX_X, BOX_Y, BOX_Z, 1), jnp.float32, -0.7, 0.7))
    values = amplitude * (baseline[None] + jnp.cos(phase_angle) * cosine_part[None] + jnp.sin(phase_angle) * sine_part[None] + jitter)
    return jnp.clip(values, -12.0, 12.0).astype(jnp.float32)


def draw_pair_mask(key, part):
    coin_flips = jax.random.randint(key, (BOX_X, BOX_Y, BOX_Z, 27), 0, 4)
    one_side = (coin_flips > 0).astype(jnp.int32)
    columns = []
    for offset in range(27):
        along_x = offset // 9 - 1
        along_y = offset // 3 % 3 - 1
        along_z = offset % 3 - 1
        if offset == 13:
            columns.append(jnp.ones_like(one_side[..., offset]))
        else:
            mirror = jnp.roll(one_side[..., 26 - offset], shift=(-along_x, -along_y, -along_z), axis=(0, 1, 2))
            columns.append(one_side[..., offset] * mirror)
    return jnp.stack(columns, -1).astype(jnp.int32)


def with_ends(drawn, own_key, low, top_value):
    extent = drawn.shape
    index_at = [jax.random.randint(jax.random.fold_in(own_key, axis), (), 0, extent[axis]) for axis in range(len(extent))]
    drawn = drawn.at[tuple(index_at)].set(low)
    longest = extent.index(max(extent))
    index_at[longest] = (index_at[longest] + 1) % extent[longest]
    return drawn.at[tuple(index_at)].set(top_value)


def shard_levels(key, extent, cuts, least, high):
    loudness = 1.0
    for axis_at, blocks in cuts:
        draws = jax.random.uniform(jax.random.fold_in(jax.random.fold_in(key, 6), axis_at), (blocks,), jnp.float32, least / len(cuts), high / len(cuts))
        loudness = loudness * jnp.repeat(jnp.exp(draws), extent[axis_at] // blocks).reshape((-1,) + (1,) * (len(extent) - 1 - axis_at))
    return loudness


def scatter_about(key, dims, width, limit, pieces=(), held_as=jnp.bfloat16):
    result = jax.random.normal(key, dims, jnp.float32) * width
    if len(pieces) > 0:
        result = shard_levels(key, dims, pieces, -0.22, 0.18) * result
    return jnp.clip(result, min=-limit, max=limit).astype(held_as)


def setup_inputs(seed: int = 0) -> dict:
    key_of = jax.random.split(jax.random.key(seed), 7)
    fractions = jnp.clip(1.0 * jax.random.uniform(key_of[0], (3, BOX_X, BOX_Y, BOX_Z, TILE), jnp.float32) ** shard_levels(key_of[0], (3, BOX_X, BOX_Y, BOX_Z, TILE), ((1, 16), (2, 4), (3, 8)), -0.2, 0.2), 0.0, 1.0)
    polarizability = jnp.clip(jnp.exp(math.log(2.0) - 1.3862944 * jax.random.uniform(key_of[1], (BOX_X, BOX_Y, BOX_Z, TILE), jnp.float32) ** shard_levels(key_of[1], (BOX_X, BOX_Y, BOX_Z, TILE), ((0, 16), (1, 4), (2, 8)), -0.2, 0.2)), 0.5, 2.0)
    occupancy = with_ends((jax.random.randint(key_of[2], (BOX_X, BOX_Y, BOX_Z, TILE), 0, 8) < 7).astype(jnp.int32), jax.random.fold_in(key_of[2], 1), 0, 1)
    pair_mask = draw_pair_mask(jax.random.fold_in(key_of[6], 71), 0)
    perm_field = scatter_about(key_of[4], (6, BOX_X, BOX_Y, BOX_Z, TILE), 1.0, 6.0, ((1, 16), (2, 4), (3, 8)), jnp.float32)
    history = draw_history(jax.random.fold_in(key_of[6], 71), 0)
    return {"fractions": fractions, "polarizability": polarizability, "occupancy": occupancy, "pair_mask": pair_mask, "perm_field": perm_field, "history": history}


CELL_EDGE = 10.0
SOFTENING = 0.3
THOLE_DAMP = 0.39
RELAXATION = 0.7

def pair_field(target, source, moment, offset_vec, itself, allowed):
    displace = [(offset_vec[axis_num] + source[axis_num][:, None, :] - target[axis_num][:, :, None]) * CELL_EDGE for axis_num in range(3)]
    dist_sq = displace[0] * displace[0] + displace[1] * displace[1] + displace[2] * displace[2] + SOFTENING
    inv_cube = lax.rsqrt(dist_sq) / dist_sq
    thole_arg = dist_sq * jnp.sqrt(dist_sq) * lax.rsqrt(target[3][:, :, None] * source[3][:, None, :])
    damping = jnp.exp(-THOLE_DAMP * thole_arg)
    lambda_three = 1.0 - damping
    lambda_five = 1.0 - (1.0 + THOLE_DAMP * thole_arg) * damping
    slots = target.shape[-1]
    self_pair = jnp.logical_and(itself, jnp.eye(slots, dtype=bool))
    weight = jnp.where(self_pair, 0.0, allowed[:, None, None])
    radial = 3.0 * lambda_five * inv_cube / dist_sq * weight
    direct = lambda_three * inv_cube * weight
    fields = []
    for which_set in range(moment.shape[0] // 3):
        parts = [moment[3 * which_set + axis_num][:, None, :] for axis_num in range(3)]
        project = displace[0] * parts[0] + displace[1] * parts[1] + displace[2] * parts[2]
        for axis_num in range(3):
            fields.append(lax.optimization_barrier(jnp.sum(radial * project * displace[axis_num] - direct * parts[axis_num], axis=-1)))
    return jnp.stack(fields)

def slab_field(geometry_pad, moment_pad, allowed_slab, slab_index):
    width_y = geometry_pad.shape[2] - 2
    width_z = geometry_pad.shape[3] - 2
    slots = geometry_pad.shape[4]
    rows = moment_pad.shape[0]
    zero = jnp.zeros((), jnp.int32)
    one = jnp.ones((), jnp.int32)
    first_x = (jnp.asarray(slab_index) + 1).astype(jnp.int32)
    target = lax.dynamic_slice(geometry_pad, (zero, first_x, one, one, zero), (4, 1, width_y, width_z, slots)).reshape(4, width_y * width_z, slots)

    def offset_step(offset, summed):
        offset = jnp.asarray(offset).astype(jnp.int32)
        along_x = offset // 9 - 1
        along_y = offset // 3 % 3 - 1
        along_z = offset % 3 - 1
        starts = (zero, first_x + along_x, one + along_y, one + along_z, zero)
        source = lax.dynamic_slice(geometry_pad, starts, (4, 1, width_y, width_z, slots)).reshape(4, width_y * width_z, slots)
        moment = lax.dynamic_slice(moment_pad, starts, (rows, 1, width_y, width_z, slots)).reshape(rows, width_y * width_z, slots)
        allowed = lax.dynamic_index_in_dim(allowed_slab, offset, 2, keepdims=False).reshape(-1).astype(jnp.float32)
        offset_vec = jnp.stack([along_x, along_y, along_z]).astype(jnp.float32)
        return summed + pair_field(target, source, moment, offset_vec, offset == 13, allowed)
    summed = lax.fori_loop(0, 27, offset_step, jnp.zeros((rows, width_y * width_z, slots), jnp.float32))
    return summed.reshape(rows, width_y, width_z, slots)

def wrap_pad(values):
    return jnp.pad(values, ((0, 0), (1, 1), (1, 1), (1, 1), (0, 0)), mode='wrap')

def box_field(geometry_pad, moment, pair_mask):
    moment_pad = wrap_pad(moment)

    def one_slab(slab_index):
        allowed_slab = lax.dynamic_index_in_dim(pair_mask, slab_index, 0, keepdims=False)
        return slab_field(geometry_pad, moment_pad, allowed_slab, slab_index)
    slabs = lax.map(one_slab, jnp.arange(pair_mask.shape[0], dtype=jnp.int32))
    return jnp.moveaxis(slabs, 0, 1)

def fit_coefficients(gram_matrix):
    past_count = gram_matrix.shape[0] - 1
    gram_past = gram_matrix[:past_count, :past_count]
    gram_next = gram_matrix[:past_count, past_count]
    ridge_term = 0.001 * jnp.trace(gram_past) / past_count + 1.0
    factor = jnp.linalg.cholesky(gram_past + ridge_term * jnp.eye(past_count, dtype=jnp.float32))
    return jax.scipy.linalg.cho_solve((factor, True), gram_next)

def reference(fractions, polarizability, occupancy, pair_mask, perm_field, history):
    filled = occupancy.astype(jnp.float32)
    geometry = jnp.concatenate([fractions, polarizability[None]], 0)
    masked = history * filled
    flat_hist = masked.reshape(masked.shape[0], -1)
    gram_matrix = jnp.dot(flat_hist, flat_hist.T, precision=lax.Precision.HIGHEST)
    coeffs = fit_coefficients(gram_matrix)
    predicted = jnp.tensordot(coeffs, masked[1:], axes=1, precision=lax.Precision.HIGHEST)
    geometry_pad = wrap_pad(geometry)
    scaled = RELAXATION * filled * polarizability
    field_one = box_field(geometry_pad, predicted, pair_mask)
    dipole_one = (1.0 - RELAXATION) * predicted + scaled * (perm_field + field_one)
    field_two = box_field(geometry_pad, dipole_one, pair_mask)
    induced = (1.0 - RELAXATION) * dipole_one + scaled * (perm_field + field_two)
    update = induced - dipole_one
    change = jnp.sqrt(jnp.sum(update * update) / (jnp.sum(induced * induced) + 1.0))
    return (induced, change)
```

```python
import functools

import jax
import jax.numpy as jnp
from jax import lax
from jax.experimental import pallas as pl
from jax.experimental.pallas import tpu as pltpu

ALL = ("gx", "gy", "gz")
CELL_EDGE = 10.0
SOFTENING = 0.3
THOLE_DAMP = 0.39
RELAXATION = 0.7
LN2 = 0.6931471805599453

SLOTS = 128
NX, NY, NZ = 3, 4, 4
TILES = NX * NY * NZ
OWN = 4
OFFSETS = 27
TERMS = 48
A_ROWS = 96
B_ROWS = 24
BATCH = 8
PAIRS = OWN + OWN * (OFFSETS - 1)
GRAM = tuple((a, b) for a in range(6) for b in range(a + 1))


def source_tile(tile, offset):
    x = offset // 9
    y = tile // 2 + offset // 3 % 3
    z = tile % 2 + offset % 3
    return (x * NY + y) * NZ + z


OWN_TILES = tuple(source_tile(t, 13) for t in range(OWN))


def split3(value):
    high = value.astype(jnp.bfloat16).astype(jnp.float32)
    rest = value - high
    middle = rest.astype(jnp.bfloat16).astype(jnp.float32)
    return high, middle, rest - middle


def positions(geo):
    tile = lax.broadcasted_iota(jnp.int32, (TILES, SLOTS), 0)
    x = (tile // (NY * NZ)).astype(jnp.float32)
    y = (tile // NZ % NY).astype(jnp.float32)
    z = (tile % NZ).astype(jnp.float32)
    return (
        (geo[0] + (x - 1.5)) * CELL_EDGE,
        (geo[1] + (y - 2.0)) * CELL_EDGE,
        (geo[2] + (z - 2.0)) * CELL_EDGE,
    )


def scale_of(polar):
    factor = (THOLE_DAMP / LN2) ** (1.0 / 3.0)
    return factor * jnp.exp(jnp.log(polar) * (-1.0 / 3.0))


def own_rows(value):
    return [value[t : t + 1] for t in OWN_TILES]


def pair_kernel(mask_ref, geo_ref, list_ref, count_ref, pair_ref, q_ref, qt_ref, p_ref):
    geo = [geo_ref[a] for a in range(4)]
    r = positions(geo)
    a = scale_of(geo[3])
    norm = r[0] * r[0] + r[1] * r[1] + r[2] * r[2]
    sources = [a, a * (norm + SOFTENING), a * r[0], a * r[1], a * r[2]]
    targets = [a * norm, a, -2.0 * a * r[0], -2.0 * a * r[1], -2.0 * a * r[2]]
    row = 0
    for source, target in zip(sources, targets):
        source_parts = split3(source)
        target_parts = split3(target)
        for s in range(3):
            for t in range(3):
                q_ref[0:TILES, row, :] = source_parts[s]
                for own in range(OWN):
                    p_ref[own, row : row + 1, :] = target_parts[t][
                        OWN_TILES[own] : OWN_TILES[own] + 1
                    ]
                row += 1
    zero = jnp.zeros((TILES, SLOTS), jnp.float32)
    for rest in range(row, TERMS):
        q_ref[0:TILES, rest, :] = zero
        for own in range(OWN):
            p_ref[own, rest : rest + 1, :] = zero[0:1]

    def flip(n, carry):
        qt_ref[n] = q_ref[n].T.astype(jnp.bfloat16)
        return carry

    lax.fori_loop(0, TILES, flip, 0)
    qt_ref[TILES] = qt_ref[0]

    count = jnp.int32(OWN)
    for t in range(OWN):
        list_ref[t] = OWN_TILES[t] * OWN + t
    for t in range(OWN):
        for k in range(OFFSETS):
            if k == 13:
                continue
            list_ref[count] = source_tile(t, k) * OWN + t
            count = count + (mask_ref[t * OFFSETS + k] != 0).astype(jnp.int32)
    for extra in range(BATCH):
        list_ref[count + extra] = TILES * OWN
    count_ref[0] = count

    def pair(slot, keep):
        entry = list_ref[slot]
        n = entry // OWN
        t = entry % OWN
        dist = jnp.dot(
            qt_ref[n], p_ref[t].astype(jnp.bfloat16), preferred_element_type=jnp.float32
        )
        inv = lax.rsqrt(dist)
        arg = dist * (dist * inv)
        damp = jnp.exp2(-arg)
        inv2 = inv * inv
        direct = (1.0 - damp) * (inv2 * inv)
        radial = inv2 * (direct - LN2 * damp)
        if keep is not None:
            direct = jnp.where(keep, direct, 0.0)
            radial = jnp.where(keep, radial, 0.0)
        for part, value in enumerate((radial, direct)):
            high = value.astype(jnp.bfloat16)
            low = (value - high.astype(jnp.float32)).astype(jnp.bfloat16)
            base = part * 2 * SLOTS
            pair_ref[slot, base : base + SLOTS, :] = high
            pair_ref[slot, base + SLOTS : base + 2 * SLOTS, :] = low

    keep = lax.broadcasted_iota(jnp.int32, (SLOTS, SLOTS), 0) != lax.broadcasted_iota(
        jnp.int32, (SLOTS, SLOTS), 1
    )
    for slot in range(OWN):
        pair(slot, keep)

    def batch(b, carry):
        for u in range(BATCH):
            pair(OWN + b * BATCH + u, None)
        return carry

    lax.fori_loop(0, (count - OWN + BATCH - 1) // BATCH, batch, 0)


def build_pairs(mask, geo):
    return pl.pallas_call(
        pair_kernel,
        name="build_pairs",
        in_specs=[
            pl.BlockSpec(memory_space=pltpu.SMEM),
            pl.BlockSpec(memory_space=pltpu.VMEM),
        ],
        out_specs=[
            pl.BlockSpec(memory_space=pltpu.SMEM),
            pl.BlockSpec(memory_space=pltpu.SMEM),
            pl.BlockSpec(memory_space=pltpu.VMEM),
        ],
        out_shape=[
            jax.ShapeDtypeStruct((PAIRS + BATCH,), jnp.int32),
            jax.ShapeDtypeStruct((1,), jnp.int32),
            jax.ShapeDtypeStruct((PAIRS, 4 * SLOTS, SLOTS), jnp.bfloat16),
        ],
        scratch_shapes=[
            pltpu.VMEM((TILES, TERMS, SLOTS), jnp.float32),
            pltpu.VMEM((TILES + 1, SLOTS, TERMS), jnp.bfloat16),
            pltpu.VMEM((OWN, TERMS, SLOTS), jnp.float32),
        ],
        compiler_params=pltpu.CompilerParams(vmem_limit_bytes=24 * 1024 * 1024),
    )(mask, geo)


def apply_pairs(list_ref, count_ref, geo_ref, pair_ref, moment, a_ref, b_ref, sum_a, sum_b):
    geo = [geo_ref[a] for a in range(4)]
    r = positions(geo)
    a = scale_of(geo[3])
    root = jnp.sqrt(a)
    scale_b = a * root
    scale_a = scale_b * a
    for kind in range(2):
        m = [moment[3 * kind + c] * scale_a for c in range(3)]
        g = r[0] * m[0] + r[1] * m[1] + r[2] * m[2]
        values = [g] + [r[c] * g for c in range(3)] + m
        values += [r[c] * m[d] for c in range(3) for d in range(3)]
        for index, value in enumerate(values):
            for s, part in enumerate(split3(value)):
                a_ref[0:TILES, 32 * s + 16 * kind + index, :] = part
    for c in range(6):
        for s, part in enumerate(split3(moment[c] * scale_b)):
            b_ref[0:TILES, 8 * s + c, :] = part
    zero = jnp.zeros((TILES, SLOTS), jnp.float32)
    for s in range(3):
        for c in (6, 7):
            b_ref[0:TILES, 8 * s + c, :] = zero
    a_ref[TILES] = jnp.zeros((A_ROWS, SLOTS), jnp.float32)
    b_ref[TILES] = jnp.zeros((B_ROWS, SLOTS), jnp.float32)

    def product(slot):
        entry = list_ref[slot]
        n = entry // OWN
        left = a_ref[n].astype(jnp.bfloat16)
        part_a = jnp.dot(
            jnp.concatenate([left, left], axis=1),
            pair_ref[slot, 0 : 2 * SLOTS, :],
            preferred_element_type=jnp.float32,
        )
        left = b_ref[n].astype(jnp.bfloat16)
        part_b = jnp.dot(
            jnp.concatenate([left, left], axis=1),
            pair_ref[slot, 2 * SLOTS : 4 * SLOTS, :],
            preferred_element_type=jnp.float32,
        )
        return entry % OWN, part_a, part_b

    for slot in range(OWN):
        t, part_a, part_b = product(slot)
        sum_a[slot] = part_a
        sum_b[slot] = part_b

    def batch(b, carry):
        for u in range(BATCH):
            t, part_a, part_b = product(OWN + b * BATCH + u)
            sum_a[t] += part_a
            sum_b[t] += part_b
        return carry

    lax.fori_loop(0, (count_ref[0] - OWN + BATCH - 1) // BATCH, batch, 0)

    own_r = [jnp.concatenate(own_rows(r[c]), 0) for c in range(3)]
    own_a = 3.0 * jnp.concatenate(own_rows(scale_a), 0)
    own_b = jnp.concatenate(own_rows(scale_b), 0)

    def total_a(kind, index):
        row = 16 * kind + index
        return sum_a[:, row, :] + sum_a[:, 32 + row, :] + sum_a[:, 64 + row, :]

    def total_b(row):
        return sum_b[:, row, :] + sum_b[:, 8 + row, :] + sum_b[:, 16 + row, :]

    fields = []
    for kind in range(2):
        g = total_a(kind, 0)
        m = [total_a(kind, 4 + c) for c in range(3)]
        dot = own_r[0] * m[0] + own_r[1] * m[1] + own_r[2] * m[2] - g
        for c in range(3):
            cross = sum(own_r[d] * total_a(kind, 7 + 3 * c + d) for d in range(3))
            radial = total_a(kind, 1 + c) - cross + own_r[c] * dot
            fields.append(own_a * radial - own_b * total_b(3 * kind + c))
    return fields


def own_part(value):
    return jnp.concatenate(own_rows(value), 0)


def solve(gram):
    count = 5
    matrix = [[gram[max(a, b), min(a, b)] for b in range(count)] for a in range(count)]
    right = [gram[count, a] for a in range(count)]
    trace = matrix[0][0]
    for a in range(1, count):
        trace = trace + matrix[a][a]
    ridge = 0.001 * trace / count + 1.0
    for a in range(count):
        matrix[a][a] = matrix[a][a] + ridge
    for c in range(count):
        for a in range(c + 1, count):
            ratio = matrix[a][c] / matrix[c][c]
            for b in range(c + 1, a + 1):
                matrix[a][b] = matrix[a][b] - ratio * matrix[b][c]
            right[a] = right[a] - ratio * right[c]
    result = [None] * count
    for a in reversed(range(count)):
        rest = right[a]
        for b in range(a + 1, count):
            rest = rest - matrix[b][a] * result[b]
        result[a] = rest / matrix[a][a]
    return result


def gram_kernel(history_ref, occupancy_ref, out_ref):
    filled = occupancy_ref[...].astype(jnp.float32)
    masked = [
        [history_ref[h, c] * filled for c in range(6)] for h in range(6)
    ]
    lane = lax.broadcasted_iota(jnp.int32, (1, SLOTS), 1)
    row = jnp.zeros((1, SLOTS), jnp.float32)
    for index, (a, b) in enumerate(GRAM):
        product = masked[a][0] * masked[b][0]
        for c in range(1, 6):
            product = product + masked[a][c] * masked[b][c]
        total = jnp.sum(jnp.sum(product, axis=0, keepdims=True), axis=1, keepdims=True)
        row = jnp.where(lane == index, total, row)
    out_ref[...] = jnp.broadcast_to(row[None], out_ref.shape)


def vmem_spec():
    return pl.BlockSpec(memory_space=pltpu.VMEM)


def smem_spec():
    return pl.BlockSpec(memory_space=pltpu.SMEM)


def local_gram(history, occupancy, copies):
    return pl.pallas_call(
        gram_kernel,
        name="local_gram",
        in_specs=[vmem_spec(), vmem_spec()],
        out_specs=vmem_spec(),
        out_shape=jax.ShapeDtypeStruct((copies, 1, SLOTS), jnp.float32),
    )(history, occupancy)


def sum_kernel(parts_ref, out_ref):
    total = jnp.sum(parts_ref[...], axis=0, keepdims=True)
    out_ref[...] = jnp.broadcast_to(total, out_ref.shape)


def sum_parts(parts, copies):
    return pl.pallas_call(
        sum_kernel,
        name="sum_parts",
        in_specs=[vmem_spec()],
        out_specs=vmem_spec(),
        out_shape=jax.ShapeDtypeStruct((copies, 1, SLOTS), jnp.float32),
    )(parts)


SCRATCH = [
    pltpu.VMEM((TILES + 1, A_ROWS, SLOTS), jnp.float32),
    pltpu.VMEM((TILES + 1, B_ROWS, SLOTS), jnp.float32),
    pltpu.VMEM((OWN, A_ROWS, SLOTS), jnp.float32),
    pltpu.VMEM((OWN, B_ROWS, SLOTS), jnp.float32),
]


def first_kernel(
    list_ref, count_ref, gram_ref, geo_ref, later_ref, occupancy_ref, perm_ref, pair_ref,
    out_ref, a_ref, b_ref, sum_a, sum_b,
):
    total = jnp.sum(gram_ref[...], axis=0)
    gram = {ab: total[0:1, i : i + 1] for i, ab in enumerate(GRAM)}
    coeffs = solve(gram)
    moment = []
    for c in range(6):
        value = coeffs[0] * later_ref[c]
        for h in range(1, 5):
            value = value + coeffs[h] * later_ref[6 * h + c]
        moment.append(value)
    fields = apply_pairs(
        list_ref, count_ref, geo_ref, pair_ref, moment, a_ref, b_ref, sum_a, sum_b
    )
    scaled = RELAXATION * occupancy_ref[...].astype(jnp.float32) * own_part(geo_ref[3])
    for c in range(6):
        out_ref[c] = (1.0 - RELAXATION) * own_part(moment[c]) + scaled * (
            perm_ref[c] + fields[c]
        )


def second_kernel(
    list_ref, count_ref, geo_ref, dipole_ref, occupancy_ref, perm_ref, pair_ref,
    out_ref, size_ref, a_ref, b_ref, sum_a, sum_b,
):
    moment = [dipole_ref[c] for c in range(6)]
    fields = apply_pairs(
        list_ref, count_ref, geo_ref, pair_ref, moment, a_ref, b_ref, sum_a, sum_b
    )
    scaled = RELAXATION * occupancy_ref[...].astype(jnp.float32) * own_part(geo_ref[3])
    moved = jnp.zeros((OWN, SLOTS), jnp.float32)
    size = jnp.zeros((OWN, SLOTS), jnp.float32)
    for c in range(6):
        old = own_part(moment[c])
        new = (1.0 - RELAXATION) * old + scaled * (perm_ref[c] + fields[c])
        out_ref[c] = new
        moved = moved + (new - old) * (new - old)
        size = size + new * new
    lane = lax.broadcasted_iota(jnp.int32, (1, SLOTS), 1)
    row = jnp.zeros((1, SLOTS), jnp.float32)
    for index, value in enumerate((moved, size)):
        total = jnp.sum(jnp.sum(value, axis=0, keepdims=True), axis=1, keepdims=True)
        row = jnp.where(lane == index, total, row)
    size_ref[...] = jnp.broadcast_to(row[None], size_ref.shape)


FIELD_PARAMS = pltpu.CompilerParams(vmem_limit_bytes=24 * 1024 * 1024)


def first_field(pair_list, count, gram, geo, later, occupancy, perm, pairs):
    return pl.pallas_call(
        first_kernel,
        name="first_field",
        in_specs=[smem_spec(), smem_spec()] + [vmem_spec()] * 6,
        out_specs=vmem_spec(),
        out_shape=jax.ShapeDtypeStruct((6, OWN, SLOTS), jnp.float32),
        scratch_shapes=SCRATCH,
        compiler_params=FIELD_PARAMS,
    )(pair_list, count, gram, geo, later, occupancy, perm, pairs)


def second_field(pair_list, count, geo, dipoles, occupancy, perm, pairs, copies):
    return pl.pallas_call(
        second_kernel,
        name="second_field",
        in_specs=[smem_spec(), smem_spec()] + [vmem_spec()] * 5,
        out_specs=[vmem_spec(), vmem_spec()],
        out_shape=[
            jax.ShapeDtypeStruct((6, OWN, SLOTS), jnp.float32),
            jax.ShapeDtypeStruct((copies, 1, SLOTS), jnp.float32),
        ],
        scratch_shapes=SCRATCH,
        compiler_params=FIELD_PARAMS,
    )(pair_list, count, geo, dipoles, occupancy, perm, pairs)


def with_halo(cells, sides):
    for axis, dim in sides:
        count = lax.axis_size(axis)
        head = lax.slice_in_dim(cells, 0, 1, axis=dim)
        tail = lax.slice_in_dim(cells, cells.shape[dim] - 1, cells.shape[dim], axis=dim)
        cells = jnp.concatenate(
            [
                lax.ppermute(tail, axis, [(i, (i + 1) % count) for i in range(count)]),
                cells,
                lax.ppermute(head, axis, [((i + 1) % count, i) for i in range(count)]),
            ],
            axis=dim,
        )
    return cells


SIDES = (("gx", 1), ("gy", 2), ("gz", 3))


def exchange(parts, axes):
    return lax.all_to_all(parts, axes, 0, 0)


def on_device(fractions, polarizability, occupancy, pair_mask, perm_field, history):
    plane = lax.axis_size("gy") * lax.axis_size("gz")
    line = lax.axis_size("gx")
    history = history.reshape(6, 6, OWN, SLOTS)
    occupancy = occupancy.reshape(OWN, SLOTS)
    perm = perm_field.reshape(6, OWN, SLOTS)

    filled = occupancy.astype(jnp.float32)
    later = (history[1:] * filled).reshape(30, 1, 2, 2, SLOTS)
    stacked = jnp.concatenate([fractions, polarizability[None], later], 0)
    ghosts = with_halo(stacked, SIDES)

    gram = exchange(local_gram(history, occupancy, plane), ("gy", "gz"))
    gram = exchange(sum_parts(gram, line), "gx")

    geo = ghosts[:4].reshape(4, TILES, SLOTS)
    later = ghosts[4:].reshape(30, TILES, SLOTS)
    pair_list, count, pairs = build_pairs(pair_mask.reshape(-1), geo)
    dipoles = first_field(pair_list, count, gram, geo, later, occupancy, perm, pairs)
    dipoles = with_halo(dipoles.reshape(6, 1, 2, 2, SLOTS), SIDES).reshape(6, TILES, SLOTS)
    induced, sizes = second_field(
        pair_list, count, geo, dipoles, occupancy, perm, pairs, plane
    )
    sizes = exchange(sizes, ("gy", "gz"))
    sizes = exchange(sum_parts(sizes, line), "gx")
    totals = jnp.sum(sizes, axis=(0, 1))
    change = jnp.sqrt(totals[0] / (totals[1] + 1.0))
    return induced.reshape(6, 1, 2, 2, SLOTS), change


def solution(mesh):
    from jax.sharding import PartitionSpec as P

    tiles = P("gx", "gy", "gz", None)
    sets = P(None, "gx", "gy", "gz", None)
    return jax.shard_map(
        on_device,
        mesh=mesh,
        in_specs=(
            sets,
            tiles,
            tiles,
            tiles,
            sets,
            P(None, None, "gx", "gy", "gz", None),
        ),
        out_specs=(sets, P()),
        check_vma=False,
    )
```

```python
import functools

import jax
import jax.numpy as jnp
from jax import lax
from jax.experimental import pallas as pl
from jax.experimental.pallas import tpu as pltpu

ALL = ("gx", "gy", "gz")
CELL_EDGE = 10.0
SOFTENING = 0.3
THOLE_DAMP = 0.39
RELAXATION = 0.7
LN2 = 0.6931471805599453

SLOTS = 128
NX, NY, NZ = 3, 4, 4
TILES = NX * NY * NZ
OWN = 4
OFFSETS = 27
TERMS = 48
A_ROWS = 96
B_ROWS = 24
BATCH = 8
PAIRS = OWN + OWN * (OFFSETS - 1)
LIST = 128
COUNT_AT = LIST - 1
GRAM = tuple((a, b) for a in range(6) for b in range(a + 1))


def source_tile(tile, offset):
    x = offset // 9
    y = tile // 2 + offset // 3 % 3
    z = tile % 2 + offset % 3
    return (x * NY + y) * NZ + z


OWN_TILES = tuple(source_tile(t, 13) for t in range(OWN))


def split3(value):
    high = value.astype(jnp.bfloat16).astype(jnp.float32)
    rest = value - high
    middle = rest.astype(jnp.bfloat16).astype(jnp.float32)
    return high, middle, rest - middle


def positions(geo):
    tile = lax.broadcasted_iota(jnp.int32, (TILES, SLOTS), 0)
    x = (tile // (NY * NZ)).astype(jnp.float32)
    y = (tile // NZ % NY).astype(jnp.float32)
    z = (tile % NZ).astype(jnp.float32)
    return (
        (geo[0] + (x - 1.5)) * CELL_EDGE,
        (geo[1] + (y - 2.0)) * CELL_EDGE,
        (geo[2] + (z - 2.0)) * CELL_EDGE,
    )


def scale_of(polar):
    factor = (THOLE_DAMP / LN2) ** (1.0 / 3.0)
    return factor * jnp.exp(jnp.log(polar) * (-1.0 / 3.0))


def own_rows(value):
    return [value[t : t + 1] for t in OWN_TILES]


def prepare_distances(geo, q_ref, p_ref):
    r = positions(geo)
    a = scale_of(geo[3])
    norm = r[0] * r[0] + r[1] * r[1] + r[2] * r[2]
    sources = [a, a * (norm + SOFTENING), a * r[0], a * r[1], a * r[2]]
    targets = [a * norm, a, -2.0 * a * r[0], -2.0 * a * r[1], -2.0 * a * r[2]]
    row = 0
    for source, target in zip(sources, targets):
        source_parts = split3(source)
        target_parts = split3(target)
        for s in range(3):
            for t in range(3):
                q_ref[pl.ds(row, TILES, stride=TERMS + 1), :] = source_parts[s]
                for own in range(OWN):
                    p_ref[own, row : row + 1, :] = target_parts[t][
                        OWN_TILES[own] : OWN_TILES[own] + 1
                    ]
                row += 1
    zero = jnp.zeros((TILES, SLOTS), jnp.float32)
    for rest in range(row, TERMS):
        q_ref[pl.ds(rest, TILES, stride=TERMS + 1), :] = zero
        for own in range(OWN):
            p_ref[own, rest : rest + 1, :] = zero[0:1]

    q_ref[TILES * (TERMS + 1) : TILES * (TERMS + 1) + TERMS, :] = q_ref[0:TERMS, :]


def list_pairs(mask_ref, list_ref):
    count = jnp.int32(OWN)
    for t in range(OWN):
        list_ref[t] = OWN_TILES[t] * OWN + t
    for t in range(OWN):
        for k in range(OFFSETS):
            if k == 13:
                continue
            list_ref[count] = source_tile(t, k) * OWN + t
            count = count + (mask_ref[t, k] != 0).astype(jnp.int32)
    for extra in range(BATCH):
        list_ref[count + extra] = TILES * OWN
    list_ref[COUNT_AT] = count
    return count


def pair_functions(n, t, q_ref, p_ref, keep):
    dist = lax.dot_general(
        q_ref[pl.ds(n * (TERMS + 1), TERMS), :].astype(jnp.bfloat16),
        p_ref[t].astype(jnp.bfloat16),
        (((0,), (0,)), ((), ())),
        preferred_element_type=jnp.float32,
    )
    inv = lax.rsqrt(dist)
    arg = dist * (dist * inv)
    damp = jnp.exp2(-arg)
    inv2 = inv * inv
    direct = (1.0 - damp) * (inv2 * inv)
    radial = inv2 * (direct - LN2 * damp)
    if keep is not None:
        direct = jnp.where(keep, direct, 0.0)
        radial = jnp.where(keep, radial, 0.0)
    result = []
    for value in (radial, direct):
        high = value.astype(jnp.bfloat16)
        low = (value - high.astype(jnp.float32)).astype(jnp.bfloat16)
        result.append(jnp.concatenate([high, low], axis=0))
    return result


def prepare_moments(geo, moment, a_ref, b_ref):
    r = positions(geo)
    scale_a, scale_b = factors(geo)
    zero = jnp.zeros((TILES, SLOTS), jnp.float32)
    for kind in range(2):
        m = [moment[3 * kind + c] * scale_a for c in range(3)]
        outer = [r[c] * m[d] for c in range(3) for d in range(3)]
        g = outer[0] + outer[4] + outer[8]
        values = [None] + [r[c] * g for c in range(3)] + m + outer
        for index, value in enumerate(values):
            parts = (zero, zero, zero) if value is None else split3(value)
            for s, part in enumerate(parts):
                row = 32 * s + 16 * kind + index
                a_ref[pl.ds(row, TILES, stride=A_ROWS + 1), :] = part
    for c in range(8):
        parts = (zero, zero, zero) if c >= 6 else split3(moment[c] * scale_b)
        for s, part in enumerate(parts):
            b_ref[pl.ds(8 * s + c, TILES, stride=B_ROWS + 1), :] = part
    a_ref[TILES * (A_ROWS + 1) : TILES * (A_ROWS + 1) + A_ROWS, :] = jnp.zeros((A_ROWS, SLOTS), jnp.float32)
    b_ref[TILES * (B_ROWS + 1) : TILES * (B_ROWS + 1) + B_ROWS, :] = jnp.zeros((B_ROWS, SLOTS), jnp.float32)


def factors(geo):
    a = scale_of(geo[3])
    scale_b = a * jnp.sqrt(a)
    return scale_b * a, scale_b


def product(n, radial, direct, a_ref, b_ref):
    left = a_ref[pl.ds(n * (A_ROWS + 1), A_ROWS), :].astype(jnp.bfloat16)
    part_a = jnp.dot(
        jnp.concatenate([left, left], axis=1), radial, preferred_element_type=jnp.float32
    )
    left = b_ref[pl.ds(n * (B_ROWS + 1), B_ROWS), :].astype(jnp.bfloat16)
    part_b = jnp.dot(
        jnp.concatenate([left, left], axis=1), direct, preferred_element_type=jnp.float32
    )
    return part_a, part_b


def field_of(geo, sum_a, sum_b):
    r = positions(geo)
    scale_a, scale_b = factors(geo)
    own_r = [jnp.concatenate(own_rows(r[c]), 0) for c in range(3)]
    own_a = 3.0 * jnp.concatenate(own_rows(scale_a), 0)
    own_b = jnp.concatenate(own_rows(scale_b), 0)

    def total_a(kind, index):
        row = 16 * kind + index
        return sum_a[:, row, :] + sum_a[:, 32 + row, :] + sum_a[:, 64 + row, :]

    def total_b(row):
        return sum_b[:, row, :] + sum_b[:, 8 + row, :] + sum_b[:, 16 + row, :]

    fields = []
    for kind in range(2):
        outer = [[total_a(kind, 7 + 3 * c + d) for d in range(3)] for c in range(3)]
        g = outer[0][0] + outer[1][1] + outer[2][2]
        m = [total_a(kind, 4 + c) for c in range(3)]
        dot = own_r[0] * m[0] + own_r[1] * m[1] + own_r[2] * m[2] - g
        for c in range(3):
            cross = sum(own_r[d] * outer[c][d] for d in range(3))
            radial = total_a(kind, 1 + c) - cross + own_r[c] * dot
            fields.append(own_a * radial - own_b * total_b(3 * kind + c))
    return fields


def own_part(value):
    return jnp.concatenate(own_rows(value), 0)


def solve(gram):
    count = 5
    matrix = [[gram[max(a, b), min(a, b)] for b in range(count)] for a in range(count)]
    right = [gram[count, a] for a in range(count)]
    trace = matrix[0][0]
    for a in range(1, count):
        trace = trace + matrix[a][a]
    ridge = 0.001 * trace / count + 1.0
    for a in range(count):
        matrix[a][a] = matrix[a][a] + ridge
    for c in range(count):
        for a in range(c + 1, count):
            ratio = matrix[a][c] / matrix[c][c]
            for b in range(c + 1, a + 1):
                matrix[a][b] = matrix[a][b] - ratio * matrix[b][c]
            right[a] = right[a] - ratio * right[c]
    result = [None] * count
    for a in reversed(range(count)):
        rest = right[a]
        for b in range(a + 1, count):
            rest = rest - matrix[b][a] * result[b]
        result[a] = rest / matrix[a][a]
    return result


def gram_kernel(history_ref, occupancy_ref, out_ref):
    filled = occupancy_ref[...].astype(jnp.float32)
    masked = [
        [history_ref[h, c] * filled for c in range(6)] for h in range(6)
    ]
    lane = lax.broadcasted_iota(jnp.int32, (1, SLOTS), 1)
    row = jnp.zeros((1, SLOTS), jnp.float32)
    for index, (a, b) in enumerate(GRAM):
        product = masked[a][0] * masked[b][0]
        for c in range(1, 6):
            product = product + masked[a][c] * masked[b][c]
        total = jnp.sum(jnp.sum(product, axis=0, keepdims=True), axis=1, keepdims=True)
        row = jnp.where(lane == index, total, row)
    out_ref[...] = jnp.broadcast_to(row[None], out_ref.shape)


def vmem_spec():
    return pl.BlockSpec(memory_space=pltpu.VMEM)


def smem_spec():
    return pl.BlockSpec(memory_space=pltpu.SMEM)


def local_gram(history, occupancy, copies):
    return pl.pallas_call(
        gram_kernel,
        name="local_gram",
        in_specs=[vmem_spec(), vmem_spec()],
        out_specs=vmem_spec(),
        out_shape=jax.ShapeDtypeStruct((copies, 1, SLOTS), jnp.float32),
    )(history, occupancy)


def sum_parts(parts, copies):
    total = jnp.sum(parts, axis=0, keepdims=True)
    return jnp.broadcast_to(total, (copies,) + total.shape[1:])


SCRATCH = [
    pltpu.VMEM(((TILES + 1) * (A_ROWS + 1), SLOTS), jnp.float32),
    pltpu.VMEM(((TILES + 1) * (B_ROWS + 1), SLOTS), jnp.float32),
    pltpu.VMEM((OWN, A_ROWS, SLOTS), jnp.float32),
    pltpu.VMEM((OWN, B_ROWS, SLOTS), jnp.float32),
]


def first_kernel(
    mask_ref, gram_ref, geo_ref, later_ref, occupancy_ref, perm_ref,
    out_ref, list_ref, pair_ref, q_ref, p_ref, a_ref, b_ref, sum_a, sum_b,
):
    geo = [geo_ref[a] for a in range(4)]
    total = jnp.sum(gram_ref[...], axis=0)
    gram = {ab: total[0:1, i : i + 1] for i, ab in enumerate(GRAM)}
    coeffs = solve(gram)
    moment = []
    for c in range(6):
        value = coeffs[0] * later_ref[c]
        for h in range(1, 5):
            value = value + coeffs[h] * later_ref[6 * h + c]
        moment.append(value)
    prepare_distances(geo, q_ref, p_ref)
    prepare_moments(geo, moment, a_ref, b_ref)
    count = list_pairs(mask_ref, list_ref)

    def pair(slot, n, t, keep):
        radial, direct = pair_functions(n, t, q_ref, p_ref, keep)
        pair_ref[slot, 0 : 2 * SLOTS, :] = radial
        pair_ref[slot, 2 * SLOTS : 4 * SLOTS, :] = direct
        return product(n, radial, direct, a_ref, b_ref)

    keep = lax.broadcasted_iota(jnp.int32, (SLOTS, SLOTS), 0) != lax.broadcasted_iota(
        jnp.int32, (SLOTS, SLOTS), 1
    )
    for slot in range(OWN):
        sum_a[slot], sum_b[slot] = pair(slot, OWN_TILES[slot], slot, keep)

    def batch(b, carry):
        for u in range(BATCH):
            slot = OWN + b * BATCH + u
            entry = list_ref[slot]
            t = entry % OWN
            part_a, part_b = pair(slot, entry // OWN, t, None)
            sum_a[t] += part_a
            sum_b[t] += part_b
        return carry

    lax.fori_loop(0, (count - OWN + BATCH - 1) // BATCH, batch, 0)
    fields = field_of(geo, sum_a, sum_b)
    scaled = RELAXATION * occupancy_ref[...].astype(jnp.float32) * own_part(geo[3])
    for c in range(6):
        out_ref[c] = (1.0 - RELAXATION) * own_part(moment[c]) + scaled * (
            perm_ref[c] + fields[c]
        )


def second_kernel(
    list_ref, geo_ref, dipole_ref, occupancy_ref, perm_ref, pair_ref,
    out_ref, size_ref, a_ref, b_ref, sum_a, sum_b,
):
    geo = [geo_ref[a] for a in range(4)]
    moment = [dipole_ref[c] for c in range(6)]
    prepare_moments(geo, moment, a_ref, b_ref)

    def pair(slot, n):
        return product(
            n,
            pair_ref[slot, 0 : 2 * SLOTS, :],
            pair_ref[slot, 2 * SLOTS : 4 * SLOTS, :],
            a_ref,
            b_ref,
        )

    for slot in range(OWN):
        sum_a[slot], sum_b[slot] = pair(slot, OWN_TILES[slot])

    def batch(b, carry):
        for u in range(BATCH):
            slot = OWN + b * BATCH + u
            entry = list_ref[slot]
            t = entry % OWN
            part_a, part_b = pair(slot, entry // OWN)
            sum_a[t] += part_a
            sum_b[t] += part_b
        return carry

    lax.fori_loop(0, (list_ref[COUNT_AT] - OWN + BATCH - 1) // BATCH, batch, 0)
    fields = field_of(geo, sum_a, sum_b)
    scaled = RELAXATION * occupancy_ref[...].astype(jnp.float32) * own_part(geo[3])
    moved = jnp.zeros((OWN, SLOTS), jnp.float32)
    size = jnp.zeros((OWN, SLOTS), jnp.float32)
    for c in range(6):
        old = own_part(moment[c])
        new = (1.0 - RELAXATION) * old + scaled * (perm_ref[c] + fields[c])
        out_ref[c] = new
        moved = moved + (new - old) * (new - old)
        size = size + new * new
    for index, value in enumerate((moved, size)):
        total = jnp.sum(jnp.sum(value, axis=0, keepdims=True), axis=1, keepdims=True)
        size_ref[:, index : index + 1, :] = jnp.broadcast_to(
            total[None], (size_ref.shape[0], 1, SLOTS)
        )


def first_field(mask, gram, geo, later, occupancy, perm):
    return pl.pallas_call(
        first_kernel,
        name="first_field",
        in_specs=[smem_spec()] + [vmem_spec()] * 5,
        out_specs=[vmem_spec(), smem_spec(), vmem_spec()],
        out_shape=[
            jax.ShapeDtypeStruct((6, OWN, SLOTS), jnp.float32),
            jax.ShapeDtypeStruct((LIST,), jnp.int32),
            jax.ShapeDtypeStruct((PAIRS, 4 * SLOTS, SLOTS), jnp.bfloat16),
        ],
        scratch_shapes=[
            pltpu.VMEM(((TILES + 1) * (TERMS + 1), SLOTS), jnp.float32),
            pltpu.VMEM((OWN, TERMS, SLOTS), jnp.float32),
        ]
        + SCRATCH,
        compiler_params=pltpu.CompilerParams(vmem_limit_bytes=24 * 1024 * 1024),
        cost_estimate=pl.CostEstimate(
            flops=2_000_000_000, bytes_accessed=1_000_000, transcendentals=0
        ),
    )(mask, gram, geo, later, occupancy, perm)


def second_field(pair_list, geo, dipoles, occupancy, perm, pairs, copies):
    return pl.pallas_call(
        second_kernel,
        name="second_field",
        in_specs=[smem_spec()] + [vmem_spec()] * 5,
        out_specs=[vmem_spec(), vmem_spec()],
        out_shape=[
            jax.ShapeDtypeStruct((6, OWN, SLOTS), jnp.float32),
            jax.ShapeDtypeStruct((copies, 2, SLOTS), jnp.float32),
        ],
        scratch_shapes=SCRATCH,
        compiler_params=pltpu.CompilerParams(vmem_limit_bytes=24 * 1024 * 1024),
        cost_estimate=pl.CostEstimate(
            flops=1_000_000_000, bytes_accessed=1_000_000, transcendentals=0
        ),
    )(pair_list, geo, dipoles, occupancy, perm, pairs)


def with_halo(cells, sides):
    for axis, dim in sides:
        count = lax.axis_size(axis)
        head = lax.slice_in_dim(cells, 0, 1, axis=dim)
        tail = lax.slice_in_dim(cells, cells.shape[dim] - 1, cells.shape[dim], axis=dim)
        cells = jnp.concatenate(
            [
                lax.ppermute(tail, axis, [(i, (i + 1) % count) for i in range(count)]),
                cells,
                lax.ppermute(head, axis, [((i + 1) % count, i) for i in range(count)]),
            ],
            axis=dim,
        )
    return cells


SIDES = (("gx", 1), ("gy", 2), ("gz", 3))


def exchange(parts, axes):
    return lax.all_to_all(parts, axes, 0, 0)


def on_device(fractions, polarizability, occupancy, pair_mask, perm_field, history):
    plane = lax.axis_size("gy") * lax.axis_size("gz")
    line = lax.axis_size("gx")
    history = history.reshape(6, 6, OWN, SLOTS)
    occupancy = occupancy.reshape(OWN, SLOTS)
    perm = perm_field.reshape(6, OWN, SLOTS)

    gram = local_gram(history, occupancy, plane)
    filled = occupancy.astype(jnp.float32)
    later = (history[1:] * filled).reshape(30, 1, 2, 2, SLOTS)
    stacked = jnp.concatenate([fractions, polarizability[None], later], 0)
    stacked, gram = lax.optimization_barrier((stacked, gram))
    gram = exchange(gram, ("gy", "gz"))
    ghosts = with_halo(stacked, SIDES[:2])
    gram = sum_parts(gram, line)
    ghosts, gram = lax.optimization_barrier((ghosts, gram))
    gram = exchange(gram, "gx")
    ghosts = with_halo(ghosts, SIDES[2:])

    geo = ghosts[:4].reshape(4, TILES, SLOTS)
    later = ghosts[4:].reshape(30, TILES, SLOTS)
    dipoles, pair_list, pairs = first_field(
        pair_mask.reshape(OWN, OFFSETS), gram, geo, later, occupancy, perm
    )
    dipoles = with_halo(dipoles.reshape(6, 1, 2, 2, SLOTS), SIDES).reshape(6, TILES, SLOTS)
    induced, sizes = second_field(
        pair_list, geo, dipoles, occupancy, perm, pairs, plane
    )
    sizes = exchange(sizes, ("gy", "gz"))
    sizes = exchange(sum_parts(sizes, line), "gx")
    totals = jnp.sum(sizes, axis=0)
    change = jnp.sqrt(totals[0] / (totals[1] + 1.0))
    return induced.reshape(6, 1, 2, 2, SLOTS), change[0]


def solution(mesh):
    from jax.sharding import PartitionSpec as P

    tiles = P("gx", "gy", "gz", None)
    sets = P(None, "gx", "gy", "gz", None)
    return jax.shard_map(
        on_device,
        mesh=mesh,
        in_specs=(
            sets,
            tiles,
            tiles,
            tiles,
            sets,
            P(None, None, "gx", "gy", "gz", None),
        ),
        out_specs=(sets, P()),
        check_vma=False,
    )
```

```python
import jax
import jax.numpy as jnp
from jax import lax
from jax.experimental import pallas as pl
from jax.experimental.pallas import tpu as pltpu


CELL_EDGE = 10.0
SOFTENING = 0.3
THOLE_DAMP = 0.39
RELAXATION = 0.7
LN2 = 0.6931471805599453

SLOTS = 128
NX, NY, NZ = 3, 4, 4
TILES = NX * NY * NZ
OWN = 4
OFFSETS = 27
TERMS = 48
A_ROWS = 96
B_ROWS = 24
BATCH = 13
PAIRS = OWN + OWN * (OFFSETS - 1)
LIST = 128
COUNT_AT = LIST - 1
GRAM = tuple((a, b) for a in range(6) for b in range(a + 1))


def source_tile(tile, offset):
    x = offset // 9
    y = tile // 2 + offset // 3 % 3
    z = tile % 2 + offset % 3
    return (x * NY + y) * NZ + z


OWN_TILES = tuple(source_tile(t, 13) for t in range(OWN))


def split3(value):
    high = value.astype(jnp.bfloat16).astype(jnp.float32)
    rest = value - high
    middle = rest.astype(jnp.bfloat16).astype(jnp.float32)
    return high, middle, rest - middle


def positions(geo):
    tile = lax.broadcasted_iota(jnp.int32, (TILES, SLOTS), 0)
    x = (tile // (NY * NZ)).astype(jnp.float32)
    y = (tile // NZ % NY).astype(jnp.float32)
    z = (tile % NZ).astype(jnp.float32)
    return (
        (geo[0] + (x - 1.5)) * CELL_EDGE,
        (geo[1] + (y - 2.0)) * CELL_EDGE,
        (geo[2] + (z - 2.0)) * CELL_EDGE,
    )


def scale_of(polar):
    factor = (THOLE_DAMP / LN2) ** (1.0 / 3.0)
    return factor * jnp.exp(jnp.log(polar) * (-1.0 / 3.0))


def own_rows(value):
    return [value[t : t + 1] for t in OWN_TILES]


def prepare_distances(geo, q_ref, p_ref):
    r = positions(geo)
    a = scale_of(geo[3])
    norm = r[0] * r[0] + r[1] * r[1] + r[2] * r[2]
    sources = [a, a * (norm + SOFTENING), a * r[0], a * r[1], a * r[2]]
    targets = [a * norm, a, -2.0 * a * r[0], -2.0 * a * r[1], -2.0 * a * r[2]]
    row = 0
    for source, target in zip(sources, targets):
        source_parts = split3(source)
        target_parts = split3(target)
        for s in range(3):
            for t in range(3):
                q_ref[pl.ds(row, TILES, stride=TERMS + 1), :] = source_parts[s]
                for own in range(OWN):
                    p_ref[own, row : row + 1, :] = target_parts[t][
                        OWN_TILES[own] : OWN_TILES[own] + 1
                    ]
                row += 1
    zero = jnp.zeros((TILES, SLOTS), jnp.float32)
    for rest in range(row, TERMS):
        q_ref[pl.ds(rest, TILES, stride=TERMS + 1), :] = zero
        for own in range(OWN):
            p_ref[own, rest : rest + 1, :] = zero[0:1]

    q_ref[TILES * (TERMS + 1) : TILES * (TERMS + 1) + TERMS, :] = q_ref[0:TERMS, :]


def list_pairs(mask_ref, list_ref):
    count = jnp.int32(OWN)
    for t in range(OWN):
        list_ref[t] = OWN_TILES[t] * OWN + t
    for t in range(OWN):
        for k in range(OFFSETS):
            if k == 13:
                continue
            list_ref[count] = source_tile(t, k) * OWN + t
            count = count + (mask_ref[t, k] != 0).astype(jnp.int32)
    for extra in range(BATCH):
        list_ref[count + extra] = TILES * OWN
    list_ref[COUNT_AT] = count
    return count


def pair_functions(n, t, q_ref, p_ref, keep):
    dist = lax.dot_general(
        q_ref[pl.ds(n * (TERMS + 1), TERMS), :].astype(jnp.bfloat16),
        p_ref[t].astype(jnp.bfloat16),
        (((0,), (0,)), ((), ())),
        preferred_element_type=jnp.float32,
    )
    inv = lax.rsqrt(dist)
    arg = dist * (dist * inv)
    damp = jnp.exp2(-arg)
    inv2 = inv * inv
    direct = (1.0 - damp) * (inv2 * inv)
    radial = inv2 * (direct - LN2 * damp)
    if keep is not None:
        direct = jnp.where(keep, direct, 0.0)
        radial = jnp.where(keep, radial, 0.0)
    result = []
    for value in (radial, direct):
        high = value.astype(jnp.bfloat16)
        low = (value - high.astype(jnp.float32)).astype(jnp.bfloat16)
        result.append(jnp.concatenate([high, low], axis=0))
    return result


def prepare_moments(geo, moment, a_ref, b_ref):
    r = positions(geo)
    scale_a, scale_b = factors(geo)
    zero = jnp.zeros((TILES, SLOTS), jnp.float32)
    for kind in range(2):
        m = [moment[3 * kind + c] * scale_a for c in range(3)]
        outer = [r[c] * m[d] for c in range(3) for d in range(3)]
        g = outer[0] + outer[4] + outer[8]
        values = [None] + [r[c] * g for c in range(3)] + m + outer
        for index, value in enumerate(values):
            parts = (zero, zero, zero) if value is None else split3(value)
            for s, part in enumerate(parts):
                row = 32 * s + 16 * kind + index
                a_ref[pl.ds(row, TILES, stride=A_ROWS + 1), :] = part
    for c in range(8):
        parts = (zero, zero, zero) if c >= 6 else split3(moment[c] * scale_b)
        for s, part in enumerate(parts):
            b_ref[pl.ds(8 * s + c, TILES, stride=B_ROWS + 1), :] = part
    a_ref[TILES * (A_ROWS + 1) : TILES * (A_ROWS + 1) + A_ROWS, :] = jnp.zeros((A_ROWS, SLOTS), jnp.float32)
    b_ref[TILES * (B_ROWS + 1) : TILES * (B_ROWS + 1) + B_ROWS, :] = jnp.zeros((B_ROWS, SLOTS), jnp.float32)


def factors(geo):
    a = scale_of(geo[3])
    scale_b = a * jnp.sqrt(a)
    return scale_b * a, scale_b


def product(n, radial, direct, a_ref, b_ref):
    left = a_ref[pl.ds(n * (A_ROWS + 1), A_ROWS), :].astype(jnp.bfloat16)
    part_a = jnp.dot(
        jnp.concatenate([left, left], axis=1), radial, preferred_element_type=jnp.float32
    )
    left = b_ref[pl.ds(n * (B_ROWS + 1), B_ROWS), :].astype(jnp.bfloat16)
    part_b = jnp.dot(
        jnp.concatenate([left, left], axis=1), direct, preferred_element_type=jnp.float32
    )
    return part_a, part_b


def apply_pairs(list_ref, pair_ref, a_ref, b_ref, sum_a, sum_b):
    def pair(slot, n):
        return product(
            n,
            pair_ref[slot, 0 : 2 * SLOTS, :],
            pair_ref[slot, 2 * SLOTS : 4 * SLOTS, :],
            a_ref,
            b_ref,
        )

    for slot in range(OWN):
        sum_a[slot], sum_b[slot] = pair(slot, OWN_TILES[slot])

    def batch(b, carry):
        for u in range(BATCH):
            slot = OWN + b * BATCH + u
            entry = list_ref[slot]
            t = entry % OWN
            part_a, part_b = pair(slot, entry // OWN)
            sum_a[t] += part_a
            sum_b[t] += part_b
        return carry

    lax.fori_loop(0, (list_ref[COUNT_AT] - OWN + BATCH - 1) // BATCH, batch, 0)


def field_of(geo, sum_a, sum_b):
    r = positions(geo)
    scale_a, scale_b = factors(geo)
    own_r = [jnp.concatenate(own_rows(r[c]), 0) for c in range(3)]
    own_a = 3.0 * jnp.concatenate(own_rows(scale_a), 0)
    own_b = jnp.concatenate(own_rows(scale_b), 0)

    def total_a(kind, index):
        row = 16 * kind + index
        return sum_a[:, row, :] + sum_a[:, 32 + row, :] + sum_a[:, 64 + row, :]

    def total_b(row):
        return sum_b[:, row, :] + sum_b[:, 8 + row, :] + sum_b[:, 16 + row, :]

    fields = []
    for kind in range(2):
        outer = [[total_a(kind, 7 + 3 * c + d) for d in range(3)] for c in range(3)]
        g = outer[0][0] + outer[1][1] + outer[2][2]
        m = [total_a(kind, 4 + c) for c in range(3)]
        dot = own_r[0] * m[0] + own_r[1] * m[1] + own_r[2] * m[2] - g
        for c in range(3):
            cross = sum(own_r[d] * outer[c][d] for d in range(3))
            radial = total_a(kind, 1 + c) - cross + own_r[c] * dot
            fields.append(own_a * radial - own_b * total_b(3 * kind + c))
    return fields


def own_part(value):
    return jnp.concatenate(own_rows(value), 0)


def solve(gram):
    count = 5
    matrix = [[gram[max(a, b), min(a, b)] for b in range(count)] for a in range(count)]
    right = [gram[count, a] for a in range(count)]
    trace = matrix[0][0]
    for a in range(1, count):
        trace = trace + matrix[a][a]
    ridge = 0.001 * trace / count + 1.0
    for a in range(count):
        matrix[a][a] = matrix[a][a] + ridge
    for c in range(count):
        for a in range(c + 1, count):
            ratio = matrix[a][c] / matrix[c][c]
            for b in range(c + 1, a + 1):
                matrix[a][b] = matrix[a][b] - ratio * matrix[b][c]
            right[a] = right[a] - ratio * right[c]
    result = [None] * count
    for a in reversed(range(count)):
        rest = right[a]
        for b in range(a + 1, count):
            rest = rest - matrix[b][a] * result[b]
        result[a] = rest / matrix[a][a]
    return result


def gram_kernel(history_ref, occupancy_ref, out_ref):
    filled = occupancy_ref[...].astype(jnp.float32)
    masked = [
        [history_ref[h, c] * filled for c in range(6)] for h in range(6)
    ]
    lane = lax.broadcasted_iota(jnp.int32, (1, SLOTS), 1)
    row = jnp.zeros((1, SLOTS), jnp.float32)
    for index, (a, b) in enumerate(GRAM):
        product = masked[a][0] * masked[b][0]
        for c in range(1, 6):
            product = product + masked[a][c] * masked[b][c]
        total = jnp.sum(jnp.sum(product, axis=0, keepdims=True), axis=1, keepdims=True)
        row = jnp.where(lane == index, total, row)
    out_ref[...] = jnp.broadcast_to(row[None], out_ref.shape)


def vmem_spec():
    return pl.BlockSpec(memory_space=pltpu.VMEM)


def smem_spec():
    return pl.BlockSpec(memory_space=pltpu.SMEM)


def local_gram(history, occupancy, copies):
    return pl.pallas_call(
        gram_kernel,
        name="local_gram",
        in_specs=[vmem_spec(), vmem_spec()],
        out_specs=vmem_spec(),
        out_shape=jax.ShapeDtypeStruct((copies, 1, SLOTS), jnp.float32),
    )(history, occupancy)


def sum_parts(parts, copies):
    total = jnp.sum(parts, axis=0, keepdims=True)
    return jnp.broadcast_to(total, (copies,) + total.shape[1:])


SCRATCH = [
    pltpu.VMEM(((TILES + 1) * (A_ROWS + 1), SLOTS), jnp.float32),
    pltpu.VMEM(((TILES + 1) * (B_ROWS + 1), SLOTS), jnp.float32),
    pltpu.VMEM((OWN, A_ROWS, SLOTS), jnp.float32),
    pltpu.VMEM((OWN, B_ROWS, SLOTS), jnp.float32),
]


def first_kernel(
    mask_ref, gram_ref, geo_ref, later_ref, occupancy_ref, perm_ref,
    out_ref, list_ref, pair_ref, q_ref, p_ref, a_ref, b_ref, sum_a, sum_b,
):
    geo = [geo_ref[a] for a in range(4)]
    total = jnp.sum(gram_ref[...], axis=0)
    gram = {ab: total[0:1, i : i + 1] for i, ab in enumerate(GRAM)}
    coeffs = solve(gram)
    moment = []
    for c in range(6):
        value = coeffs[0] * later_ref[c]
        for h in range(1, 5):
            value = value + coeffs[h] * later_ref[6 * h + c]
        moment.append(value)
    prepare_distances(geo, q_ref, p_ref)
    prepare_moments(geo, moment, a_ref, b_ref)
    count = list_pairs(mask_ref, list_ref)

    def build(slot, n, t, keep):
        radial, direct = pair_functions(n, t, q_ref, p_ref, keep)
        pair_ref[slot, 0 : 2 * SLOTS, :] = radial
        pair_ref[slot, 2 * SLOTS : 4 * SLOTS, :] = direct

    keep = lax.broadcasted_iota(jnp.int32, (SLOTS, SLOTS), 0) != lax.broadcasted_iota(
        jnp.int32, (SLOTS, SLOTS), 1
    )
    for slot in range(OWN):
        build(slot, OWN_TILES[slot], slot, keep)

    def batch(b, carry):
        for u in range(BATCH):
            slot = OWN + b * BATCH + u
            entry = list_ref[slot]
            build(slot, entry // OWN, entry % OWN, None)
        return carry

    lax.fori_loop(0, (count - OWN + BATCH - 1) // BATCH, batch, 0)
    apply_pairs(list_ref, pair_ref, a_ref, b_ref, sum_a, sum_b)
    fields = field_of(geo, sum_a, sum_b)
    scaled = RELAXATION * occupancy_ref[...].astype(jnp.float32) * own_part(geo[3])
    for c in range(6):
        out_ref[c] = (1.0 - RELAXATION) * own_part(moment[c]) + scaled * (
            perm_ref[c] + fields[c]
        )


def second_kernel(
    list_ref, geo_ref, dipole_ref, occupancy_ref, perm_ref, pair_ref,
    out_ref, size_ref, a_ref, b_ref, sum_a, sum_b,
):
    geo = [geo_ref[a] for a in range(4)]
    moment = [dipole_ref[c] for c in range(6)]
    prepare_moments(geo, moment, a_ref, b_ref)

    apply_pairs(list_ref, pair_ref, a_ref, b_ref, sum_a, sum_b)
    fields = field_of(geo, sum_a, sum_b)
    scaled = RELAXATION * occupancy_ref[...].astype(jnp.float32) * own_part(geo[3])
    moved = jnp.zeros((OWN, SLOTS), jnp.float32)
    size = jnp.zeros((OWN, SLOTS), jnp.float32)
    for c in range(6):
        old = own_part(moment[c])
        new = (1.0 - RELAXATION) * old + scaled * (perm_ref[c] + fields[c])
        out_ref[c] = new
        moved = moved + (new - old) * (new - old)
        size = size + new * new
    for index, value in enumerate((moved, size)):
        total = jnp.sum(jnp.sum(value, axis=0, keepdims=True), axis=1, keepdims=True)
        size_ref[:, index : index + 1, :] = jnp.broadcast_to(
            total[None], (size_ref.shape[0], 1, SLOTS)
        )


def first_field(mask, gram, geo, later, occupancy, perm):
    return pl.pallas_call(
        first_kernel,
        name="first_field",
        in_specs=[smem_spec()] + [vmem_spec()] * 5,
        out_specs=[vmem_spec(), smem_spec(), vmem_spec()],
        out_shape=[
            jax.ShapeDtypeStruct((6, OWN, SLOTS), jnp.float32),
            jax.ShapeDtypeStruct((LIST,), jnp.int32),
            jax.ShapeDtypeStruct((PAIRS, 4 * SLOTS, SLOTS), jnp.bfloat16),
        ],
        scratch_shapes=[
            pltpu.VMEM(((TILES + 1) * (TERMS + 1), SLOTS), jnp.float32),
            pltpu.VMEM((OWN, TERMS, SLOTS), jnp.float32),
        ]
        + SCRATCH,
        compiler_params=pltpu.CompilerParams(vmem_limit_bytes=24 * 1024 * 1024),
        cost_estimate=pl.CostEstimate(
            flops=2_000_000_000, bytes_accessed=1_000_000, transcendentals=0
        ),
    )(mask, gram, geo, later, occupancy, perm)


def second_field(pair_list, geo, dipoles, occupancy, perm, pairs, copies):
    return pl.pallas_call(
        second_kernel,
        name="second_field",
        in_specs=[smem_spec()] + [vmem_spec()] * 5,
        out_specs=[vmem_spec(), vmem_spec()],
        out_shape=[
            jax.ShapeDtypeStruct((6, OWN, SLOTS), jnp.float32),
            jax.ShapeDtypeStruct((copies, 2, SLOTS), jnp.float32),
        ],
        scratch_shapes=SCRATCH,
        compiler_params=pltpu.CompilerParams(vmem_limit_bytes=24 * 1024 * 1024),
        cost_estimate=pl.CostEstimate(
            flops=1_000_000_000, bytes_accessed=1_000_000, transcendentals=0
        ),
    )(pair_list, geo, dipoles, occupancy, perm, pairs)


def with_halo(cells, sides):
    for axis, dim in sides:
        count = lax.axis_size(axis)
        head = lax.slice_in_dim(cells, 0, 1, axis=dim)
        tail = lax.slice_in_dim(cells, cells.shape[dim] - 1, cells.shape[dim], axis=dim)
        before = lax.ppermute(tail, axis, [(i, (i + 1) % count) for i in range(count)])
        after = lax.ppermute(head, axis, [((i + 1) % count, i) for i in range(count)])
        cells = jnp.concatenate([before, cells, after], axis=dim)
    return cells


SIDES = (("gx", 1), ("gy", 2), ("gz", 3))


def exchange(parts, axes):
    return lax.all_to_all(parts, axes, 0, 0)


def device_step(fractions, polarizability, occupancy, pair_mask, perm_field, history):
    plane = lax.axis_size("gy") * lax.axis_size("gz")
    line = lax.axis_size("gx")
    history = history.reshape(6, 6, OWN, SLOTS)
    occupancy = occupancy.reshape(OWN, SLOTS)
    perm = perm_field.reshape(6, OWN, SLOTS)

    gram = local_gram(history, occupancy, plane)
    filled = occupancy.astype(jnp.float32)
    later = (history[1:] * filled).reshape(30, 1, 2, 2, SLOTS)
    stacked = jnp.concatenate([fractions, polarizability[None], later], 0)
    stacked, gram = lax.optimization_barrier((stacked, gram))
    gram = exchange(gram, ("gy", "gz"))
    ghosts = with_halo(stacked, SIDES[:2])
    gram = sum_parts(gram, line)
    ghosts, gram = lax.optimization_barrier((ghosts, gram))
    gram = exchange(gram, "gx")
    ghosts = with_halo(ghosts, SIDES[2:])

    geo = ghosts[:4].reshape(4, TILES, SLOTS)
    later = ghosts[4:].reshape(30, TILES, SLOTS)
    dipoles, pair_list, pairs = first_field(
        pair_mask.reshape(OWN, OFFSETS), gram, geo, later, occupancy, perm
    )
    dipoles = with_halo(dipoles.reshape(6, 1, 2, 2, SLOTS), SIDES).reshape(6, TILES, SLOTS)
    induced, sizes = second_field(
        pair_list, geo, dipoles, occupancy, perm, pairs, plane
    )
    sizes = exchange(sizes, ("gy", "gz"))
    sizes = exchange(sum_parts(sizes, line), "gx")
    totals = jnp.sum(sizes, axis=0)
    change = jnp.sqrt(totals[0] / (totals[1] + 1.0))
    return induced.reshape(6, 1, 2, 2, SLOTS), change[0]


def solution(mesh):
    from jax.sharding import PartitionSpec as P

    tiles = P("gx", "gy", "gz", None)
    sets = P(None, "gx", "gy", "gz", None)
    return jax.shard_map(
        device_step,
        mesh=mesh,
        in_specs=(
            sets,
            tiles,
            tiles,
            tiles,
            sets,
            P(None, None, "gx", "gy", "gz", None),
        ),
        out_specs=(sets, P()),
        check_vma=False,
    )
```

```python
import jax
import jax.numpy as jnp
from jax import lax
from jax.experimental import pallas as pl
from jax.experimental.pallas import tpu as pltpu


CELL_EDGE = 10.0
SOFTENING = 0.3
THOLE_DAMP = 0.39
RELAXATION = 0.7
LN2 = 0.6931471805599453

SLOTS = 128
NX, NY, NZ = 3, 4, 4
TILES = NX * NY * NZ
OWN = 4
OFFSETS = 27
TERMS = 48
A_ROWS = 96
B_ROWS = 24
BATCH = 13
PAIRS = OWN + OWN * (OFFSETS - 1)
LIST = 128
COUNT_AT = LIST - 1
ROWS = 34
PLANE = NY * NZ
GRAM = tuple((a, b) for a in range(6) for b in range(a + 1))


def source_tile(tile, offset):
    x = offset // 9
    y = tile // 2 + offset // 3 % 3
    z = tile % 2 + offset % 3
    return (x * NY + y) * NZ + z


OWN_TILES = tuple(source_tile(t, 13) for t in range(OWN))


def split3(value):
    high = value.astype(jnp.bfloat16).astype(jnp.float32)
    rest = value - high
    middle = rest.astype(jnp.bfloat16).astype(jnp.float32)
    return high, middle, rest - middle


def positions(geo):
    tile = lax.broadcasted_iota(jnp.int32, (TILES, SLOTS), 0)
    x = (tile // (NY * NZ)).astype(jnp.float32)
    y = (tile // NZ % NY).astype(jnp.float32)
    z = (tile % NZ).astype(jnp.float32)
    return (
        (geo[0] + (x - 1.5)) * CELL_EDGE,
        (geo[1] + (y - 2.0)) * CELL_EDGE,
        (geo[2] + (z - 2.0)) * CELL_EDGE,
    )


def scale_of(polar):
    factor = (THOLE_DAMP / LN2) ** (1.0 / 3.0)
    return factor * jnp.exp(jnp.log(polar) * (-1.0 / 3.0))


def own_rows(value):
    return [value[t : t + 1] for t in OWN_TILES]


def prepare_distances(geo, q_ref, p_ref):
    r = positions(geo)
    a = scale_of(geo[3])
    norm = r[0] * r[0] + r[1] * r[1] + r[2] * r[2]
    sources = [a, a * (norm + SOFTENING), a * r[0], a * r[1], a * r[2]]
    targets = [a * norm, a, -2.0 * a * r[0], -2.0 * a * r[1], -2.0 * a * r[2]]
    row = 0
    for source, target in zip(sources, targets):
        source_parts = split3(source)
        target_parts = split3(target)
        for s in range(3):
            for t in range(3):
                q_ref[pl.ds(row, TILES, stride=TERMS + 1), :] = source_parts[s]
                for own in range(OWN):
                    p_ref[own, row : row + 1, :] = target_parts[t][
                        OWN_TILES[own] : OWN_TILES[own] + 1
                    ]
                row += 1
    zero = jnp.zeros((TILES, SLOTS), jnp.float32)
    for rest in range(row, TERMS):
        q_ref[pl.ds(rest, TILES, stride=TERMS + 1), :] = zero
        for own in range(OWN):
            p_ref[own, rest : rest + 1, :] = zero[0:1]

    q_ref[TILES * (TERMS + 1) : TILES * (TERMS + 1) + TERMS, :] = q_ref[0:TERMS, :]


def list_pairs(mask_ref, list_ref):
    count = jnp.int32(OWN)
    for t in range(OWN):
        list_ref[t] = OWN_TILES[t] * OWN + t
    for t in range(OWN):
        for k in range(OFFSETS):
            if k == 13:
                continue
            list_ref[count] = source_tile(t, k) * OWN + t
            count = count + (mask_ref[t, k] != 0).astype(jnp.int32)
    for extra in range(BATCH):
        list_ref[count + extra] = TILES * OWN
    list_ref[COUNT_AT] = count
    return count


def pair_functions(n, t, q_ref, p_ref, keep):
    dist = lax.dot_general(
        q_ref[pl.ds(n * (TERMS + 1), TERMS), :].astype(jnp.bfloat16),
        p_ref[t].astype(jnp.bfloat16),
        (((0,), (0,)), ((), ())),
        preferred_element_type=jnp.float32,
    )
    inv = lax.rsqrt(dist)
    arg = dist * (dist * inv)
    damp = jnp.exp2(-arg)
    inv2 = inv * inv
    direct = (1.0 - damp) * (inv2 * inv)
    radial = inv2 * (direct - LN2 * damp)
    if keep is not None:
        direct = jnp.where(keep, direct, 0.0)
        radial = jnp.where(keep, radial, 0.0)
    result = []
    for value in (radial, direct):
        high = value.astype(jnp.bfloat16)
        low = (value - high.astype(jnp.float32)).astype(jnp.bfloat16)
        result.append(jnp.concatenate([high, low], axis=0))
    return result


def prepare_moments(geo, moment, a_ref, b_ref):
    r = positions(geo)
    scale_a, scale_b = factors(geo)
    zero = jnp.zeros((TILES, SLOTS), jnp.float32)
    for kind in range(2):
        m = [moment[3 * kind + c] * scale_a for c in range(3)]
        outer = [r[c] * m[d] for c in range(3) for d in range(3)]
        g = outer[0] + outer[4] + outer[8]
        values = [None] + [r[c] * g for c in range(3)] + m + outer
        for index, value in enumerate(values):
            parts = (zero, zero, zero) if value is None else split3(value)
            for s, part in enumerate(parts):
                row = 32 * s + 16 * kind + index
                a_ref[pl.ds(row, TILES, stride=A_ROWS + 1), :] = part
    for c in range(8):
        parts = (zero, zero, zero) if c >= 6 else split3(moment[c] * scale_b)
        for s, part in enumerate(parts):
            b_ref[pl.ds(8 * s + c, TILES, stride=B_ROWS + 1), :] = part
    a_ref[TILES * (A_ROWS + 1) : TILES * (A_ROWS + 1) + A_ROWS, :] = jnp.zeros((A_ROWS, SLOTS), jnp.float32)
    b_ref[TILES * (B_ROWS + 1) : TILES * (B_ROWS + 1) + B_ROWS, :] = jnp.zeros((B_ROWS, SLOTS), jnp.float32)


def factors(geo):
    a = scale_of(geo[3])
    scale_b = a * jnp.sqrt(a)
    return scale_b * a, scale_b


def product(n, radial, direct, a_ref, b_ref):
    left = a_ref[pl.ds(n * (A_ROWS + 1), A_ROWS), :].astype(jnp.bfloat16)
    part_a = jnp.dot(
        jnp.concatenate([left, left], axis=1), radial, preferred_element_type=jnp.float32
    )
    left = b_ref[pl.ds(n * (B_ROWS + 1), B_ROWS), :].astype(jnp.bfloat16)
    part_b = jnp.dot(
        jnp.concatenate([left, left], axis=1), direct, preferred_element_type=jnp.float32
    )
    return part_a, part_b


def apply_pairs(list_ref, pair_ref, a_ref, b_ref, sum_a, sum_b):
    def pair(slot, n):
        return product(
            n,
            pair_ref[slot, 0 : 2 * SLOTS, :],
            pair_ref[slot, 2 * SLOTS : 4 * SLOTS, :],
            a_ref,
            b_ref,
        )

    for slot in range(OWN):
        sum_a[slot], sum_b[slot] = pair(slot, OWN_TILES[slot])

    def batch(b, carry):
        for u in range(BATCH):
            slot = OWN + b * BATCH + u
            entry = list_ref[slot]
            t = entry % OWN
            part_a, part_b = pair(slot, entry // OWN)
            sum_a[t] += part_a
            sum_b[t] += part_b
        return carry

    lax.fori_loop(0, (list_ref[COUNT_AT] - OWN + BATCH - 1) // BATCH, batch, 0)


def field_of(geo, sum_a, sum_b):
    r = positions(geo)
    scale_a, scale_b = factors(geo)
    own_r = [jnp.concatenate(own_rows(r[c]), 0) for c in range(3)]
    own_a = 3.0 * jnp.concatenate(own_rows(scale_a), 0)
    own_b = jnp.concatenate(own_rows(scale_b), 0)

    def total_a(kind, index):
        row = 16 * kind + index
        return sum_a[:, row, :] + sum_a[:, 32 + row, :] + sum_a[:, 64 + row, :]

    def total_b(row):
        return sum_b[:, row, :] + sum_b[:, 8 + row, :] + sum_b[:, 16 + row, :]

    fields = []
    for kind in range(2):
        outer = [[total_a(kind, 7 + 3 * c + d) for d in range(3)] for c in range(3)]
        g = outer[0][0] + outer[1][1] + outer[2][2]
        m = [total_a(kind, 4 + c) for c in range(3)]
        dot = own_r[0] * m[0] + own_r[1] * m[1] + own_r[2] * m[2] - g
        for c in range(3):
            cross = sum(own_r[d] * outer[c][d] for d in range(3))
            radial = total_a(kind, 1 + c) - cross + own_r[c] * dot
            fields.append(own_a * radial - own_b * total_b(3 * kind + c))
    return fields


def own_part(value):
    return jnp.concatenate(own_rows(value), 0)


def solve(gram):
    count = 5
    matrix = [[gram[max(a, b), min(a, b)] for b in range(count)] for a in range(count)]
    right = [gram[count, a] for a in range(count)]
    trace = matrix[0][0]
    for a in range(1, count):
        trace = trace + matrix[a][a]
    ridge = 0.001 * trace / count + 1.0
    for a in range(count):
        matrix[a][a] = matrix[a][a] + ridge
    for c in range(count):
        for a in range(c + 1, count):
            ratio = matrix[a][c] / matrix[c][c]
            for b in range(c + 1, a + 1):
                matrix[a][b] = matrix[a][b] - ratio * matrix[b][c]
            right[a] = right[a] - ratio * right[c]
    result = [None] * count
    for a in reversed(range(count)):
        rest = right[a]
        for b in range(a + 1, count):
            rest = rest - matrix[b][a] * result[b]
        result[a] = rest / matrix[a][a]
    return result


def prepare_kernel(fractions_ref, polar_ref, occupancy_ref, history_ref, stacked_ref, gram_ref):
    filled = occupancy_ref[...].astype(jnp.float32)
    masked = [[history_ref[h, c] * filled for c in range(6)] for h in range(6)]
    for a in range(3):
        stacked_ref[a] = fractions_ref[a]
    stacked_ref[3] = polar_ref[...]
    for h in range(1, 6):
        for c in range(6):
            stacked_ref[4 + 6 * (h - 1) + c] = masked[h][c]
    lane = lax.broadcasted_iota(jnp.int32, (1, SLOTS), 1)
    row = jnp.zeros((1, SLOTS), jnp.float32)
    for index, (a, b) in enumerate(GRAM):
        product = masked[a][0] * masked[b][0]
        for c in range(1, 6):
            product = product + masked[a][c] * masked[b][c]
        total = jnp.sum(jnp.sum(product, axis=0, keepdims=True), axis=1, keepdims=True)
        row = jnp.where(lane == index, total, row)
    gram_ref[...] = jnp.broadcast_to(row[None], gram_ref.shape)


def vmem_spec():
    return pl.BlockSpec(memory_space=pltpu.VMEM)


def smem_spec():
    return pl.BlockSpec(memory_space=pltpu.SMEM)


def prepare(fractions, polarizability, occupancy, history, copies):
    return pl.pallas_call(
        prepare_kernel,
        name="prepare",
        in_specs=[vmem_spec()] * 4,
        out_specs=[vmem_spec(), vmem_spec()],
        out_shape=[
            jax.ShapeDtypeStruct((ROWS, OWN, SLOTS), jnp.float32),
            jax.ShapeDtypeStruct((copies, 1, SLOTS), jnp.float32),
        ],
    )(fractions, polarizability, occupancy, history)


def sum_parts(parts, copies):
    total = jnp.sum(parts, axis=0, keepdims=True)
    return jnp.broadcast_to(total, (copies,) + total.shape[1:])


SCRATCH = [
    pltpu.VMEM(((TILES + 1) * (A_ROWS + 1), SLOTS), jnp.float32),
    pltpu.VMEM(((TILES + 1) * (B_ROWS + 1), SLOTS), jnp.float32),
    pltpu.VMEM((OWN, A_ROWS, SLOTS), jnp.float32),
    pltpu.VMEM((OWN, B_ROWS, SLOTS), jnp.float32),
]


def whole(slabs, row):
    return jnp.concatenate([slab[row] for slab in slabs], axis=0)


def first_kernel(
    mask_hbm, occupancy_hbm, perm_hbm, gram_ref, before_ref, own_ref, after_ref,
    out_ref, list_ref, geo_ref, scaled_ref, perm_ref, pair_ref,
    mask_ref, occupancy_ref, q_ref, p_ref, a_ref, b_ref, sum_a, sum_b, mask_sem, own_sem, perm_sem,
):
    copies = [
        pltpu.make_async_copy(mask_hbm, mask_ref, mask_sem),
        pltpu.make_async_copy(occupancy_hbm, occupancy_ref, own_sem),
        pltpu.make_async_copy(perm_hbm, perm_ref, perm_sem),
    ]
    for copy in copies:
        copy.start()
    slabs = (before_ref, own_ref, after_ref)
    geo = [whole(slabs, a) for a in range(4)]
    for a in range(4):
        geo_ref[a] = geo[a]
    later_ref = [whole(slabs, row) for row in range(4, ROWS)]
    total = jnp.sum(gram_ref[...], axis=0)
    gram = {ab: total[0:1, i : i + 1] for i, ab in enumerate(GRAM)}
    coeffs = solve(gram)
    moment = []
    for c in range(6):
        value = coeffs[0] * later_ref[c]
        for h in range(1, 5):
            value = value + coeffs[h] * later_ref[6 * h + c]
        moment.append(value)
    prepare_distances(geo, q_ref, p_ref)
    prepare_moments(geo, moment, a_ref, b_ref)
    for copy in copies:
        copy.wait()
    count = list_pairs(mask_ref, list_ref)

    def build(slot, n, t, keep):
        radial, direct = pair_functions(n, t, q_ref, p_ref, keep)
        pair_ref[slot, 0 : 2 * SLOTS, :] = radial
        pair_ref[slot, 2 * SLOTS : 4 * SLOTS, :] = direct

    keep = lax.broadcasted_iota(jnp.int32, (SLOTS, SLOTS), 0) != lax.broadcasted_iota(
        jnp.int32, (SLOTS, SLOTS), 1
    )
    for slot in range(OWN):
        build(slot, OWN_TILES[slot], slot, keep)

    def batch(b, carry):
        for u in range(BATCH):
            slot = OWN + b * BATCH + u
            entry = list_ref[slot]
            build(slot, entry // OWN, entry % OWN, None)
        return carry

    lax.fori_loop(0, (count - OWN + BATCH - 1) // BATCH, batch, 0)
    apply_pairs(list_ref, pair_ref, a_ref, b_ref, sum_a, sum_b)
    fields = field_of(geo, sum_a, sum_b)
    scaled = RELAXATION * occupancy_ref[...].astype(jnp.float32) * own_part(geo[3])
    scaled_ref[...] = scaled
    for c in range(6):
        out_ref[c] = (1.0 - RELAXATION) * own_part(moment[c]) + scaled * (
            perm_ref[c] + fields[c]
        )


def second_kernel(
    list_ref, geo_ref, before_ref, own_ref, after_ref, scaled_ref, perm_ref, pair_ref,
    out_ref, size_ref, a_ref, b_ref, sum_a, sum_b,
):
    geo = [geo_ref[a] for a in range(4)]
    slabs = (before_ref, own_ref, after_ref)
    moment = [whole(slabs, c) for c in range(6)]
    prepare_moments(geo, moment, a_ref, b_ref)

    apply_pairs(list_ref, pair_ref, a_ref, b_ref, sum_a, sum_b)
    fields = field_of(geo, sum_a, sum_b)
    scaled = scaled_ref[...]
    moved = jnp.zeros((OWN, SLOTS), jnp.float32)
    size = jnp.zeros((OWN, SLOTS), jnp.float32)
    for c in range(6):
        old = own_part(moment[c])
        new = (1.0 - RELAXATION) * old + scaled * (perm_ref[c] + fields[c])
        out_ref[c] = new
        moved = moved + (new - old) * (new - old)
        size = size + new * new
    for index, value in enumerate((moved, size)):
        total = jnp.sum(jnp.sum(value, axis=0, keepdims=True), axis=1, keepdims=True)
        size_ref[:, index : index + 1, :] = jnp.broadcast_to(
            total[None], (size_ref.shape[0], 1, SLOTS)
        )


def first_field(mask, occupancy, perm, gram, slabs):
    whole_array = pl.BlockSpec(memory_space=pltpu.HBM)
    return pl.pallas_call(
        first_kernel,
        name="first_field",
        in_specs=[whole_array] * 3 + [vmem_spec()] * 4,
        out_specs=[vmem_spec(), smem_spec()] + [vmem_spec()] * 4,
        out_shape=[
            jax.ShapeDtypeStruct((6, OWN, SLOTS), jnp.float32),
            jax.ShapeDtypeStruct((LIST,), jnp.int32),
            jax.ShapeDtypeStruct((4, TILES, SLOTS), jnp.float32),
            jax.ShapeDtypeStruct((OWN, SLOTS), jnp.float32),
            jax.ShapeDtypeStruct((6, OWN, SLOTS), jnp.float32),
            jax.ShapeDtypeStruct((PAIRS, 4 * SLOTS, SLOTS), jnp.bfloat16),
        ],
        scratch_shapes=[
            pltpu.SMEM((OWN, OFFSETS), jnp.int32),
            pltpu.VMEM((OWN, SLOTS), jnp.int32),
            pltpu.VMEM(((TILES + 1) * (TERMS + 1), SLOTS), jnp.float32),
            pltpu.VMEM((OWN, TERMS, SLOTS), jnp.float32),
        ]
        + SCRATCH
        + [pltpu.SemaphoreType.DMA] * 3,
        compiler_params=pltpu.CompilerParams(vmem_limit_bytes=24 * 1024 * 1024),
        cost_estimate=pl.CostEstimate(
            flops=2_000_000_000, bytes_accessed=1_000_000, transcendentals=0
        ),
    )(mask, occupancy, perm, gram, *slabs)


def second_field(pair_list, geo, slabs, scaled, perm, pairs, copies):
    return pl.pallas_call(
        second_kernel,
        name="second_field",
        in_specs=[smem_spec()] + [vmem_spec()] * 7,
        out_specs=[vmem_spec(), vmem_spec()],
        out_shape=[
            jax.ShapeDtypeStruct((6, OWN, SLOTS), jnp.float32),
            jax.ShapeDtypeStruct((copies, 2, SLOTS), jnp.float32),
        ],
        scratch_shapes=SCRATCH,
        compiler_params=pltpu.CompilerParams(vmem_limit_bytes=24 * 1024 * 1024),
        cost_estimate=pl.CostEstimate(
            flops=1_000_000_000, bytes_accessed=1_000_000, transcendentals=0
        ),
    )(pair_list, geo, *slabs, scaled, perm, pairs)


def both_ways(low, high, axis):
    count = lax.axis_size(axis)
    before = lax.ppermute(high, axis, [(i, (i + 1) % count) for i in range(count)])
    after = lax.ppermute(low, axis, [((i + 1) % count, i) for i in range(count)])
    return before, after


def joined(cells, axis, dim):
    size = cells.shape[dim]
    low = lax.slice_in_dim(cells, 0, 1, axis=dim)
    high = lax.slice_in_dim(cells, size - 1, size, axis=dim)
    before, after = both_ways(low, high, axis)
    return jnp.concatenate([before, cells, after], axis=dim)


def three_slabs(cells):
    before, after = both_ways(cells, cells, "gx")
    return [
        slab.reshape(slab.shape[0], PLANE, SLOTS) for slab in (before, cells, after)
    ]


def exchange(parts, axes):
    return lax.all_to_all(parts, axes, 0, 0)


def device_step(fractions, polarizability, occupancy, pair_mask, perm_field, history):
    plane = lax.axis_size("gy") * lax.axis_size("gz")
    line = lax.axis_size("gx")
    occupancy = occupancy.reshape(OWN, SLOTS)
    stacked, gram = prepare(
        fractions.reshape(3, OWN, SLOTS),
        polarizability.reshape(OWN, SLOTS),
        occupancy,
        history.reshape(6, 6, OWN, SLOTS),
        plane,
    )
    gram = exchange(gram, ("gy", "gz"))
    cells = joined(stacked.reshape(ROWS, 2, 2, SLOTS), "gz", 2)
    cells = joined(cells, "gy", 1)
    gram = sum_parts(gram, line)
    cells, gram = lax.optimization_barrier((cells, gram))
    gram = exchange(gram, "gx")
    slabs = three_slabs(cells)
    dipoles, pair_list, geo, scaled, perm, pairs = first_field(
        pair_mask.reshape(OWN, OFFSETS),
        occupancy,
        perm_field.reshape(6, OWN, SLOTS),
        gram,
        slabs,
    )
    cells = joined(dipoles.reshape(6, 2, 2, SLOTS), "gz", 2)
    cells = joined(cells, "gy", 1)
    induced, sizes = second_field(
        pair_list, geo, three_slabs(cells), scaled, perm, pairs, plane
    )
    sizes = exchange(sizes, ("gy", "gz"))
    sizes = exchange(sum_parts(sizes, line), "gx")
    totals = jnp.sum(sizes, axis=0)
    change = jnp.sqrt(totals[0] / (totals[1] + 1.0))
    return induced.reshape(6, 1, 2, 2, SLOTS), change[0]


def solution(mesh):
    from jax.sharding import PartitionSpec as P

    tiles = P("gx", "gy", "gz", None)
    sets = P(None, "gx", "gy", "gz", None)
    return jax.shard_map(
        device_step,
        mesh=mesh,
        in_specs=(
            sets,
            tiles,
            tiles,
            tiles,
            sets,
            P(None, None, "gx", "gy", "gz", None),
        ),
        out_specs=(sets, P()),
        check_vma=False,
    )
```

```python
import jax
import jax.numpy as jnp
from jax import lax
from jax.experimental import pallas as pl
from jax.experimental.pallas import tpu as pltpu


CELL_EDGE = 10.0
SOFTENING = 0.3
THOLE_DAMP = 0.39
RELAXATION = 0.7
LN2 = 0.6931471805599453

SLOTS = 128
NX, NY, NZ = 3, 4, 4
TILES = NX * NY * NZ
OWN = 4
OFFSETS = 27
TERMS = 48
A_ROWS = 96
B_ROWS = 24
BATCH = 13
LIST = 128
COUNT_AT = LIST - 1
ROWS = 34
LAYER = NX * NY
INNER = 2 * LAYER
GRAM = tuple((a, b) for a in range(6) for b in range(a + 1))


def source_tile(tile, offset):
    x = offset // 9
    y = tile // 2 + offset // 3 % 3
    z = tile % 2 + offset % 3
    column = x * NY + y
    if z == 0:
        return INNER + column
    if z == NZ - 1:
        return INNER + LAYER + column
    return column * 2 + z - 1


def candidates(inner):
    return [
        (t, k)
        for t in range(OWN)
        for k in range(OFFSETS)
        if k != 13 and (source_tile(t, k) < INNER) == inner
    ]


OWN_TILES = tuple(source_tile(t, 13) for t in range(OWN))


def split3(value):
    high = value.astype(jnp.bfloat16).astype(jnp.float32)
    rest = value - high
    middle = rest.astype(jnp.bfloat16).astype(jnp.float32)
    return high, middle, rest - middle


def positions(geo, first):
    shape = geo[0].shape
    tile = lax.broadcasted_iota(jnp.int32, shape, 0) + first
    own = tile < INNER
    edge = tile - INNER
    above = edge >= LAYER
    column = jnp.where(own, tile // 2, jnp.where(above, edge - LAYER, edge))
    layer = jnp.where(own, tile % 2 + 1, jnp.where(above, NZ - 1, 0))
    x = (column // NY).astype(jnp.float32)
    y = (column % NY).astype(jnp.float32)
    z = layer.astype(jnp.float32)
    return (
        (geo[0] + (x - 1.5)) * CELL_EDGE,
        (geo[1] + (y - 2.0)) * CELL_EDGE,
        (geo[2] + (z - 2.0)) * CELL_EDGE,
    )


def scale_of(polar):
    factor = (THOLE_DAMP / LN2) ** (1.0 / 3.0)
    return factor * jnp.exp(jnp.log(polar) * (-1.0 / 3.0))


def own_rows(value):
    return [value[t : t + 1] for t in OWN_TILES]


def prepare_distances(own_geo, source_geo, first, q_ref, p_ref):
    def terms(geo, at):
        r = positions(geo, at)
        a = scale_of(geo[3])
        return r, a, r[0] * r[0] + r[1] * r[1] + r[2] * r[2]

    r, a, norm = terms(source_geo, first)
    count = a.shape[0]
    sources = [a, a * (norm + SOFTENING), a * r[0], a * r[1], a * r[2]]
    r, a, norm = terms(own_geo, 0)
    targets = [a * norm, a, -2.0 * a * r[0], -2.0 * a * r[1], -2.0 * a * r[2]]
    row = 0
    for source, target in zip(sources, targets):
        source_parts = split3(source)
        target_parts = split3(target)
        for s in range(3):
            for t in range(3):
                q_ref[pl.ds(row, count, stride=TERMS + 1), :] = source_parts[s]
                for own in range(OWN):
                    p_ref[own, row : row + 1, :] = target_parts[t][
                        OWN_TILES[own] : OWN_TILES[own] + 1
                    ]
                row += 1
    zero = jnp.zeros((count, SLOTS), jnp.float32)
    for rest in range(row, TERMS):
        q_ref[pl.ds(rest, count, stride=TERMS + 1), :] = zero
        for own in range(OWN):
            p_ref[own, rest : rest + 1, :] = zero[0:1]
    last = INNER * (TERMS + 1)
    q_ref[last : last + TERMS, :] = q_ref[0:TERMS, :]


def list_pairs(mask_ref, list_ref, inner):
    first = 0 if inner else INNER
    count = jnp.int32(0)
    for t, k in candidates(inner):
        list_ref[count] = (source_tile(t, k) - first) * OWN + t
        count = count + (mask_ref[t, k] != 0).astype(jnp.int32)
    for extra in range(BATCH):
        list_ref[count + extra] = INNER * OWN
    list_ref[COUNT_AT] = count
    return count


def trips(count):
    return (count + BATCH - 1) // BATCH


def build_all(list_ref, count, start, pair_ref, q_ref, p_ref):
    def batch(b, carry):
        for u in range(BATCH):
            slot = b * BATCH + u
            entry = list_ref[slot]
            build(start + slot, entry // OWN, entry % OWN, None, pair_ref, q_ref, p_ref)
        return carry

    lax.fori_loop(0, trips(count), batch, 0)


def build(slot, n, t, keep, pair_ref, q_ref, p_ref):
    radial, direct = pair_functions(n, t, q_ref, p_ref, keep)
    pair_ref[slot, 0 : 2 * SLOTS, :] = radial
    pair_ref[slot, 2 * SLOTS : 4 * SLOTS, :] = direct


def pair_functions(n, t, q_ref, p_ref, keep):
    dist = lax.dot_general(
        q_ref[pl.ds(n * (TERMS + 1), TERMS), :].astype(jnp.bfloat16),
        p_ref[t].astype(jnp.bfloat16),
        (((0,), (0,)), ((), ())),
        preferred_element_type=jnp.float32,
    )
    inv = lax.rsqrt(dist)
    arg = dist * (dist * inv)
    damp = jnp.exp2(-arg)
    inv2 = inv * inv
    direct = (1.0 - damp) * (inv2 * inv)
    radial = inv2 * (direct - LN2 * damp)
    if keep is not None:
        direct = jnp.where(keep, direct, 0.0)
        radial = jnp.where(keep, radial, 0.0)
    result = []
    for value in (radial, direct):
        high = value.astype(jnp.bfloat16)
        low = (value - high.astype(jnp.float32)).astype(jnp.bfloat16)
        result.append(jnp.concatenate([high, low], axis=0))
    return result


def prepare_moments(geo, first, moment, a_ref, b_ref):
    r = positions(geo, first)
    count = geo[0].shape[0]
    scale_a, scale_b = factors(geo)
    zero = jnp.zeros((count, SLOTS), jnp.float32)
    for kind in range(2):
        m = [moment[3 * kind + c] * scale_a for c in range(3)]
        outer = [r[c] * m[d] for c in range(3) for d in range(3)]
        g = outer[0] + outer[4] + outer[8]
        values = [None] + [r[c] * g for c in range(3)] + m + outer
        for index, value in enumerate(values):
            parts = (zero, zero, zero) if value is None else split3(value)
            for s, part in enumerate(parts):
                row = 32 * s + 16 * kind + index
                a_ref[pl.ds(row, count, stride=A_ROWS + 1), :] = part
    for c in range(8):
        parts = (zero, zero, zero) if c >= 6 else split3(moment[c] * scale_b)
        for s, part in enumerate(parts):
            b_ref[pl.ds(8 * s + c, count, stride=B_ROWS + 1), :] = part
    last_a = INNER * (A_ROWS + 1)
    last_b = INNER * (B_ROWS + 1)
    a_ref[last_a : last_a + A_ROWS, :] = jnp.zeros((A_ROWS, SLOTS), jnp.float32)
    b_ref[last_b : last_b + B_ROWS, :] = jnp.zeros((B_ROWS, SLOTS), jnp.float32)


def factors(geo):
    a = scale_of(geo[3])
    scale_b = a * jnp.sqrt(a)
    return scale_b * a, scale_b


def product(n, radial, direct, a_ref, b_ref):
    left = a_ref[pl.ds(n * (A_ROWS + 1), A_ROWS), :].astype(jnp.bfloat16)
    part_a = jnp.dot(
        jnp.concatenate([left, left], axis=1), radial, preferred_element_type=jnp.float32
    )
    left = b_ref[pl.ds(n * (B_ROWS + 1), B_ROWS), :].astype(jnp.bfloat16)
    part_b = jnp.dot(
        jnp.concatenate([left, left], axis=1), direct, preferred_element_type=jnp.float32
    )
    return part_a, part_b


def apply_slot(slot, n, pair_ref, a_ref, b_ref):
    return product(
        n,
        pair_ref[slot, 0 : 2 * SLOTS, :],
        pair_ref[slot, 2 * SLOTS : 4 * SLOTS, :],
        a_ref,
        b_ref,
    )


def apply_selves(pair_ref, a_ref, b_ref, sum_a, sum_b):
    for slot in range(OWN):
        sum_a[slot], sum_b[slot] = apply_slot(slot, OWN_TILES[slot], pair_ref, a_ref, b_ref)


def apply_all(list_ref, count, start, pair_ref, a_ref, b_ref, sum_a, sum_b):
    def batch(b, carry):
        for u in range(BATCH):
            slot = b * BATCH + u
            entry = list_ref[slot]
            t = entry % OWN
            part_a, part_b = apply_slot(start + slot, entry // OWN, pair_ref, a_ref, b_ref)
            sum_a[t] += part_a
            sum_b[t] += part_b
        return carry

    lax.fori_loop(0, trips(count), batch, 0)


def field_of(geo, sum_a, sum_b):
    r = positions(geo, 0)
    scale_a, scale_b = factors(geo)
    own_r = [jnp.concatenate(own_rows(r[c]), 0) for c in range(3)]
    own_a = 3.0 * jnp.concatenate(own_rows(scale_a), 0)
    own_b = jnp.concatenate(own_rows(scale_b), 0)

    def total_a(kind, index):
        row = 16 * kind + index
        return sum_a[:, row, :] + sum_a[:, 32 + row, :] + sum_a[:, 64 + row, :]

    def total_b(row):
        return sum_b[:, row, :] + sum_b[:, 8 + row, :] + sum_b[:, 16 + row, :]

    fields = []
    for kind in range(2):
        outer = [[total_a(kind, 7 + 3 * c + d) for d in range(3)] for c in range(3)]
        g = outer[0][0] + outer[1][1] + outer[2][2]
        m = [total_a(kind, 4 + c) for c in range(3)]
        dot = own_r[0] * m[0] + own_r[1] * m[1] + own_r[2] * m[2] - g
        for c in range(3):
            cross = sum(own_r[d] * outer[c][d] for d in range(3))
            radial = total_a(kind, 1 + c) - cross + own_r[c] * dot
            fields.append(own_a * radial - own_b * total_b(3 * kind + c))
    return fields


def own_part(value):
    return jnp.concatenate(own_rows(value), 0)


def solve(gram):
    count = 5
    matrix = [[gram[max(a, b), min(a, b)] for b in range(count)] for a in range(count)]
    right = [gram[count, a] for a in range(count)]
    trace = matrix[0][0]
    for a in range(1, count):
        trace = trace + matrix[a][a]
    ridge = 0.001 * trace / count + 1.0
    for a in range(count):
        matrix[a][a] = matrix[a][a] + ridge
    for c in range(count):
        for a in range(c + 1, count):
            ratio = matrix[a][c] / matrix[c][c]
            for b in range(c + 1, a + 1):
                matrix[a][b] = matrix[a][b] - ratio * matrix[b][c]
            right[a] = right[a] - ratio * right[c]
    result = [None] * count
    for a in reversed(range(count)):
        rest = right[a]
        for b in range(a + 1, count):
            rest = rest - matrix[b][a] * result[b]
        result[a] = rest / matrix[a][a]
    return result


def prepare_kernel(
    fractions_ref, polar_ref, occupancy_ref, history_ref, perm_ref, mask_ref,
    stacked_ref, gram_ref, own_ref, mask_copy_ref,
):
    filled = occupancy_ref[...].astype(jnp.float32)
    scaled = RELAXATION * filled * polar_ref[...]
    own_ref[0] = scaled
    for c in range(6):
        own_ref[1 + c] = perm_ref[c]
    mask_copy_ref[...] = mask_ref[...]
    masked = [[history_ref[h, c] * filled for c in range(6)] for h in range(6)]
    for a in range(3):
        stacked_ref[a] = fractions_ref[a]
    stacked_ref[3] = polar_ref[...]
    for h in range(1, 6):
        for c in range(6):
            stacked_ref[4 + 6 * (h - 1) + c] = masked[h][c]
    lane = lax.broadcasted_iota(jnp.int32, (1, SLOTS), 1)
    row = jnp.zeros((1, SLOTS), jnp.float32)
    for index, (a, b) in enumerate(GRAM):
        product = masked[a][0] * masked[b][0]
        for c in range(1, 6):
            product = product + masked[a][c] * masked[b][c]
        total = jnp.sum(jnp.sum(product, axis=0, keepdims=True), axis=1, keepdims=True)
        row = jnp.where(lane == index, total, row)
    gram_ref[...] = jnp.broadcast_to(row[None], gram_ref.shape)


def vmem_spec():
    return pl.BlockSpec(memory_space=pltpu.VMEM)


def smem_spec():
    return pl.BlockSpec(memory_space=pltpu.SMEM)


def prepare(fractions, polarizability, occupancy, history, perm, mask, copies):
    return pl.pallas_call(
        prepare_kernel,
        name="prepare",
        in_specs=[vmem_spec()] * 6,
        out_specs=[vmem_spec()] * 4,
        out_shape=[
            jax.ShapeDtypeStruct((ROWS, OWN, SLOTS), jnp.float32),
            jax.ShapeDtypeStruct((copies, 1, SLOTS), jnp.float32),
            jax.ShapeDtypeStruct((7, OWN, SLOTS), jnp.float32),
            jax.ShapeDtypeStruct((OWN, OFFSETS), jnp.int32),
        ],
    )(fractions, polarizability, occupancy, history, perm, mask)


def sum_parts(parts, copies):
    total = jnp.sum(parts, axis=0, keepdims=True)
    return jnp.broadcast_to(total, (copies,) + total.shape[1:])


MOMENT_ROWS = [
    pltpu.VMEM(((INNER + 1) * (A_ROWS + 1), SLOTS), jnp.float32),
    pltpu.VMEM(((INNER + 1) * (B_ROWS + 1), SLOTS), jnp.float32),
]
DISTANCE_ROWS = [
    pltpu.VMEM(((INNER + 1) * (TERMS + 1), SLOTS), jnp.float32),
    pltpu.VMEM((OWN, TERMS, SLOTS), jnp.float32),
]
SUMS = [
    jax.ShapeDtypeStruct((OWN, A_ROWS, SLOTS), jnp.float32),
    jax.ShapeDtypeStruct((OWN, B_ROWS, SLOTS), jnp.float32),
]
PARAMS = pltpu.CompilerParams(vmem_limit_bytes=16 * 1024 * 1024)


def slots_for(inner):
    batches = -(-len(candidates(inner)) // BATCH)
    return batches * BATCH + (OWN if inner else 0)


def pair_shape(inner):
    return jax.ShapeDtypeStruct((slots_for(inner), 4 * SLOTS, SLOTS), jnp.bfloat16)


def cost(flops):
    return pl.CostEstimate(flops=flops, bytes_accessed=1_000_000, transcendentals=0)


def edge_rows(before_ref, after_ref, row):
    rows = pl.ds(row * LAYER, LAYER)
    return jnp.concatenate([before_ref[rows, :], after_ref[rows, :]], axis=0)


def coefficients(gram_ref):
    total = jnp.sum(gram_ref[...], axis=0)
    return solve({ab: total[0:1, i : i + 1] for i, ab in enumerate(GRAM)})


def predict(coeffs, later):
    moment = []
    for c in range(6):
        value = coeffs[0] * later[c]
        for h in range(1, 5):
            value = value + coeffs[h] * later[6 * h + c]
        moment.append(value)
    return moment


def inner_build_kernel(
    mask_ref, gram_ref, own_ref,
    list_ref, pair_ref, moment_ref, sum_a, sum_b,
    q_ref, p_ref, a_ref, b_ref,
):
    geo = [own_ref[a] for a in range(4)]
    prepare_distances(geo, geo, 0, q_ref, p_ref)
    count = list_pairs(mask_ref, list_ref, True)
    moment = predict(coefficients(gram_ref), [own_ref[row] for row in range(4, ROWS)])
    prepare_moments(geo, 0, moment, a_ref, b_ref)
    for c in range(6):
        moment_ref[c] = own_part(moment[c])
    keep = lax.broadcasted_iota(jnp.int32, (SLOTS, SLOTS), 0) != lax.broadcasted_iota(
        jnp.int32, (SLOTS, SLOTS), 1
    )
    for slot in range(OWN):
        build(slot, OWN_TILES[slot], slot, keep, pair_ref, q_ref, p_ref)
    build_all(list_ref, count, OWN, pair_ref, q_ref, p_ref)
    apply_selves(pair_ref, a_ref, b_ref, sum_a, sum_b)
    apply_all(list_ref, count, OWN, pair_ref, a_ref, b_ref, sum_a, sum_b)


def inner_build(mask, gram, own):
    return pl.pallas_call(
        inner_build_kernel,
        name="inner_build",
        in_specs=[smem_spec()] + [vmem_spec()] * 2,
        out_specs=[smem_spec()] + [vmem_spec()] * 4,
        out_shape=[
            jax.ShapeDtypeStruct((LIST,), jnp.int32),
            pair_shape(True),
            jax.ShapeDtypeStruct((6, OWN, SLOTS), jnp.float32),
        ]
        + SUMS,
        scratch_shapes=DISTANCE_ROWS + MOMENT_ROWS,
        compiler_params=PARAMS,
        cost_estimate=cost(2_000_000_000),
    )(mask, gram, own)


def first_kernel(
    mask_ref, gram_ref, own_ref, before_ref, after_ref, mine_ref, moment_ref, start_a, start_b,
    out_ref, list_ref, geo_ref, pair_ref,
    q_ref, p_ref, a_ref, b_ref, sum_a, sum_b,
):
    own_geo = [own_ref[a] for a in range(4)]
    edge_geo = [edge_rows(before_ref, after_ref, a) for a in range(4)]
    for a in range(4):
        geo_ref[a, 0:INNER, :] = own_geo[a]
        geo_ref[a, INNER:TILES, :] = edge_geo[a]
    prepare_distances(own_geo, edge_geo, INNER, q_ref, p_ref)
    count = list_pairs(mask_ref, list_ref, False)
    sum_a[...] = start_a[...]
    sum_b[...] = start_b[...]
    moment = predict(
        coefficients(gram_ref),
        [edge_rows(before_ref, after_ref, row) for row in range(4, ROWS)],
    )
    prepare_moments(edge_geo, INNER, moment, a_ref, b_ref)
    build_all(list_ref, count, 0, pair_ref, q_ref, p_ref)
    apply_all(list_ref, count, 0, pair_ref, a_ref, b_ref, sum_a, sum_b)

    fields = field_of(own_geo, sum_a, sum_b)
    for c in range(6):
        out_ref[c] = (1.0 - RELAXATION) * moment_ref[c] + mine_ref[0] * (
            mine_ref[1 + c] + fields[c]
        )


def first_field(mask, gram, own, before, after, mine, moment, sums):
    return pl.pallas_call(
        first_kernel,
        name="first_field",
        in_specs=[smem_spec()] + [vmem_spec()] * 8,
        out_specs=[vmem_spec(), smem_spec(), vmem_spec(), vmem_spec()],
        out_shape=[
            jax.ShapeDtypeStruct((6, OWN, SLOTS), jnp.float32),
            jax.ShapeDtypeStruct((LIST,), jnp.int32),
            jax.ShapeDtypeStruct((4, TILES, SLOTS), jnp.float32),
            pair_shape(False),
        ],
        scratch_shapes=DISTANCE_ROWS
        + MOMENT_ROWS
        + [pltpu.VMEM(part.shape, part.dtype) for part in SUMS],
        compiler_params=PARAMS,
        cost_estimate=cost(2_000_000_000),
    )(mask, gram, own, before, after, mine, moment, *sums)


def inner_apply_kernel(
    list_ref, geo_ref, own_ref, pair_ref, sum_a, sum_b, a_ref, b_ref
):
    geo = [geo_ref[a, 0:INNER, :] for a in range(4)]
    prepare_moments(geo, 0, [own_ref[c] for c in range(6)], a_ref, b_ref)
    apply_selves(pair_ref, a_ref, b_ref, sum_a, sum_b)
    apply_all(list_ref, list_ref[COUNT_AT], OWN, pair_ref, a_ref, b_ref, sum_a, sum_b)


def inner_apply(pair_list, geo, own, pairs):
    return pl.pallas_call(
        inner_apply_kernel,
        name="inner_apply",
        in_specs=[smem_spec()] + [vmem_spec()] * 3,
        out_specs=[vmem_spec()] * 2,
        out_shape=SUMS,
        scratch_shapes=MOMENT_ROWS,
        compiler_params=PARAMS,
        cost_estimate=cost(1_000_000_000),
    )(pair_list, geo, own, pairs)


def second_kernel(
    list_ref, geo_ref, own_ref, before_ref, after_ref, mine_ref, pair_ref, start_a, start_b,
    out_ref, size_ref, a_ref, b_ref, sum_a, sum_b,
):
    sum_a[...] = start_a[...]
    sum_b[...] = start_b[...]
    edge_geo = [geo_ref[a, INNER:TILES, :] for a in range(4)]
    moment = [edge_rows(before_ref, after_ref, c) for c in range(6)]
    prepare_moments(edge_geo, INNER, moment, a_ref, b_ref)
    apply_all(list_ref, list_ref[COUNT_AT], 0, pair_ref, a_ref, b_ref, sum_a, sum_b)

    fields = field_of([geo_ref[a, 0:INNER, :] for a in range(4)], sum_a, sum_b)
    moved = jnp.zeros((OWN, SLOTS), jnp.float32)
    size = jnp.zeros((OWN, SLOTS), jnp.float32)
    for c in range(6):
        old = own_part(own_ref[c])
        new = (1.0 - RELAXATION) * old + mine_ref[0] * (mine_ref[1 + c] + fields[c])
        out_ref[c] = new
        moved = moved + (new - old) * (new - old)
        size = size + new * new
    for index, value in enumerate((moved, size)):
        total = jnp.sum(jnp.sum(value, axis=0, keepdims=True), axis=1, keepdims=True)
        size_ref[:, index : index + 1, :] = jnp.broadcast_to(
            total[None], (size_ref.shape[0], 1, SLOTS)
        )


def second_field(pair_list, geo, own, before, after, mine, pairs, sums, copies):
    return pl.pallas_call(
        second_kernel,
        name="second_field",
        in_specs=[smem_spec()] + [vmem_spec()] * 8,
        out_specs=[vmem_spec(), vmem_spec()],
        out_shape=[
            jax.ShapeDtypeStruct((6, OWN, SLOTS), jnp.float32),
            jax.ShapeDtypeStruct((copies, 2, SLOTS), jnp.float32),
        ],
        scratch_shapes=MOMENT_ROWS + [pltpu.VMEM(sums.shape, sums.dtype) for sums in SUMS],
        compiler_params=PARAMS,
        cost_estimate=cost(1_000_000_000),
    )(pair_list, geo, own, before, after, mine, pairs, *sums)


def both_ways(low, high, axis):
    count = lax.axis_size(axis)
    before = lax.ppermute(high, axis, [(i, (i + 1) % count) for i in range(count)])
    after = lax.ppermute(low, axis, [((i + 1) % count, i) for i in range(count)])
    return before, after


def joined(cells, axis, dim):
    size = cells.shape[dim]
    low = lax.slice_in_dim(cells, 0, 1, axis=dim)
    high = lax.slice_in_dim(cells, size - 1, size, axis=dim)
    before, after = both_ways(low, high, axis)
    return jnp.concatenate([before, cells, after], axis=dim)


def z_layers(cells):
    rows = cells.shape[0]
    low = lax.slice_in_dim(cells, 0, 1, axis=3)
    high = lax.slice_in_dim(cells, 1, 2, axis=3)
    before, after = both_ways(low, high, "gz")
    return (
        cells.reshape(rows, INNER, SLOTS),
        before.reshape(rows * LAYER, SLOTS),
        after.reshape(rows * LAYER, SLOTS),
    )


def exchange(parts, axes):
    return lax.all_to_all(parts, axes, 0, 0)


def device_step(fractions, polarizability, occupancy, pair_mask, perm_field, history):
    plane = lax.axis_size("gy") * lax.axis_size("gz")
    line = lax.axis_size("gx")
    stacked, gram, mine, mask = prepare(
        fractions.reshape(3, OWN, SLOTS),
        polarizability.reshape(OWN, SLOTS),
        occupancy.reshape(OWN, SLOTS),
        history.reshape(6, 6, OWN, SLOTS),
        perm_field.reshape(6, OWN, SLOTS),
        pair_mask.reshape(OWN, OFFSETS),
        plane,
    )
    gram = exchange(gram, ("gy", "gz"))
    cells = joined(stacked.reshape(ROWS, 1, 2, 2, SLOTS), "gx", 1)
    cells = joined(cells, "gy", 2)
    gram = sum_parts(gram, line)
    cells, gram = lax.optimization_barrier((cells, gram))
    gram = exchange(gram, "gx")
    own, before, after = z_layers(cells)
    inner_list, inner_pairs, moment, *sums = inner_build(mask, gram, own)
    dipoles, outer_list, geo, outer_pairs = first_field(
        mask, gram, own, before, after, mine, moment, sums
    )
    cells = joined(dipoles.reshape(6, 1, 2, 2, SLOTS), "gx", 1)
    cells = joined(cells, "gy", 2)
    own, before, after = z_layers(cells)
    sums = inner_apply(inner_list, geo, own, inner_pairs)
    induced, sizes = second_field(
        outer_list, geo, own, before, after, mine, outer_pairs, sums, plane
    )
    sizes = exchange(sizes, ("gy", "gz"))
    sizes = exchange(sum_parts(sizes, line), "gx")
    totals = jnp.sum(sizes, axis=0)
    change = jnp.sqrt(totals[0] / (totals[1] + 1.0))
    return induced.reshape(6, 1, 2, 2, SLOTS), change[0]


def solution(mesh):
    from jax.sharding import PartitionSpec as P

    tiles = P("gx", "gy", "gz", None)
    sets = P(None, "gx", "gy", "gz", None)
    return jax.shard_map(
        device_step,
        mesh=mesh,
        in_specs=(
            sets,
            tiles,
            tiles,
            tiles,
            sets,
            P(None, None, "gx", "gy", "gz", None),
        ),
        out_specs=(sets, P()),
        check_vma=False,
    )
```

```python
import jax
import jax.numpy as jnp
from jax import lax
from jax.experimental import pallas as pl
from jax.experimental.pallas import tpu as pltpu


CELL_EDGE = 10.0
SOFTENING = 0.3
THOLE_DAMP = 0.39
RELAXATION = 0.7
LN2 = 0.6931471805599453

SLOTS = 128
NX, NY, NZ = 3, 4, 4
TILES = NX * NY * NZ
OWN = 4
OFFSETS = 27
TERMS = 48
A_ROWS = 96
B_ROWS = 24
BATCH = 13
LIST = 128
COUNT_AT = LIST - 1
ROWS = 36
LATER = 4
MASK_ROW = 34
LAYER = NX * NY
INNER = 2 * LAYER
GRAM = tuple((a, b) for a in range(6) for b in range(a + 1))


def source_tile(tile, offset):
    x = offset // 9
    y = tile // 2 + offset // 3 % 3
    z = tile % 2 + offset % 3
    column = x * NY + y
    return (2, 0, 1, 3)[z] * LAYER + column


def candidates(inner):
    return [
        (t, k)
        for t in range(OWN)
        for k in range(OFFSETS)
        if k != 13 and (source_tile(t, k) < INNER) == inner
    ]


OWN_TILES = tuple(source_tile(t, 13) for t in range(OWN))


def split3(value):
    high = value.astype(jnp.bfloat16).astype(jnp.float32)
    rest = value - high
    middle = rest.astype(jnp.bfloat16).astype(jnp.float32)
    return high, middle, rest - middle


def positions(geo, first):
    shape = geo[0].shape
    tile = lax.broadcasted_iota(jnp.int32, shape, 0) + first
    second = tile - first >= LAYER
    column = tile - first - jnp.where(second, LAYER, 0)
    layer = jnp.where(second, 2, 1) if first == 0 else jnp.where(second, NZ - 1, 0)
    x = (column // NY).astype(jnp.float32)
    y = (column % NY).astype(jnp.float32)
    z = layer.astype(jnp.float32)
    return (
        (geo[0] + (x - 1.5)) * CELL_EDGE,
        (geo[1] + (y - 2.0)) * CELL_EDGE,
        (geo[2] + (z - 2.0)) * CELL_EDGE,
    )


def scale_of(polar):
    factor = (THOLE_DAMP / LN2) ** (1.0 / 3.0)
    return factor * jnp.exp(jnp.log(polar) * (-1.0 / 3.0))


def own_rows(value):
    return [value[t : t + 1] for t in OWN_TILES]


def prepare_distances(own_geo, source_geo, first, q_ref, p_ref):
    def terms(geo, at):
        r = positions(geo, at)
        a = scale_of(geo[3])
        return r, a, r[0] * r[0] + r[1] * r[1] + r[2] * r[2]

    r, a, norm = terms(source_geo, first)
    count = a.shape[0]
    sources = [a, a * (norm + SOFTENING), a * r[0], a * r[1], a * r[2]]
    r, a, norm = terms(own_geo, 0)
    targets = [a * norm, a, -2.0 * a * r[0], -2.0 * a * r[1], -2.0 * a * r[2]]
    row = 0
    for source, target in zip(sources, targets):
        source_parts = split3(source)
        target_parts = split3(target)
        for s in range(3):
            for t in range(3):
                q_ref[pl.ds(row, count, stride=TERMS + 1), :] = source_parts[s]
                for own in range(OWN):
                    p_ref[own, row : row + 1, :] = target_parts[t][
                        OWN_TILES[own] : OWN_TILES[own] + 1
                    ]
                row += 1
    zero = jnp.zeros((count, SLOTS), jnp.float32)
    for rest in range(row, TERMS):
        q_ref[pl.ds(rest, count, stride=TERMS + 1), :] = zero
        for own in range(OWN):
            p_ref[own, rest : rest + 1, :] = zero[0:1]
    last = INNER * (TERMS + 1)
    q_ref[last : last + TERMS, :] = q_ref[0:TERMS, :]


def read_mask(own_ref, mask_ref, sems):
    copies = []
    for t in range(OWN):
        row = MASK_ROW * LAYER + NY + 1 + t // 2
        copy = pltpu.make_async_copy(
            own_ref.at[t % 2, pl.ds(row, 1), :], mask_ref.at[pl.ds(t, 1), :], sems.at[t]
        )
        copy.start()
        copies.append(copy)
    return copies


def list_pairs(mask_ref, list_ref, inner):
    first = 0 if inner else INNER
    count = jnp.int32(0)
    for t, k in candidates(inner):
        list_ref[count] = (source_tile(t, k) - first) * OWN + t
        count = count + (mask_ref[t, k] != 0.0).astype(jnp.int32)
    for extra in range(BATCH):
        list_ref[count + extra] = INNER * OWN
    list_ref[COUNT_AT] = count
    return count


def trips(count):
    return (count + BATCH - 1) // BATCH


def build_all(list_ref, count, start, pair_ref, q_ref, p_ref):
    def batch(b, carry):
        for u in range(BATCH):
            slot = b * BATCH + u
            entry = list_ref[slot]
            build(start + slot, entry // OWN, entry % OWN, None, pair_ref, q_ref, p_ref)
        return carry

    lax.fori_loop(0, trips(count), batch, 0)


def build(slot, n, t, keep, pair_ref, q_ref, p_ref):
    radial, direct = pair_functions(n, t, q_ref, p_ref, keep)
    pair_ref[slot, 0 : 2 * SLOTS, :] = radial
    pair_ref[slot, 2 * SLOTS : 4 * SLOTS, :] = direct


def pair_functions(n, t, q_ref, p_ref, keep):
    dist = lax.dot_general(
        q_ref[pl.ds(n * (TERMS + 1), TERMS), :].astype(jnp.bfloat16),
        p_ref[t].astype(jnp.bfloat16),
        (((0,), (0,)), ((), ())),
        preferred_element_type=jnp.float32,
    )
    inv = lax.rsqrt(dist)
    arg = dist * (dist * inv)
    damp = jnp.exp2(-arg)
    inv2 = inv * inv
    direct = (1.0 - damp) * (inv2 * inv)
    radial = inv2 * (direct - LN2 * damp)
    if keep is not None:
        direct = jnp.where(keep, direct, 0.0)
        radial = jnp.where(keep, radial, 0.0)
    result = []
    for value in (radial, direct):
        high = value.astype(jnp.bfloat16)
        low = (value - high.astype(jnp.float32)).astype(jnp.bfloat16)
        result.append(jnp.concatenate([high, low], axis=0))
    return result


def prepare_moments(geo, first, moment, a_ref, b_ref):
    r = positions(geo, first)
    count = geo[0].shape[0]
    scale_a, scale_b = factors(geo)
    zero = jnp.zeros((count, SLOTS), jnp.float32)
    for kind in range(2):
        m = [moment[3 * kind + c] * scale_a for c in range(3)]
        outer = [r[c] * m[d] for c in range(3) for d in range(3)]
        g = outer[0] + outer[4] + outer[8]
        values = [None] + [r[c] * g for c in range(3)] + m + outer
        for index, value in enumerate(values):
            parts = (zero, zero, zero) if value is None else split3(value)
            for s, part in enumerate(parts):
                row = 32 * s + 16 * kind + index
                a_ref[pl.ds(row, count, stride=A_ROWS + 1), :] = part
    for c in range(8):
        parts = (zero, zero, zero) if c >= 6 else split3(moment[c] * scale_b)
        for s, part in enumerate(parts):
            b_ref[pl.ds(8 * s + c, count, stride=B_ROWS + 1), :] = part
    last_a = INNER * (A_ROWS + 1)
    last_b = INNER * (B_ROWS + 1)
    a_ref[last_a : last_a + A_ROWS, :] = jnp.zeros((A_ROWS, SLOTS), jnp.float32)
    b_ref[last_b : last_b + B_ROWS, :] = jnp.zeros((B_ROWS, SLOTS), jnp.float32)


def factors(geo):
    a = scale_of(geo[3])
    scale_b = a * jnp.sqrt(a)
    return scale_b * a, scale_b


def product(n, radial, direct, a_ref, b_ref):
    left = a_ref[pl.ds(n * (A_ROWS + 1), A_ROWS), :].astype(jnp.bfloat16)
    part_a = jnp.dot(
        jnp.concatenate([left, left], axis=1), radial, preferred_element_type=jnp.float32
    )
    left = b_ref[pl.ds(n * (B_ROWS + 1), B_ROWS), :].astype(jnp.bfloat16)
    part_b = jnp.dot(
        jnp.concatenate([left, left], axis=1), direct, preferred_element_type=jnp.float32
    )
    return part_a, part_b


def apply_slot(slot, n, pair_ref, a_ref, b_ref):
    return product(
        n,
        pair_ref[slot, 0 : 2 * SLOTS, :],
        pair_ref[slot, 2 * SLOTS : 4 * SLOTS, :],
        a_ref,
        b_ref,
    )


def apply_selves(pair_ref, a_ref, b_ref, sum_a, sum_b):
    for slot in range(OWN):
        sum_a[slot], sum_b[slot] = apply_slot(slot, OWN_TILES[slot], pair_ref, a_ref, b_ref)


def apply_all(list_ref, count, start, pair_ref, a_ref, b_ref, sum_a, sum_b):
    def batch(b, carry):
        for u in range(BATCH):
            slot = b * BATCH + u
            entry = list_ref[slot]
            t = entry % OWN
            part_a, part_b = apply_slot(start + slot, entry // OWN, pair_ref, a_ref, b_ref)
            sum_a[t] += part_a
            sum_b[t] += part_b
        return carry

    lax.fori_loop(0, trips(count), batch, 0)


def field_of(geo, sum_a, sum_b):
    r = positions(geo, 0)
    scale_a, scale_b = factors(geo)
    own_r = [jnp.concatenate(own_rows(r[c]), 0) for c in range(3)]
    own_a = 3.0 * jnp.concatenate(own_rows(scale_a), 0)
    own_b = jnp.concatenate(own_rows(scale_b), 0)

    def total_a(kind, index):
        row = 16 * kind + index
        return sum_a[:, row, :] + sum_a[:, 32 + row, :] + sum_a[:, 64 + row, :]

    def total_b(row):
        return sum_b[:, row, :] + sum_b[:, 8 + row, :] + sum_b[:, 16 + row, :]

    fields = []
    for kind in range(2):
        outer = [[total_a(kind, 7 + 3 * c + d) for d in range(3)] for c in range(3)]
        g = outer[0][0] + outer[1][1] + outer[2][2]
        m = [total_a(kind, 4 + c) for c in range(3)]
        dot = own_r[0] * m[0] + own_r[1] * m[1] + own_r[2] * m[2] - g
        for c in range(3):
            cross = sum(own_r[d] * outer[c][d] for d in range(3))
            radial = total_a(kind, 1 + c) - cross + own_r[c] * dot
            fields.append(own_a * radial - own_b * total_b(3 * kind + c))
    return fields


def own_part(value):
    return jnp.concatenate(own_rows(value), 0)


def solve(gram):
    count = 5
    matrix = [[gram[max(a, b), min(a, b)] for b in range(count)] for a in range(count)]
    right = [gram[count, a] for a in range(count)]
    trace = matrix[0][0]
    for a in range(1, count):
        trace = trace + matrix[a][a]
    ridge = 0.001 * trace / count + 1.0
    for a in range(count):
        matrix[a][a] = matrix[a][a] + ridge
    for c in range(count):
        for a in range(c + 1, count):
            ratio = matrix[a][c] / matrix[c][c]
            for b in range(c + 1, a + 1):
                matrix[a][b] = matrix[a][b] - ratio * matrix[b][c]
            right[a] = right[a] - ratio * right[c]
    result = [None] * count
    for a in reversed(range(count)):
        rest = right[a]
        for b in range(a + 1, count):
            rest = rest - matrix[b][a] * result[b]
        result[a] = rest / matrix[a][a]
    return result


def store_layers(ref, rows, row, value):
    for t in range(OWN):
        at = ((t % 2) * rows + row) * 2 + t // 2
        ref[at : at + 1, :] = value[t : t + 1]


def prepare_kernel(
    fractions_ref, polar_ref, occupancy_ref, history_ref, perm_ref, mask_ref,
    stacked_ref, gram_ref, own_ref,
):
    filled = occupancy_ref[...].astype(jnp.float32)
    own_ref[0] = RELAXATION * filled * polar_ref[...]
    for c in range(6):
        own_ref[1 + c] = perm_ref[c]
    masked = [[history_ref[h, c] * filled for c in range(6)] for h in range(6)]
    for a in range(3):
        store_layers(stacked_ref, ROWS, a, fractions_ref[a])
    store_layers(stacked_ref, ROWS, 3, polar_ref[...])
    for h in range(1, 6):
        for c in range(6):
            store_layers(stacked_ref, ROWS, LATER + 6 * (h - 1) + c, masked[h][c])
    allowed = jnp.concatenate(
        [mask_ref[...].astype(jnp.float32), jnp.zeros((OWN, SLOTS - OFFSETS), jnp.float32)], axis=1
    )
    store_layers(stacked_ref, ROWS, MASK_ROW, allowed)
    store_layers(stacked_ref, ROWS, ROWS - 1, jnp.zeros((OWN, SLOTS), jnp.float32))
    lane = lax.broadcasted_iota(jnp.int32, (1, SLOTS), 1)
    row = jnp.zeros((1, SLOTS), jnp.float32)
    for index, (a, b) in enumerate(GRAM):
        product = masked[a][0] * masked[b][0]
        for c in range(1, 6):
            product = product + masked[a][c] * masked[b][c]
        total = jnp.sum(jnp.sum(product, axis=0, keepdims=True), axis=1, keepdims=True)
        row = jnp.where(lane == index, total, row)
    gram_ref[...] = jnp.broadcast_to(row[None], gram_ref.shape)


def vmem_spec():
    return pl.BlockSpec(memory_space=pltpu.VMEM)


def smem_spec():
    return pl.BlockSpec(memory_space=pltpu.SMEM)


def prepare(fractions, polarizability, occupancy, history, perm, mask, copies):
    return pl.pallas_call(
        prepare_kernel,
        name="prepare",
        in_specs=[vmem_spec()] * 6,
        out_specs=[vmem_spec()] * 3,
        out_shape=[
            jax.ShapeDtypeStruct((ROWS * OWN, SLOTS), jnp.float32),
            jax.ShapeDtypeStruct((copies, 1, SLOTS), jnp.float32),
            jax.ShapeDtypeStruct((7, OWN, SLOTS), jnp.float32),
        ],
    )(fractions, polarizability, occupancy, history, perm, mask)


def sum_parts(parts, copies):
    total = jnp.sum(parts, axis=0, keepdims=True)
    return jnp.broadcast_to(total, (copies,) + total.shape[1:])


MOMENT_ROWS = [
    pltpu.VMEM(((INNER + 1) * (A_ROWS + 1), SLOTS), jnp.float32),
    pltpu.VMEM(((INNER + 1) * (B_ROWS + 1), SLOTS), jnp.float32),
]
DISTANCE_ROWS = [
    pltpu.VMEM(((INNER + 1) * (TERMS + 1), SLOTS), jnp.float32),
    pltpu.VMEM((OWN, TERMS, SLOTS), jnp.float32),
]
SUMS = [
    jax.ShapeDtypeStruct((OWN, A_ROWS, SLOTS), jnp.float32),
    jax.ShapeDtypeStruct((OWN, B_ROWS, SLOTS), jnp.float32),
]
PARAMS = pltpu.CompilerParams(vmem_limit_bytes=16 * 1024 * 1024)


def slots_for(inner):
    batches = -(-len(candidates(inner)) // BATCH)
    return batches * BATCH + (OWN if inner else 0)


def pair_shape(inner):
    return jax.ShapeDtypeStruct((slots_for(inner), 4 * SLOTS, SLOTS), jnp.bfloat16)


def cost(flops):
    return pl.CostEstimate(flops=flops, bytes_accessed=1_000_000, transcendentals=0)


def edge_rows(before_ref, after_ref, row):
    rows = pl.ds(row * LAYER, LAYER)
    return jnp.concatenate([before_ref[rows, :], after_ref[rows, :]], axis=0)


def own_rows_of(own_ref, row):
    rows = pl.ds(row * LAYER, LAYER)
    return jnp.concatenate([own_ref[0, rows, :], own_ref[1, rows, :]], axis=0)


def coefficients(gram_ref):
    total = jnp.sum(gram_ref[...], axis=0)
    return solve({ab: total[0:1, i : i + 1] for i, ab in enumerate(GRAM)})


def predict(coeffs, later):
    moment = []
    for c in range(6):
        value = coeffs[0] * later[c]
        for h in range(1, 5):
            value = value + coeffs[h] * later[6 * h + c]
        moment.append(value)
    return moment


def inner_build_kernel(
    gram_ref, own_ref,
    list_ref, pair_ref, moment_ref, sum_a, sum_b,
    mask_ref, q_ref, p_ref, a_ref, b_ref, sems,
):
    copies = read_mask(own_ref, mask_ref, sems)
    geo = [own_rows_of(own_ref, a) for a in range(4)]
    prepare_distances(geo, geo, 0, q_ref, p_ref)
    later = [own_rows_of(own_ref, row) for row in range(LATER, MASK_ROW)]
    moment = predict(coefficients(gram_ref), later)
    prepare_moments(geo, 0, moment, a_ref, b_ref)
    for c in range(6):
        moment_ref[c] = own_part(moment[c])
    keep = lax.broadcasted_iota(jnp.int32, (SLOTS, SLOTS), 0) != lax.broadcasted_iota(
        jnp.int32, (SLOTS, SLOTS), 1
    )
    for slot in range(OWN):
        build(slot, OWN_TILES[slot], slot, keep, pair_ref, q_ref, p_ref)
    for copy in copies:
        copy.wait()
    count = list_pairs(mask_ref, list_ref, True)
    build_all(list_ref, count, OWN, pair_ref, q_ref, p_ref)
    apply_selves(pair_ref, a_ref, b_ref, sum_a, sum_b)
    apply_all(list_ref, count, OWN, pair_ref, a_ref, b_ref, sum_a, sum_b)


MASK_SCRATCH = [pltpu.SMEM((OWN, SLOTS), jnp.float32)]
MASK_SEMS = [pltpu.SemaphoreType.DMA((OWN,))]


def inner_build(gram, own):
    return pl.pallas_call(
        inner_build_kernel,
        name="inner_build",
        in_specs=[vmem_spec()] * 2,
        out_specs=[smem_spec()] + [vmem_spec()] * 4,
        out_shape=[
            jax.ShapeDtypeStruct((LIST,), jnp.int32),
            pair_shape(True),
            jax.ShapeDtypeStruct((6, OWN, SLOTS), jnp.float32),
        ]
        + SUMS,
        scratch_shapes=MASK_SCRATCH + DISTANCE_ROWS + MOMENT_ROWS + MASK_SEMS,
        compiler_params=PARAMS,
        cost_estimate=cost(2_000_000_000),
    )(gram, own)


def first_kernel(
    gram_ref, own_ref, before_ref, after_ref, mine_ref, moment_ref, start_a, start_b,
    out_ref, list_ref, geo_ref, pair_ref,
    mask_ref, q_ref, p_ref, a_ref, b_ref, sum_a, sum_b, sems,
):
    copies = read_mask(own_ref, mask_ref, sems)
    own_geo = [own_rows_of(own_ref, a) for a in range(4)]
    edge_geo = [edge_rows(before_ref, after_ref, a) for a in range(4)]
    for a in range(4):
        geo_ref[a, 0:INNER, :] = own_geo[a]
        geo_ref[a, INNER:TILES, :] = edge_geo[a]
    prepare_distances(own_geo, edge_geo, INNER, q_ref, p_ref)
    sum_a[...] = start_a[...]
    sum_b[...] = start_b[...]
    moment = predict(
        coefficients(gram_ref),
        [edge_rows(before_ref, after_ref, row) for row in range(LATER, MASK_ROW)],
    )
    prepare_moments(edge_geo, INNER, moment, a_ref, b_ref)
    for copy in copies:
        copy.wait()
    count = list_pairs(mask_ref, list_ref, False)
    build_all(list_ref, count, 0, pair_ref, q_ref, p_ref)
    apply_all(list_ref, count, 0, pair_ref, a_ref, b_ref, sum_a, sum_b)

    fields = field_of(own_geo, sum_a, sum_b)
    for c in range(6):
        dipole = (1.0 - RELAXATION) * moment_ref[c] + mine_ref[0] * (mine_ref[1 + c] + fields[c])
        store_layers(out_ref, 6, c, dipole)


def first_field(gram, own, before, after, mine, moment, sums):
    return pl.pallas_call(
        first_kernel,
        name="first_field",
        in_specs=[vmem_spec()] * 8,
        out_specs=[vmem_spec(), smem_spec(), vmem_spec(), vmem_spec()],
        out_shape=[
            jax.ShapeDtypeStruct((6 * OWN, SLOTS), jnp.float32),
            jax.ShapeDtypeStruct((LIST,), jnp.int32),
            jax.ShapeDtypeStruct((4, TILES, SLOTS), jnp.float32),
            pair_shape(False),
        ],
        scratch_shapes=MASK_SCRATCH
        + DISTANCE_ROWS
        + MOMENT_ROWS
        + [pltpu.VMEM(part.shape, part.dtype) for part in SUMS]
        + MASK_SEMS,
        compiler_params=PARAMS,
        cost_estimate=cost(2_000_000_000),
    )(gram, own, before, after, mine, moment, *sums)


def inner_apply_kernel(
    list_ref, geo_ref, own_ref, pair_ref, sum_a, sum_b, a_ref, b_ref
):
    geo = [geo_ref[a, 0:INNER, :] for a in range(4)]
    prepare_moments(geo, 0, [own_rows_of(own_ref, c) for c in range(6)], a_ref, b_ref)
    apply_selves(pair_ref, a_ref, b_ref, sum_a, sum_b)
    apply_all(list_ref, list_ref[COUNT_AT], OWN, pair_ref, a_ref, b_ref, sum_a, sum_b)


def inner_apply(pair_list, geo, own, pairs):
    return pl.pallas_call(
        inner_apply_kernel,
        name="inner_apply",
        in_specs=[smem_spec()] + [vmem_spec()] * 3,
        out_specs=[vmem_spec()] * 2,
        out_shape=SUMS,
        scratch_shapes=MOMENT_ROWS,
        compiler_params=PARAMS,
        cost_estimate=cost(1_000_000_000),
    )(pair_list, geo, own, pairs)


def second_kernel(
    list_ref, geo_ref, own_ref, before_ref, after_ref, mine_ref, pair_ref, start_a, start_b,
    out_ref, size_ref, a_ref, b_ref, sum_a, sum_b,
):
    sum_a[...] = start_a[...]
    sum_b[...] = start_b[...]
    edge_geo = [geo_ref[a, INNER:TILES, :] for a in range(4)]
    moment = [edge_rows(before_ref, after_ref, c) for c in range(6)]
    prepare_moments(edge_geo, INNER, moment, a_ref, b_ref)
    apply_all(list_ref, list_ref[COUNT_AT], 0, pair_ref, a_ref, b_ref, sum_a, sum_b)

    fields = field_of([geo_ref[a, 0:INNER, :] for a in range(4)], sum_a, sum_b)
    moved = jnp.zeros((OWN, SLOTS), jnp.float32)
    size = jnp.zeros((OWN, SLOTS), jnp.float32)
    for c in range(6):
        old = own_part(own_rows_of(own_ref, c))
        new = (1.0 - RELAXATION) * old + mine_ref[0] * (mine_ref[1 + c] + fields[c])
        out_ref[c] = new
        moved = moved + (new - old) * (new - old)
        size = size + new * new
    for index, value in enumerate((moved, size)):
        total = jnp.sum(jnp.sum(value, axis=0, keepdims=True), axis=1, keepdims=True)
        size_ref[:, index : index + 1, :] = jnp.broadcast_to(
            total[None], (size_ref.shape[0], 1, SLOTS)
        )


def second_field(pair_list, geo, own, before, after, mine, pairs, sums, copies):
    return pl.pallas_call(
        second_kernel,
        name="second_field",
        in_specs=[smem_spec()] + [vmem_spec()] * 8,
        out_specs=[vmem_spec(), vmem_spec()],
        out_shape=[
            jax.ShapeDtypeStruct((6, OWN, SLOTS), jnp.float32),
            jax.ShapeDtypeStruct((copies, 2, SLOTS), jnp.float32),
        ],
        scratch_shapes=MOMENT_ROWS + [pltpu.VMEM(sums.shape, sums.dtype) for sums in SUMS],
        compiler_params=PARAMS,
        cost_estimate=cost(1_000_000_000),
    )(pair_list, geo, own, before, after, mine, pairs, *sums)


def both_ways(low, high, axis):
    count = lax.axis_size(axis)
    before = lax.ppermute(high, axis, [(i, (i + 1) % count) for i in range(count)])
    after = lax.ppermute(low, axis, [((i + 1) % count, i) for i in range(count)])
    return before, after


def joined(cells, axis, dim):
    size = cells.shape[dim]
    low = lax.slice_in_dim(cells, 0, 1, axis=dim)
    high = lax.slice_in_dim(cells, size - 1, size, axis=dim)
    before, after = both_ways(low, high, axis)
    return jnp.concatenate([before, cells, after], axis=dim)


def z_layers(cells):
    rows = cells.shape[1] * LAYER
    low = lax.slice_in_dim(cells, 0, 1, axis=0)
    high = lax.slice_in_dim(cells, 1, 2, axis=0)
    before, after = both_ways(low, high, "gz")
    return (
        cells.reshape(2, rows, SLOTS),
        before.reshape(rows, SLOTS),
        after.reshape(rows, SLOTS),
    )


def exchange(parts, axes):
    return lax.all_to_all(parts, axes, 0, 0)


def device_step(fractions, polarizability, occupancy, pair_mask, perm_field, history):
    plane = lax.axis_size("gy") * lax.axis_size("gz")
    line = lax.axis_size("gx")
    stacked, gram, mine = prepare(
        fractions.reshape(3, OWN, SLOTS),
        polarizability.reshape(OWN, SLOTS),
        occupancy.reshape(OWN, SLOTS),
        history.reshape(6, 6, OWN, SLOTS),
        perm_field.reshape(6, OWN, SLOTS),
        pair_mask.reshape(OWN, OFFSETS),
        plane,
    )
    gram = exchange(gram, ("gy", "gz"))
    cells = joined(stacked.reshape(2, ROWS, 1, 2, SLOTS), "gx", 2)
    cells = joined(cells, "gy", 3)
    gram = sum_parts(gram, line)
    gram = exchange(gram, "gx")
    own, before, after = z_layers(cells)
    inner_list, inner_pairs, moment, *sums = inner_build(gram, own)
    dipoles, outer_list, geo, outer_pairs = first_field(
        gram, own, before, after, mine, moment, sums
    )
    cells = joined(dipoles.reshape(2, 6, 1, 2, SLOTS), "gx", 2)
    cells = joined(cells, "gy", 3)
    own, before, after = z_layers(cells)
    sums = inner_apply(inner_list, geo, own, inner_pairs)
    induced, sizes = second_field(
        outer_list, geo, own, before, after, mine, outer_pairs, sums, plane
    )
    sizes = exchange(sizes, ("gy", "gz"))
    sizes = exchange(sum_parts(sizes, line), "gx")
    totals = jnp.sum(sizes, axis=0)
    change = jnp.sqrt(totals[0] / (totals[1] + 1.0))
    return induced.reshape(6, 1, 2, 2, SLOTS), change[0]


def solution(mesh):
    from jax.sharding import PartitionSpec as P

    tiles = P("gx", "gy", "gz", None)
    sets = P(None, "gx", "gy", "gz", None)
    return jax.shard_map(
        device_step,
        mesh=mesh,
        in_specs=(
            sets,
            tiles,
            tiles,
            tiles,
            sets,
            P(None, None, "gx", "gy", "gz", None),
        ),
        out_specs=(sets, P()),
        check_vma=False,
    )
```

```python
import jax
import jax.numpy as jnp
from jax import lax
from jax.experimental import pallas as pl
from jax.experimental.pallas import tpu as pltpu


CELL_EDGE = 10.0
SOFTENING = 0.3
THOLE_DAMP = 0.39
RELAXATION = 0.7
LN2 = 0.6931471805599453

SLOTS = 128
NX, NY, NZ = 3, 4, 4
TILES = NX * NY * NZ
OWN = 4
OFFSETS = 27
TERMS = 48
A_ROWS = 96
B_ROWS = 24
BATCH = 13
LIST = 128
COUNT_AT = LIST - 1
ROWS = 36
LATER = 4
MASK_ROW = 34
LAYER = NX * NY
INNER = 2 * LAYER
GRAM = tuple((a, b) for a in range(6) for b in range(a + 1))


def source_tile(tile, offset):
    x = offset // 9
    y = tile // 2 + offset // 3 % 3
    z = tile % 2 + offset % 3
    column = x * NY + y
    return (2, 0, 1, 3)[z] * LAYER + column


def candidates(inner):
    return [
        (t, k)
        for t in range(OWN)
        for k in range(OFFSETS)
        if k != 13 and (source_tile(t, k) < INNER) == inner
    ]


OWN_TILES = tuple(source_tile(t, 13) for t in range(OWN))


def split3(value):
    high = value.astype(jnp.bfloat16).astype(jnp.float32)
    rest = value - high
    middle = rest.astype(jnp.bfloat16).astype(jnp.float32)
    return high, middle, rest - middle


def positions(geo, first):
    shape = geo[0].shape
    tile = lax.broadcasted_iota(jnp.int32, shape, 0) + first
    second = tile - first >= LAYER
    column = tile - first - jnp.where(second, LAYER, 0)
    layer = jnp.where(second, 2, 1) if first == 0 else jnp.where(second, NZ - 1, 0)
    x = (column // NY).astype(jnp.float32)
    y = (column % NY).astype(jnp.float32)
    z = layer.astype(jnp.float32)
    return (
        (geo[0] + (x - 1.5)) * CELL_EDGE,
        (geo[1] + (y - 2.0)) * CELL_EDGE,
        (geo[2] + (z - 2.0)) * CELL_EDGE,
    )


def scale_of(polar):
    factor = (THOLE_DAMP / LN2) ** (1.0 / 3.0)
    return factor * jnp.exp(jnp.log(polar) * (-1.0 / 3.0))


def own_rows(value):
    return [value[t : t + 1] for t in OWN_TILES]


def prepare_distances(own_geo, source_geo, first, q_ref, p_ref):
    def terms(geo, at):
        r = positions(geo, at)
        a = scale_of(geo[3])
        return r, a, r[0] * r[0] + r[1] * r[1] + r[2] * r[2]

    r, a, norm = terms(source_geo, first)
    count = a.shape[0]
    sources = [a, a * (norm + SOFTENING), a * r[0], a * r[1], a * r[2]]
    r, a, norm = terms(own_geo, 0)
    targets = [a * norm, a, -2.0 * a * r[0], -2.0 * a * r[1], -2.0 * a * r[2]]
    row = 0
    for source, target in zip(sources, targets):
        source_parts = split3(source)
        target_parts = split3(target)
        for s in range(3):
            for t in range(3):
                q_ref[pl.ds(row, count, stride=TERMS + 1), :] = source_parts[s]
                for own in range(OWN):
                    p_ref[own, row : row + 1, :] = target_parts[t][
                        OWN_TILES[own] : OWN_TILES[own] + 1
                    ]
                row += 1
    zero = jnp.zeros((count, SLOTS), jnp.float32)
    for rest in range(row, TERMS):
        q_ref[pl.ds(rest, count, stride=TERMS + 1), :] = zero
        for own in range(OWN):
            p_ref[own, rest : rest + 1, :] = zero[0:1]
    last = INNER * (TERMS + 1)
    q_ref[last : last + TERMS, :] = q_ref[0:TERMS, :]


def read_mask(own_ref, mask_ref, sems):
    copies = []
    for t in range(OWN):
        row = MASK_ROW * LAYER + NY + 1 + t // 2
        copy = pltpu.make_async_copy(
            own_ref.at[t % 2, pl.ds(row, 1), :], mask_ref.at[pl.ds(t, 1), :], sems.at[t]
        )
        copy.start()
        copies.append(copy)
    return copies


def list_pairs(mask_ref, list_ref, inner):
    first = 0 if inner else INNER
    count = jnp.int32(0)
    for t, k in candidates(inner):
        list_ref[count] = (source_tile(t, k) - first) * OWN + t
        count = count + (mask_ref[t, k] != 0.0).astype(jnp.int32)
    for extra in range(BATCH):
        list_ref[count + extra] = INNER * OWN
    list_ref[COUNT_AT] = count
    return count


def trips(count):
    return (count + BATCH - 1) // BATCH


def build_all(list_ref, count, start, pair_ref, q_ref, p_ref):
    def batch(b, carry):
        for u in range(BATCH):
            slot = b * BATCH + u
            entry = list_ref[slot]
            build(start + slot, entry // OWN, entry % OWN, None, pair_ref, q_ref, p_ref)
        return carry

    lax.fori_loop(0, trips(count), batch, 0)


def build(slot, n, t, keep, pair_ref, q_ref, p_ref):
    radial, direct = pair_functions(n, t, q_ref, p_ref, keep)
    pair_ref[slot, 0 : 2 * SLOTS, :] = radial
    pair_ref[slot, 2 * SLOTS : 4 * SLOTS, :] = direct


def pair_functions(n, t, q_ref, p_ref, keep):
    dist = lax.dot_general(
        q_ref[pl.ds(n * (TERMS + 1), TERMS), :].astype(jnp.bfloat16),
        p_ref[t].astype(jnp.bfloat16),
        (((0,), (0,)), ((), ())),
        preferred_element_type=jnp.float32,
    )
    inv = lax.rsqrt(dist)
    arg = dist * (dist * inv)
    damp = jnp.exp2(-arg)
    inv2 = inv * inv
    direct = (1.0 - damp) * (inv2 * inv)
    radial = inv2 * (direct - LN2 * damp)
    if keep is not None:
        direct = jnp.where(keep, direct, 0.0)
        radial = jnp.where(keep, radial, 0.0)
    result = []
    for value in (radial, direct):
        high = value.astype(jnp.bfloat16)
        low = (value - high.astype(jnp.float32)).astype(jnp.bfloat16)
        result.append(jnp.concatenate([high, low], axis=0))
    return result


def prepare_moments(geo, first, moment, a_ref, b_ref):
    r = positions(geo, first)
    count = geo[0].shape[0]
    scale_a, scale_b = factors(geo)
    zero = jnp.zeros((count, SLOTS), jnp.float32)
    for kind in range(2):
        m = [moment[3 * kind + c] * scale_a for c in range(3)]
        outer = [r[c] * m[d] for c in range(3) for d in range(3)]
        g = outer[0] + outer[4] + outer[8]
        values = [None] + [r[c] * g for c in range(3)] + m + outer
        for index, value in enumerate(values):
            parts = (zero, zero, zero) if value is None else split3(value)
            for s, part in enumerate(parts):
                row = 32 * s + 16 * kind + index
                a_ref[pl.ds(row, count, stride=A_ROWS + 1), :] = part
    for c in range(8):
        parts = (zero, zero, zero) if c >= 6 else split3(moment[c] * scale_b)
        for s, part in enumerate(parts):
            b_ref[pl.ds(8 * s + c, count, stride=B_ROWS + 1), :] = part
    last_a = INNER * (A_ROWS + 1)
    last_b = INNER * (B_ROWS + 1)
    a_ref[last_a : last_a + A_ROWS, :] = jnp.zeros((A_ROWS, SLOTS), jnp.float32)
    b_ref[last_b : last_b + B_ROWS, :] = jnp.zeros((B_ROWS, SLOTS), jnp.float32)


def factors(geo):
    a = scale_of(geo[3])
    scale_b = a * jnp.sqrt(a)
    return scale_b * a, scale_b


def product(n, radial, direct, a_ref, b_ref):
    left = a_ref[pl.ds(n * (A_ROWS + 1), A_ROWS), :].astype(jnp.bfloat16)
    part_a = jnp.dot(
        jnp.concatenate([left, left], axis=1), radial, preferred_element_type=jnp.float32
    )
    left = b_ref[pl.ds(n * (B_ROWS + 1), B_ROWS), :].astype(jnp.bfloat16)
    part_b = jnp.dot(
        jnp.concatenate([left, left], axis=1), direct, preferred_element_type=jnp.float32
    )
    return part_a, part_b


def apply_slot(slot, n, pair_ref, a_ref, b_ref):
    return product(
        n,
        pair_ref[slot, 0 : 2 * SLOTS, :],
        pair_ref[slot, 2 * SLOTS : 4 * SLOTS, :],
        a_ref,
        b_ref,
    )


def apply_selves(pair_ref, a_ref, b_ref, sum_a, sum_b):
    for slot in range(OWN):
        sum_a[slot], sum_b[slot] = apply_slot(slot, OWN_TILES[slot], pair_ref, a_ref, b_ref)


def apply_all(list_ref, count, start, pair_ref, a_ref, b_ref, sum_a, sum_b):
    def batch(b, carry):
        for u in range(BATCH):
            slot = b * BATCH + u
            entry = list_ref[slot]
            t = entry % OWN
            part_a, part_b = apply_slot(start + slot, entry // OWN, pair_ref, a_ref, b_ref)
            sum_a[t] += part_a
            sum_b[t] += part_b
        return carry

    lax.fori_loop(0, trips(count), batch, 0)


def field_of(geo, sum_a, sum_b):
    r = positions(geo, 0)
    scale_a, scale_b = factors(geo)
    own_r = [jnp.concatenate(own_rows(r[c]), 0) for c in range(3)]
    own_a = 3.0 * jnp.concatenate(own_rows(scale_a), 0)
    own_b = jnp.concatenate(own_rows(scale_b), 0)

    def total_a(kind, index):
        row = 16 * kind + index
        return sum_a[:, row, :] + sum_a[:, 32 + row, :] + sum_a[:, 64 + row, :]

    def total_b(row):
        return sum_b[:, row, :] + sum_b[:, 8 + row, :] + sum_b[:, 16 + row, :]

    fields = []
    for kind in range(2):
        outer = [[total_a(kind, 7 + 3 * c + d) for d in range(3)] for c in range(3)]
        g = outer[0][0] + outer[1][1] + outer[2][2]
        m = [total_a(kind, 4 + c) for c in range(3)]
        dot = own_r[0] * m[0] + own_r[1] * m[1] + own_r[2] * m[2] - g
        for c in range(3):
            cross = sum(own_r[d] * outer[c][d] for d in range(3))
            radial = total_a(kind, 1 + c) - cross + own_r[c] * dot
            fields.append(own_a * radial - own_b * total_b(3 * kind + c))
    return fields


def own_part(value):
    return jnp.concatenate(own_rows(value), 0)


def solve(gram):
    count = 5
    matrix = [[gram[max(a, b), min(a, b)] for b in range(count)] for a in range(count)]
    right = [gram[count, a] for a in range(count)]
    trace = matrix[0][0]
    for a in range(1, count):
        trace = trace + matrix[a][a]
    ridge = 0.001 * trace / count + 1.0
    for a in range(count):
        matrix[a][a] = matrix[a][a] + ridge
    inverse = []
    for c in range(count):
        inverse.append(1.0 / matrix[c][c])
        ratios = [matrix[a][c] * inverse[c] for a in range(c + 1, count)]
        for a in range(c + 1, count):
            ratio = ratios[a - c - 1]
            for b in range(c + 1, a + 1):
                matrix[a][b] = matrix[a][b] - ratio * matrix[b][c]
            right[a] = right[a] - ratio * right[c]
    result = [None] * count
    for a in reversed(range(count)):
        rest = right[a]
        for b in range(a + 1, count):
            rest = rest - matrix[b][a] * result[b]
        result[a] = rest * inverse[a]
    return result


def store_layers(ref, rows, row, value):
    for t in range(OWN):
        at = ((t % 2) * rows + row) * 2 + t // 2
        ref[at : at + 1, :] = value[t : t + 1]


def prepare_kernel(
    fractions_ref, polar_ref, occupancy_ref, history_ref, perm_ref, mask_ref,
    stacked_ref, gram_ref, own_ref,
):
    filled = occupancy_ref[...].astype(jnp.float32)
    own_ref[0] = RELAXATION * filled * polar_ref[...]
    for c in range(6):
        own_ref[1 + c] = perm_ref[c]
    masked = [[history_ref[h, c] * filled for c in range(6)] for h in range(6)]
    for a in range(3):
        store_layers(stacked_ref, ROWS, a, fractions_ref[a])
    store_layers(stacked_ref, ROWS, 3, polar_ref[...])
    for h in range(1, 6):
        for c in range(6):
            store_layers(stacked_ref, ROWS, LATER + 6 * (h - 1) + c, masked[h][c])
    allowed = jnp.concatenate(
        [mask_ref[...].astype(jnp.float32), jnp.zeros((OWN, SLOTS - OFFSETS), jnp.float32)], axis=1
    )
    store_layers(stacked_ref, ROWS, MASK_ROW, allowed)
    store_layers(stacked_ref, ROWS, ROWS - 1, jnp.zeros((OWN, SLOTS), jnp.float32))
    lane = lax.broadcasted_iota(jnp.int32, (1, SLOTS), 1)
    row = jnp.zeros((1, SLOTS), jnp.float32)
    for index, (a, b) in enumerate(GRAM):
        product = masked[a][0] * masked[b][0]
        for c in range(1, 6):
            product = product + masked[a][c] * masked[b][c]
        total = jnp.sum(jnp.sum(product, axis=0, keepdims=True), axis=1, keepdims=True)
        row = jnp.where(lane == index, total, row)
    gram_ref[...] = jnp.broadcast_to(row[None], gram_ref.shape)


def vmem_spec():
    return pl.BlockSpec(memory_space=pltpu.VMEM)


def smem_spec():
    return pl.BlockSpec(memory_space=pltpu.SMEM)


def prepare(fractions, polarizability, occupancy, history, perm, mask, copies):
    return pl.pallas_call(
        prepare_kernel,
        name="prepare",
        in_specs=[vmem_spec()] * 6,
        out_specs=[vmem_spec()] * 3,
        out_shape=[
            jax.ShapeDtypeStruct((ROWS * OWN, SLOTS), jnp.float32),
            jax.ShapeDtypeStruct((copies, 1, SLOTS), jnp.float32),
            jax.ShapeDtypeStruct((7, OWN, SLOTS), jnp.float32),
        ],
    )(fractions, polarizability, occupancy, history, perm, mask)


def settle(values):
    lowest = jnp.finfo(jnp.float32).min
    return lax.optimization_barrier(jnp.maximum(values, lowest))


def sum_parts(parts, copies):
    total = jnp.sum(parts, axis=0, keepdims=True)
    return jnp.broadcast_to(total, (copies,) + total.shape[1:])


MOMENT_ROWS = [
    pltpu.VMEM(((INNER + 1) * (A_ROWS + 1), SLOTS), jnp.float32),
    pltpu.VMEM(((INNER + 1) * (B_ROWS + 1), SLOTS), jnp.float32),
]
DISTANCE_ROWS = [
    pltpu.VMEM(((INNER + 1) * (TERMS + 1), SLOTS), jnp.float32),
    pltpu.VMEM((OWN, TERMS, SLOTS), jnp.float32),
]
SUMS = [
    jax.ShapeDtypeStruct((OWN, A_ROWS, SLOTS), jnp.float32),
    jax.ShapeDtypeStruct((OWN, B_ROWS, SLOTS), jnp.float32),
]
PARAMS = pltpu.CompilerParams(vmem_limit_bytes=16 * 1024 * 1024)


def slots_for(inner):
    batches = -(-len(candidates(inner)) // BATCH)
    return batches * BATCH + (OWN if inner else 0)


def pair_shape(inner):
    return jax.ShapeDtypeStruct((slots_for(inner), 4 * SLOTS, SLOTS), jnp.bfloat16)


def cost(flops):
    return pl.CostEstimate(flops=flops, bytes_accessed=1_000_000, transcendentals=0)


def edge_rows(before_ref, after_ref, row):
    rows = pl.ds(row * LAYER, LAYER)
    return jnp.concatenate([before_ref[rows, :], after_ref[rows, :]], axis=0)


def own_rows_of(own_ref, row):
    rows = pl.ds(row * LAYER, LAYER)
    return jnp.concatenate([own_ref[0, rows, :], own_ref[1, rows, :]], axis=0)


def coefficients(gram_ref):
    total = jnp.sum(gram_ref[...], axis=0)
    return solve(
        {
            ab: jnp.broadcast_to(total[0:1, i : i + 1], (1, SLOTS))
            for i, ab in enumerate(GRAM)
        }
    )


def predict(coeffs, later):
    moment = []
    for c in range(6):
        value = coeffs[0] * later[c]
        for h in range(1, 5):
            value = value + coeffs[h] * later[6 * h + c]
        moment.append(value)
    return moment


def inner_build_kernel(
    gram_ref, own_ref,
    list_ref, pair_ref, moment_ref, coeffs_ref, sum_a, sum_b,
    mask_ref, q_ref, p_ref, a_ref, b_ref, sems,
):
    copies = read_mask(own_ref, mask_ref, sems)
    geo = [own_rows_of(own_ref, a) for a in range(4)]
    prepare_distances(geo, geo, 0, q_ref, p_ref)
    later = [own_rows_of(own_ref, row) for row in range(LATER, MASK_ROW)]
    coeffs = coefficients(gram_ref)
    for h in range(5):
        coeffs_ref[h : h + 1, :] = jnp.broadcast_to(coeffs[h], (1, SLOTS))
    moment = predict(coeffs, later)
    prepare_moments(geo, 0, moment, a_ref, b_ref)
    for c in range(6):
        moment_ref[c] = own_part(moment[c])
    keep = lax.broadcasted_iota(jnp.int32, (SLOTS, SLOTS), 0) != lax.broadcasted_iota(
        jnp.int32, (SLOTS, SLOTS), 1
    )
    for slot in range(OWN):
        build(slot, OWN_TILES[slot], slot, keep, pair_ref, q_ref, p_ref)
    for copy in copies:
        copy.wait()
    count = list_pairs(mask_ref, list_ref, True)
    build_all(list_ref, count, OWN, pair_ref, q_ref, p_ref)
    apply_selves(pair_ref, a_ref, b_ref, sum_a, sum_b)
    apply_all(list_ref, count, OWN, pair_ref, a_ref, b_ref, sum_a, sum_b)


MASK_SCRATCH = [pltpu.SMEM((OWN, SLOTS), jnp.float32)]
MASK_SEMS = [pltpu.SemaphoreType.DMA((OWN,))]


def inner_build(gram, own):
    return pl.pallas_call(
        inner_build_kernel,
        name="inner_build",
        in_specs=[vmem_spec()] * 2,
        out_specs=[smem_spec()] + [vmem_spec()] * 5,
        out_shape=[
            jax.ShapeDtypeStruct((LIST,), jnp.int32),
            pair_shape(True),
            jax.ShapeDtypeStruct((6, OWN, SLOTS), jnp.float32),
            jax.ShapeDtypeStruct((5, SLOTS), jnp.float32),
        ]
        + SUMS,
        scratch_shapes=MASK_SCRATCH + DISTANCE_ROWS + MOMENT_ROWS + MASK_SEMS,
        compiler_params=PARAMS,
        cost_estimate=cost(2_000_000_000),
    )(gram, own)


def first_kernel(
    coeffs_ref, own_ref, before_ref, after_ref, mine_ref, moment_ref, start_a, start_b,
    out_ref, list_ref, geo_ref, pair_ref,
    mask_ref, q_ref, p_ref, a_ref, b_ref, sum_a, sum_b, sems,
):
    copies = read_mask(own_ref, mask_ref, sems)
    own_geo = [own_rows_of(own_ref, a) for a in range(4)]
    edge_geo = [edge_rows(before_ref, after_ref, a) for a in range(4)]
    for a in range(4):
        geo_ref[a, 0:INNER, :] = own_geo[a]
        geo_ref[a, INNER:TILES, :] = edge_geo[a]
    prepare_distances(own_geo, edge_geo, INNER, q_ref, p_ref)
    sum_a[...] = start_a[...]
    sum_b[...] = start_b[...]
    moment = predict(
        [coeffs_ref[h : h + 1, :] for h in range(5)],
        [edge_rows(before_ref, after_ref, row) for row in range(LATER, MASK_ROW)],
    )
    prepare_moments(edge_geo, INNER, moment, a_ref, b_ref)
    for copy in copies:
        copy.wait()
    count = list_pairs(mask_ref, list_ref, False)
    build_all(list_ref, count, 0, pair_ref, q_ref, p_ref)
    apply_all(list_ref, count, 0, pair_ref, a_ref, b_ref, sum_a, sum_b)

    fields = field_of(own_geo, sum_a, sum_b)
    for c in range(6):
        dipole = (1.0 - RELAXATION) * moment_ref[c] + mine_ref[0] * (mine_ref[1 + c] + fields[c])
        store_layers(out_ref, 6, c, dipole)


def first_field(coeffs, own, before, after, mine, moment, sums):
    return pl.pallas_call(
        first_kernel,
        name="first_field",
        in_specs=[vmem_spec()] * 8,
        out_specs=[vmem_spec(), smem_spec(), vmem_spec(), vmem_spec()],
        out_shape=[
            jax.ShapeDtypeStruct((6 * OWN, SLOTS), jnp.float32),
            jax.ShapeDtypeStruct((LIST,), jnp.int32),
            jax.ShapeDtypeStruct((4, TILES, SLOTS), jnp.float32),
            pair_shape(False),
        ],
        scratch_shapes=MASK_SCRATCH
        + DISTANCE_ROWS
        + MOMENT_ROWS
        + [pltpu.VMEM(part.shape, part.dtype) for part in SUMS]
        + MASK_SEMS,
        compiler_params=PARAMS,
        cost_estimate=cost(2_000_000_000),
    )(coeffs, own, before, after, mine, moment, *sums)


def inner_apply_kernel(
    list_ref, geo_ref, own_ref, pair_ref, sum_a, sum_b, a_ref, b_ref
):
    geo = [geo_ref[a, 0:INNER, :] for a in range(4)]
    prepare_moments(geo, 0, [own_rows_of(own_ref, c) for c in range(6)], a_ref, b_ref)
    apply_selves(pair_ref, a_ref, b_ref, sum_a, sum_b)
    apply_all(list_ref, list_ref[COUNT_AT], OWN, pair_ref, a_ref, b_ref, sum_a, sum_b)


def inner_apply(pair_list, geo, own, pairs):
    return pl.pallas_call(
        inner_apply_kernel,
        name="inner_apply",
        in_specs=[smem_spec()] + [vmem_spec()] * 3,
        out_specs=[vmem_spec()] * 2,
        out_shape=SUMS,
        scratch_shapes=MOMENT_ROWS,
        compiler_params=PARAMS,
        cost_estimate=cost(1_000_000_000),
    )(pair_list, geo, own, pairs)


def second_kernel(
    list_ref, geo_ref, own_ref, before_ref, after_ref, mine_ref, pair_ref, start_a, start_b,
    out_ref, size_ref, a_ref, b_ref, sum_a, sum_b,
):
    sum_a[...] = start_a[...]
    sum_b[...] = start_b[...]
    edge_geo = [geo_ref[a, INNER:TILES, :] for a in range(4)]
    moment = [edge_rows(before_ref, after_ref, c) for c in range(6)]
    prepare_moments(edge_geo, INNER, moment, a_ref, b_ref)
    apply_all(list_ref, list_ref[COUNT_AT], 0, pair_ref, a_ref, b_ref, sum_a, sum_b)

    fields = field_of([geo_ref[a, 0:INNER, :] for a in range(4)], sum_a, sum_b)
    moved = jnp.zeros((OWN, SLOTS), jnp.float32)
    size = jnp.zeros((OWN, SLOTS), jnp.float32)
    for c in range(6):
        old = own_part(own_rows_of(own_ref, c))
        new = (1.0 - RELAXATION) * old + mine_ref[0] * (mine_ref[1 + c] + fields[c])
        out_ref[c] = new
        moved = moved + (new - old) * (new - old)
        size = size + new * new
    for index, value in enumerate((moved, size)):
        total = jnp.sum(jnp.sum(value, axis=0, keepdims=True), axis=1, keepdims=True)
        size_ref[:, index : index + 1, :] = jnp.broadcast_to(
            total[None], (size_ref.shape[0], 1, SLOTS)
        )


def second_field(pair_list, geo, own, before, after, mine, pairs, sums, copies):
    return pl.pallas_call(
        second_kernel,
        name="second_field",
        in_specs=[smem_spec()] + [vmem_spec()] * 8,
        out_specs=[vmem_spec(), vmem_spec()],
        out_shape=[
            jax.ShapeDtypeStruct((6, OWN, SLOTS), jnp.float32),
            jax.ShapeDtypeStruct((copies, 2, SLOTS), jnp.float32),
        ],
        scratch_shapes=MOMENT_ROWS + [pltpu.VMEM(sums.shape, sums.dtype) for sums in SUMS],
        compiler_params=PARAMS,
        cost_estimate=cost(1_000_000_000),
    )(pair_list, geo, own, before, after, mine, pairs, *sums)


def both_ways(low, high, axis):
    count = lax.axis_size(axis)
    before = lax.ppermute(high, axis, [(i, (i + 1) % count) for i in range(count)])
    after = lax.ppermute(low, axis, [((i + 1) % count, i) for i in range(count)])
    return before, after


def joined(cells, axis, dim, middle=None):
    size = cells.shape[dim]
    low = lax.slice_in_dim(cells, 0, 1, axis=dim)
    high = lax.slice_in_dim(cells, size - 1, size, axis=dim)
    before, after = both_ways(low, high, axis)
    middle = cells if middle is None else middle
    return jnp.concatenate([before, middle, after], axis=dim)


def z_layers(cells):
    rows = cells.shape[1] * LAYER
    low = lax.slice_in_dim(cells, 0, 1, axis=0)
    high = lax.slice_in_dim(cells, 1, 2, axis=0)
    before, after = both_ways(low, high, "gz")
    return (
        cells.reshape(2, rows, SLOTS),
        before.reshape(rows, SLOTS),
        after.reshape(rows, SLOTS),
    )


def exchange(parts, axes):
    return lax.all_to_all(parts, axes, 0, 0)


def device_step(fractions, polarizability, occupancy, pair_mask, perm_field, history):
    plane = lax.axis_size("gy") * lax.axis_size("gz")
    line = lax.axis_size("gx")
    stacked, gram, mine = prepare(
        fractions.reshape(3, OWN, SLOTS),
        polarizability.reshape(OWN, SLOTS),
        occupancy.reshape(OWN, SLOTS),
        history.reshape(6, 6, OWN, SLOTS),
        perm_field.reshape(6, OWN, SLOTS),
        pair_mask.reshape(OWN, OFFSETS),
        plane,
    )
    gram = exchange(gram, ("gy", "gz"))
    cells = joined(
        stacked.reshape(2, ROWS, 1, 2, SLOTS),
        "gx",
        2,
        settle(stacked).reshape(2, ROWS, 1, 2, SLOTS),
    )
    mine = settle(mine)
    cells = lax.optimization_barrier(cells)
    cells = joined(cells, "gy", 3)
    gram = sum_parts(gram, line)
    gram = exchange(gram, "gx")
    own, before, after = z_layers(cells)
    inner_list, inner_pairs, moment, coeffs, *sums = inner_build(gram, own)
    dipoles, outer_list, geo, outer_pairs = first_field(
        coeffs, own, before, after, mine, moment, sums
    )
    cells = joined(dipoles.reshape(2, 6, 1, 2, SLOTS), "gx", 2)
    cells = joined(cells, "gy", 3)
    own, before, after = z_layers(cells)
    sums = inner_apply(inner_list, geo, own, inner_pairs)
    induced, sizes = second_field(
        outer_list, geo, own, before, after, mine, outer_pairs, sums, plane
    )
    sizes = exchange(sizes, ("gy", "gz"))
    sizes = exchange(sum_parts(sizes, line), "gx")
    totals = jnp.sum(sizes, axis=0)
    change = jnp.sqrt(totals[0] / (totals[1] + 1.0))
    return induced.reshape(6, 1, 2, 2, SLOTS), change[0]


def solution(mesh):
    from jax.sharding import PartitionSpec as P

    tiles = P("gx", "gy", "gz", None)
    sets = P(None, "gx", "gy", "gz", None)
    return jax.shard_map(
        device_step,
        mesh=mesh,
        in_specs=(
            sets,
            tiles,
            tiles,
            tiles,
            sets,
            P(None, None, "gx", "gy", "gz", None),
        ),
        out_specs=(sets, P()),
        check_vma=False,
    )
```

```python
import jax
import jax.numpy as jnp
from jax import lax
from jax.experimental import pallas as pl
from jax.experimental.pallas import tpu as pltpu


CELL_EDGE = 10.0
SOFTENING = 0.3
THOLE_DAMP = 0.39
RELAXATION = 0.7
LN2 = 0.6931471805599453

SLOTS = 128
NX, NY, NZ = 3, 4, 4
TILES = NX * NY * NZ
OWN = 4
OFFSETS = 27
TERMS = 48
A_ROWS = 96
B_ROWS = 24
INNER_BATCH = 13
OUTER_BATCH = 15
LIST = 128
COUNT_AT = LIST - 1
ROWS = 36
LATER = 4
MASK_ROW = 34
LAYER = NX * NY
INNER = 2 * LAYER
GRAM = tuple((a, b) for a in range(6) for b in range(a + 1))


def source_tile(tile, offset):
    x = offset // 9
    y = tile // 2 + offset // 3 % 3
    z = tile % 2 + offset % 3
    column = x * NY + y
    return (2, 0, 1, 3)[z] * LAYER + column


def candidates(inner):
    return [
        (t, k)
        for t in range(OWN)
        for k in range(OFFSETS)
        if k != 13 and (source_tile(t, k) < INNER) == inner
    ]


OWN_TILES = tuple(source_tile(t, 13) for t in range(OWN))


def split3(value):
    high = value.astype(jnp.bfloat16).astype(jnp.float32)
    rest = value - high
    middle = rest.astype(jnp.bfloat16).astype(jnp.float32)
    return high, middle, rest - middle


def positions(geo, first):
    shape = geo[0].shape
    tile = lax.broadcasted_iota(jnp.int32, shape, 0) + first
    second = tile - first >= LAYER
    column = tile - first - jnp.where(second, LAYER, 0)
    layer = jnp.where(second, 2, 1) if first == 0 else jnp.where(second, NZ - 1, 0)
    x = (column // NY).astype(jnp.float32)
    y = (column % NY).astype(jnp.float32)
    z = layer.astype(jnp.float32)
    return (
        (geo[0] + (x - 1.5)) * CELL_EDGE,
        (geo[1] + (y - 2.0)) * CELL_EDGE,
        (geo[2] + (z - 2.0)) * CELL_EDGE,
    )


def scale_of(polar):
    factor = (THOLE_DAMP / LN2) ** (1.0 / 3.0)
    return factor * jnp.exp(jnp.log(polar) * (-1.0 / 3.0))


def own_rows(value):
    return [value[t : t + 1] for t in OWN_TILES]


def prepare_distances(own_geo, source_geo, first, q_ref, p_ref):
    def terms(geo, at):
        r = positions(geo, at)
        a = scale_of(geo[3])
        return r, a, r[0] * r[0] + r[1] * r[1] + r[2] * r[2]

    r, a, norm = terms(source_geo, first)
    count = a.shape[0]
    sources = [a, a * (norm + SOFTENING), a * r[0], a * r[1], a * r[2]]
    r, a, norm = terms(own_geo, 0)
    targets = [a * norm, a, -2.0 * a * r[0], -2.0 * a * r[1], -2.0 * a * r[2]]
    row = 0
    for source, target in zip(sources, targets):
        source_parts = split3(source)
        target_parts = split3(target)
        for s in range(3):
            for t in range(3):
                q_ref[pl.ds(row, count, stride=TERMS + 1), :] = source_parts[s]
                for own in range(OWN):
                    p_ref[own, row : row + 1, :] = target_parts[t][
                        OWN_TILES[own] : OWN_TILES[own] + 1
                    ]
                row += 1
    zero = jnp.zeros((count, SLOTS), jnp.float32)
    for rest in range(row, TERMS):
        q_ref[pl.ds(rest, count, stride=TERMS + 1), :] = zero
        for own in range(OWN):
            p_ref[own, rest : rest + 1, :] = zero[0:1]
    last = INNER * (TERMS + 1)
    q_ref[last : last + TERMS, :] = q_ref[0:TERMS, :]


def read_mask(own_ref, mask_ref, sems):
    copies = []
    for t in range(OWN):
        row = MASK_ROW * LAYER + NY + 1 + t // 2
        copy = pltpu.make_async_copy(
            own_ref.at[t % 2, pl.ds(row, 1), :], mask_ref.at[pl.ds(t, 1), :], sems.at[t]
        )
        copy.start()
        copies.append(copy)
    return copies


def list_pairs(mask_ref, list_ref, inner):
    first = 0 if inner else INNER
    count = jnp.int32(0)
    for t, k in candidates(inner):
        list_ref[count] = (source_tile(t, k) - first) * OWN + t
        count = count + (mask_ref[t, k] != 0.0).astype(jnp.int32)
    for extra in range(OUTER_BATCH):
        list_ref[count + extra] = INNER * OWN
    list_ref[COUNT_AT] = count
    return count


def trips(count, batch):
    return (count + batch - 1) // batch


def build_all(list_ref, count, start, size, pair_ref, q_ref, p_ref):
    def batch(b, carry):
        for u in range(size):
            slot = b * size + u
            entry = list_ref[slot]
            build(start + slot, entry // OWN, entry % OWN, None, pair_ref, q_ref, p_ref)
        return carry

    lax.fori_loop(0, trips(count, size), batch, 0)


def build(slot, n, t, keep, pair_ref, q_ref, p_ref):
    radial, direct = pair_functions(n, t, q_ref, p_ref, keep)
    pair_ref[slot, 0 : 2 * SLOTS, :] = radial
    pair_ref[slot, 2 * SLOTS : 4 * SLOTS, :] = direct


def pair_functions(n, t, q_ref, p_ref, keep):
    dist = lax.dot_general(
        q_ref[pl.ds(n * (TERMS + 1), TERMS), :].astype(jnp.bfloat16),
        p_ref[t].astype(jnp.bfloat16),
        (((0,), (0,)), ((), ())),
        preferred_element_type=jnp.float32,
    )
    inv = lax.rsqrt(dist)
    arg = dist * (dist * inv)
    damp = jnp.exp2(-arg)
    inv2 = inv * inv
    direct = (1.0 - damp) * (inv2 * inv)
    radial = inv2 * (direct - LN2 * damp)
    if keep is not None:
        direct = jnp.where(keep, direct, 0.0)
        radial = jnp.where(keep, radial, 0.0)
    result = []
    for value in (radial, direct):
        high = value.astype(jnp.bfloat16)
        low = (value - high.astype(jnp.float32)).astype(jnp.bfloat16)
        result.append(jnp.concatenate([high, low], axis=0))
    return result


def prepare_moments(geo, first, moment, a_ref, b_ref):
    r = positions(geo, first)
    count = geo[0].shape[0]
    scale_a, scale_b = factors(geo)
    zero = jnp.zeros((count, SLOTS), jnp.float32)
    for kind in range(2):
        m = [moment[3 * kind + c] * scale_a for c in range(3)]
        outer = [r[c] * m[d] for c in range(3) for d in range(3)]
        g = outer[0] + outer[4] + outer[8]
        values = [None] + [r[c] * g for c in range(3)] + m + outer
        for index, value in enumerate(values):
            parts = (zero, zero, zero) if value is None else split3(value)
            for s, part in enumerate(parts):
                row = 32 * s + 16 * kind + index
                a_ref[pl.ds(row, count, stride=A_ROWS + 1), :] = part
    for c in range(8):
        parts = (zero, zero, zero) if c >= 6 else split3(moment[c] * scale_b)
        for s, part in enumerate(parts):
            b_ref[pl.ds(8 * s + c, count, stride=B_ROWS + 1), :] = part
    last_a = INNER * (A_ROWS + 1)
    last_b = INNER * (B_ROWS + 1)
    a_ref[last_a : last_a + A_ROWS, :] = jnp.zeros((A_ROWS, SLOTS), jnp.float32)
    b_ref[last_b : last_b + B_ROWS, :] = jnp.zeros((B_ROWS, SLOTS), jnp.float32)


def factors(geo):
    a = scale_of(geo[3])
    scale_b = a * jnp.sqrt(a)
    return scale_b * a, scale_b


def product(n, radial, direct, a_ref, b_ref):
    left = a_ref[pl.ds(n * (A_ROWS + 1), A_ROWS), :].astype(jnp.bfloat16)
    part_a = jnp.dot(
        jnp.concatenate([left, left], axis=1), radial, preferred_element_type=jnp.float32
    )
    left = b_ref[pl.ds(n * (B_ROWS + 1), B_ROWS), :].astype(jnp.bfloat16)
    part_b = jnp.dot(
        jnp.concatenate([left, left], axis=1), direct, preferred_element_type=jnp.float32
    )
    return part_a, part_b


def apply_slot(slot, n, pair_ref, a_ref, b_ref):
    return product(
        n,
        pair_ref[slot, 0 : 2 * SLOTS, :],
        pair_ref[slot, 2 * SLOTS : 4 * SLOTS, :],
        a_ref,
        b_ref,
    )


def apply_selves(pair_ref, a_ref, b_ref, sum_a, sum_b):
    for slot in range(OWN):
        sum_a[slot], sum_b[slot] = apply_slot(slot, OWN_TILES[slot], pair_ref, a_ref, b_ref)


def apply_all(list_ref, count, start, size, pair_ref, a_ref, b_ref, sum_a, sum_b):
    def batch(b, carry):
        for u in range(size):
            slot = b * size + u
            entry = list_ref[slot]
            t = entry % OWN
            part_a, part_b = apply_slot(start + slot, entry // OWN, pair_ref, a_ref, b_ref)
            sum_a[t] += part_a
            sum_b[t] += part_b
        return carry

    lax.fori_loop(0, trips(count, size), batch, 0)


def field_of(geo, sum_a, sum_b):
    r = positions(geo, 0)
    scale_a, scale_b = factors(geo)
    own_r = [jnp.concatenate(own_rows(r[c]), 0) for c in range(3)]
    own_a = 3.0 * jnp.concatenate(own_rows(scale_a), 0)
    own_b = jnp.concatenate(own_rows(scale_b), 0)

    def total_a(kind, index):
        row = 16 * kind + index
        return sum_a[:, row, :] + sum_a[:, 32 + row, :] + sum_a[:, 64 + row, :]

    def total_b(row):
        return sum_b[:, row, :] + sum_b[:, 8 + row, :] + sum_b[:, 16 + row, :]

    fields = []
    for kind in range(2):
        outer = [[total_a(kind, 7 + 3 * c + d) for d in range(3)] for c in range(3)]
        g = outer[0][0] + outer[1][1] + outer[2][2]
        m = [total_a(kind, 4 + c) for c in range(3)]
        dot = own_r[0] * m[0] + own_r[1] * m[1] + own_r[2] * m[2] - g
        for c in range(3):
            cross = sum(own_r[d] * outer[c][d] for d in range(3))
            radial = total_a(kind, 1 + c) - cross + own_r[c] * dot
            fields.append(own_a * radial - own_b * total_b(3 * kind + c))
    return fields


def own_part(value):
    return jnp.concatenate(own_rows(value), 0)


def solve(gram):
    count = 5
    matrix = [[gram[max(a, b), min(a, b)] for b in range(count)] for a in range(count)]
    right = [gram[count, a] for a in range(count)]
    trace = matrix[0][0]
    for a in range(1, count):
        trace = trace + matrix[a][a]
    ridge = 0.001 * trace / count + 1.0
    for a in range(count):
        matrix[a][a] = matrix[a][a] + ridge
    inverse = []
    for c in range(count):
        inverse.append(1.0 / matrix[c][c])
        ratios = [matrix[a][c] * inverse[c] for a in range(c + 1, count)]
        for a in range(c + 1, count):
            ratio = ratios[a - c - 1]
            for b in range(c + 1, a + 1):
                matrix[a][b] = matrix[a][b] - ratio * matrix[b][c]
            right[a] = right[a] - ratio * right[c]
    result = [None] * count
    for a in reversed(range(count)):
        rest = right[a]
        for b in range(a + 1, count):
            rest = rest - matrix[b][a] * result[b]
        result[a] = rest * inverse[a]
    return result


def store_layers(ref, rows, row, value):
    for t in range(OWN):
        at = ((t % 2) * rows + row) * 2 + t // 2
        ref[at : at + 1, :] = value[t : t + 1]


def prepare_kernel(
    fractions_ref, polar_ref, occupancy_ref, history_ref, perm_ref, mask_ref,
    stacked_ref, gram_ref, both_ref,
):
    filled = occupancy_ref[...].astype(jnp.float32)
    start = ROWS * OWN
    both_ref[start : start + OWN, :] = RELAXATION * filled * polar_ref[...]
    for c in range(6):
        at = start + OWN * (1 + c)
        both_ref[at : at + OWN, :] = perm_ref[c]
    masked = [[history_ref[h, c] * filled for c in range(6)] for h in range(6)]
    for a in range(3):
        store_layers(stacked_ref, ROWS, a, fractions_ref[a])
    store_layers(stacked_ref, ROWS, 3, polar_ref[...])
    for h in range(1, 6):
        for c in range(6):
            store_layers(stacked_ref, ROWS, LATER + 6 * (h - 1) + c, masked[h][c])
    allowed = jnp.concatenate(
        [mask_ref[...].astype(jnp.float32), jnp.zeros((OWN, SLOTS - OFFSETS), jnp.float32)], axis=1
    )
    store_layers(stacked_ref, ROWS, MASK_ROW, allowed)
    store_layers(stacked_ref, ROWS, ROWS - 1, jnp.zeros((OWN, SLOTS), jnp.float32))
    both_ref[0:start, :] = stacked_ref[...]
    both_ref[start + 7 * OWN :, :] = jnp.zeros((4, SLOTS), jnp.float32)
    lane = lax.broadcasted_iota(jnp.int32, (1, SLOTS), 1)
    row = jnp.zeros((1, SLOTS), jnp.float32)
    for index, (a, b) in enumerate(GRAM):
        product = masked[a][0] * masked[b][0]
        for c in range(1, 6):
            product = product + masked[a][c] * masked[b][c]
        total = jnp.sum(jnp.sum(product, axis=0, keepdims=True), axis=1, keepdims=True)
        row = jnp.where(lane == index, total, row)
    gram_ref[...] = jnp.broadcast_to(row[None], gram_ref.shape)


def vmem_spec():
    return pl.BlockSpec(memory_space=pltpu.VMEM)


def smem_spec():
    return pl.BlockSpec(memory_space=pltpu.SMEM)


def prepare(fractions, polarizability, occupancy, history, perm, mask, copies):
    return pl.pallas_call(
        prepare_kernel,
        name="prepare",
        in_specs=[vmem_spec()] * 6,
        out_specs=[vmem_spec()] * 3,
        out_shape=[
            jax.ShapeDtypeStruct((ROWS * OWN, SLOTS), jnp.float32),
            jax.ShapeDtypeStruct((copies, 1, SLOTS), jnp.float32),
            jax.ShapeDtypeStruct(((ROWS + 7) * OWN + 4, SLOTS), jnp.float32),
        ],
    )(fractions, polarizability, occupancy, history, perm, mask)


def settle(values):
    lowest = jnp.finfo(jnp.float32).min
    return lax.optimization_barrier(jnp.maximum(values, lowest))


def sum_parts(parts, copies):
    total = jnp.sum(parts, axis=0, keepdims=True)
    return jnp.broadcast_to(total, (copies,) + total.shape[1:])


MOMENT_ROWS = [
    pltpu.VMEM(((INNER + 1) * (A_ROWS + 1), SLOTS), jnp.float32),
    pltpu.VMEM(((INNER + 1) * (B_ROWS + 1), SLOTS), jnp.float32),
]
DISTANCE_ROWS = [
    pltpu.VMEM(((INNER + 1) * (TERMS + 1), SLOTS), jnp.float32),
    pltpu.VMEM((OWN, TERMS, SLOTS), jnp.float32),
]
SUMS = [
    jax.ShapeDtypeStruct((OWN, A_ROWS, SLOTS), jnp.float32),
    jax.ShapeDtypeStruct((OWN, B_ROWS, SLOTS), jnp.float32),
]
PARAMS = pltpu.CompilerParams(vmem_limit_bytes=16 * 1024 * 1024)


def slots_for(inner):
    size = INNER_BATCH if inner else OUTER_BATCH
    batches = -(-len(candidates(inner)) // size)
    return batches * size + (OWN if inner else 0)


def pair_shape(inner):
    return jax.ShapeDtypeStruct((slots_for(inner), 4 * SLOTS, SLOTS), jnp.bfloat16)


def cost(flops):
    return pl.CostEstimate(flops=flops, bytes_accessed=1_000_000, transcendentals=0)


def edge_rows(before_ref, after_ref, row):
    rows = pl.ds(row * LAYER, LAYER)
    return jnp.concatenate([before_ref[rows, :], after_ref[rows, :]], axis=0)


def own_rows_of(own_ref, row):
    rows = pl.ds(row * LAYER, LAYER)
    return jnp.concatenate([own_ref[0, rows, :], own_ref[1, rows, :]], axis=0)


def coefficients(gram_ref):
    total = jnp.sum(gram_ref[...], axis=0)
    return solve(
        {
            ab: jnp.broadcast_to(total[0:1, i : i + 1], (1, SLOTS))
            for i, ab in enumerate(GRAM)
        }
    )


def predict(coeffs, later):
    moment = []
    for c in range(6):
        value = coeffs[0] * later[c]
        for h in range(1, 5):
            value = value + coeffs[h] * later[6 * h + c]
        moment.append(value)
    return moment


def inner_build_kernel(
    gram_ref, own_ref,
    list_ref, pair_ref, moment_ref, coeffs_ref, sum_a, sum_b,
    mask_ref, q_ref, p_ref, a_ref, b_ref, sems,
):
    copies = read_mask(own_ref, mask_ref, sems)
    geo = [own_rows_of(own_ref, a) for a in range(4)]
    prepare_distances(geo, geo, 0, q_ref, p_ref)
    later = [own_rows_of(own_ref, row) for row in range(LATER, MASK_ROW)]
    coeffs = coefficients(gram_ref)
    for h in range(5):
        coeffs_ref[h : h + 1, :] = jnp.broadcast_to(coeffs[h], (1, SLOTS))
    moment = predict(coeffs, later)
    prepare_moments(geo, 0, moment, a_ref, b_ref)
    for c in range(6):
        moment_ref[c] = own_part(moment[c])
    keep = lax.broadcasted_iota(jnp.int32, (SLOTS, SLOTS), 0) != lax.broadcasted_iota(
        jnp.int32, (SLOTS, SLOTS), 1
    )
    for slot in range(OWN):
        build(slot, OWN_TILES[slot], slot, keep, pair_ref, q_ref, p_ref)
    for copy in copies:
        copy.wait()
    count = list_pairs(mask_ref, list_ref, True)
    build_all(list_ref, count, OWN, INNER_BATCH, pair_ref, q_ref, p_ref)
    apply_selves(pair_ref, a_ref, b_ref, sum_a, sum_b)
    apply_all(list_ref, count, OWN, INNER_BATCH, pair_ref, a_ref, b_ref, sum_a, sum_b)


MASK_SCRATCH = [pltpu.SMEM((OWN, SLOTS), jnp.float32)]
MASK_SEMS = [pltpu.SemaphoreType.DMA((OWN,))]


def inner_build(gram, own):
    return pl.pallas_call(
        inner_build_kernel,
        name="inner_build",
        in_specs=[vmem_spec()] * 2,
        out_specs=[smem_spec()] + [vmem_spec()] * 5,
        out_shape=[
            jax.ShapeDtypeStruct((LIST,), jnp.int32),
            pair_shape(True),
            jax.ShapeDtypeStruct((6, OWN, SLOTS), jnp.float32),
            jax.ShapeDtypeStruct((5, SLOTS), jnp.float32),
        ]
        + SUMS,
        scratch_shapes=MASK_SCRATCH + DISTANCE_ROWS + MOMENT_ROWS + MASK_SEMS,
        compiler_params=PARAMS,
        cost_estimate=cost(2_000_000_000),
    )(gram, own)


def first_kernel(
    coeffs_ref, own_ref, before_ref, after_ref, mine_ref, moment_ref, start_a, start_b,
    out_ref, list_ref, geo_ref, pair_ref,
    mask_ref, q_ref, p_ref, a_ref, b_ref, sum_a, sum_b, sems,
):
    copies = read_mask(own_ref, mask_ref, sems)
    own_geo = [own_rows_of(own_ref, a) for a in range(4)]
    edge_geo = [edge_rows(before_ref, after_ref, a) for a in range(4)]
    for a in range(4):
        geo_ref[a, 0:INNER, :] = own_geo[a]
        geo_ref[a, INNER:TILES, :] = edge_geo[a]
    prepare_distances(own_geo, edge_geo, INNER, q_ref, p_ref)
    sum_a[...] = start_a[...]
    sum_b[...] = start_b[...]
    moment = predict(
        [coeffs_ref[h : h + 1, :] for h in range(5)],
        [edge_rows(before_ref, after_ref, row) for row in range(LATER, MASK_ROW)],
    )
    prepare_moments(edge_geo, INNER, moment, a_ref, b_ref)
    for copy in copies:
        copy.wait()
    count = list_pairs(mask_ref, list_ref, False)
    build_all(list_ref, count, 0, OUTER_BATCH, pair_ref, q_ref, p_ref)
    apply_all(list_ref, count, 0, OUTER_BATCH, pair_ref, a_ref, b_ref, sum_a, sum_b)

    fields = field_of(own_geo, sum_a, sum_b)
    for c in range(6):
        dipole = (1.0 - RELAXATION) * moment_ref[c] + mine_ref[0] * (mine_ref[1 + c] + fields[c])
        store_layers(out_ref, 6, c, dipole)


def first_field(coeffs, own, before, after, mine, moment, sums):
    return pl.pallas_call(
        first_kernel,
        name="first_field",
        in_specs=[vmem_spec()] * 8,
        out_specs=[vmem_spec(), smem_spec(), vmem_spec(), vmem_spec()],
        out_shape=[
            jax.ShapeDtypeStruct((6 * OWN, SLOTS), jnp.float32),
            jax.ShapeDtypeStruct((LIST,), jnp.int32),
            jax.ShapeDtypeStruct((4, TILES, SLOTS), jnp.float32),
            pair_shape(False),
        ],
        scratch_shapes=MASK_SCRATCH
        + DISTANCE_ROWS
        + MOMENT_ROWS
        + [pltpu.VMEM(part.shape, part.dtype) for part in SUMS]
        + MASK_SEMS,
        compiler_params=PARAMS,
        cost_estimate=cost(2_000_000_000),
    )(coeffs, own, before, after, mine, moment, *sums)


def inner_apply_kernel(
    list_ref, geo_ref, own_ref, pair_ref, sum_a, sum_b, a_ref, b_ref
):
    geo = [geo_ref[a, 0:INNER, :] for a in range(4)]
    prepare_moments(geo, 0, [own_rows_of(own_ref, c) for c in range(6)], a_ref, b_ref)
    apply_selves(pair_ref, a_ref, b_ref, sum_a, sum_b)
    apply_all(list_ref, list_ref[COUNT_AT], OWN, INNER_BATCH, pair_ref, a_ref, b_ref, sum_a, sum_b)


def inner_apply(pair_list, geo, own, pairs):
    return pl.pallas_call(
        inner_apply_kernel,
        name="inner_apply",
        in_specs=[smem_spec()] + [vmem_spec()] * 3,
        out_specs=[vmem_spec()] * 2,
        out_shape=SUMS,
        scratch_shapes=MOMENT_ROWS,
        compiler_params=PARAMS,
        cost_estimate=cost(1_000_000_000),
    )(pair_list, geo, own, pairs)


def second_kernel(
    list_ref, geo_ref, own_ref, before_ref, after_ref, mine_ref, pair_ref, start_a, start_b,
    out_ref, size_ref, a_ref, b_ref, sum_a, sum_b,
):
    sum_a[...] = start_a[...]
    sum_b[...] = start_b[...]
    edge_geo = [geo_ref[a, INNER:TILES, :] for a in range(4)]
    moment = [edge_rows(before_ref, after_ref, c) for c in range(6)]
    prepare_moments(edge_geo, INNER, moment, a_ref, b_ref)
    apply_all(list_ref, list_ref[COUNT_AT], 0, OUTER_BATCH, pair_ref, a_ref, b_ref, sum_a, sum_b)

    fields = field_of([geo_ref[a, 0:INNER, :] for a in range(4)], sum_a, sum_b)
    moved = jnp.zeros((OWN, SLOTS), jnp.float32)
    size = jnp.zeros((OWN, SLOTS), jnp.float32)
    for c in range(6):
        old = own_part(own_rows_of(own_ref, c))
        new = (1.0 - RELAXATION) * old + mine_ref[0] * (mine_ref[1 + c] + fields[c])
        out_ref[c] = new
        moved = moved + (new - old) * (new - old)
        size = size + new * new
    for index, value in enumerate((moved, size)):
        total = jnp.sum(jnp.sum(value, axis=0, keepdims=True), axis=1, keepdims=True)
        size_ref[:, index : index + 1, :] = jnp.broadcast_to(
            total[None], (size_ref.shape[0], 1, SLOTS)
        )


def second_field(pair_list, geo, own, before, after, mine, pairs, sums, copies):
    return pl.pallas_call(
        second_kernel,
        name="second_field",
        in_specs=[smem_spec()] + [vmem_spec()] * 8,
        out_specs=[vmem_spec(), vmem_spec()],
        out_shape=[
            jax.ShapeDtypeStruct((6, OWN, SLOTS), jnp.float32),
            jax.ShapeDtypeStruct((copies, 2, SLOTS), jnp.float32),
        ],
        scratch_shapes=MOMENT_ROWS + [pltpu.VMEM(sums.shape, sums.dtype) for sums in SUMS],
        compiler_params=PARAMS,
        cost_estimate=cost(1_000_000_000),
    )(pair_list, geo, own, before, after, mine, pairs, *sums)


def both_ways(low, high, axis):
    count = lax.axis_size(axis)
    before = lax.ppermute(high, axis, [(i, (i + 1) % count) for i in range(count)])
    after = lax.ppermute(low, axis, [((i + 1) % count, i) for i in range(count)])
    return before, after


def joined(cells, axis, dim, middle=None):
    size = cells.shape[dim]
    low = lax.slice_in_dim(cells, 0, 1, axis=dim)
    high = lax.slice_in_dim(cells, size - 1, size, axis=dim)
    before, after = both_ways(low, high, axis)
    middle = cells if middle is None else middle
    return jnp.concatenate([before, middle, after], axis=dim)


def z_layers(cells):
    rows = cells.shape[1] * LAYER
    low = lax.slice_in_dim(cells, 0, 1, axis=0)
    high = lax.slice_in_dim(cells, 1, 2, axis=0)
    before, after = both_ways(low, high, "gz")
    return (
        cells.reshape(2, rows, SLOTS),
        before.reshape(rows, SLOTS),
        after.reshape(rows, SLOTS),
    )


def exchange(parts, axes):
    return lax.all_to_all(parts, axes, 0, 0)


def device_step(fractions, polarizability, occupancy, pair_mask, perm_field, history):
    plane = lax.axis_size("gy") * lax.axis_size("gz")
    line = lax.axis_size("gx")
    stacked, gram, both = prepare(
        fractions.reshape(3, OWN, SLOTS),
        polarizability.reshape(OWN, SLOTS),
        occupancy.reshape(OWN, SLOTS),
        history.reshape(6, 6, OWN, SLOTS),
        perm_field.reshape(6, OWN, SLOTS),
        pair_mask.reshape(OWN, OFFSETS),
        plane,
    )
    both = settle(both)
    gram = exchange(gram, ("gy", "gz"))
    cells = joined(
        stacked.reshape(2, ROWS, 1, 2, SLOTS),
        "gx",
        2,
        both[: ROWS * OWN].reshape(2, ROWS, 1, 2, SLOTS),
    )
    mine = both[ROWS * OWN : (ROWS + 7) * OWN].reshape(7, OWN, SLOTS)
    cells = lax.optimization_barrier(cells)
    cells = joined(cells, "gy", 3)
    gram = sum_parts(gram, line)
    gram = exchange(gram, "gx")
    own, before, after = z_layers(cells)
    inner_list, inner_pairs, moment, coeffs, *sums = inner_build(gram, own)
    dipoles, outer_list, geo, outer_pairs = first_field(
        coeffs, own, before, after, mine, moment, sums
    )
    cells = joined(dipoles.reshape(2, 6, 1, 2, SLOTS), "gx", 2)
    cells = joined(cells, "gy", 3)
    own, before, after = z_layers(cells)
    sums = inner_apply(inner_list, geo, own, inner_pairs)
    induced, sizes = second_field(
        outer_list, geo, own, before, after, mine, outer_pairs, sums, plane
    )
    sizes = exchange(sizes, ("gy", "gz"))
    sizes = exchange(sum_parts(sizes, line), "gx")
    totals = jnp.sum(sizes, axis=0)
    change = jnp.sqrt(totals[0] / (totals[1] + 1.0))
    return induced.reshape(6, 1, 2, 2, SLOTS), change[0]


def solution(mesh):
    from jax.sharding import PartitionSpec as P

    tiles = P("gx", "gy", "gz", None)
    sets = P(None, "gx", "gy", "gz", None)
    return jax.shard_map(
        device_step,
        mesh=mesh,
        in_specs=(
            sets,
            tiles,
            tiles,
            tiles,
            sets,
            P(None, None, "gx", "gy", "gz", None),
        ),
        out_specs=(sets, P()),
        check_vma=False,
    )
```
